32 devices in a mesh: lat: 4 (over x, core), lon: 4 (over z), lev: 2 (over y).
Axes of the slice: x: 2, y: 2, z: 4, core: 2. Of those that a mesh axis runs over, the one named last changes fastest.
Arguments:
- initial_heat: float32 [128, 512, 8, 128], P('lat', 'lon', 'lev'), may hold values from 0.5 to 2
- diffusivity_ratio: float32 [128, 512, 8, 128], P('lat', 'lon', 'lev'), may hold values from 0.03 to 0.15
- forcing_term: float32 [128, 512, 8, 128], P('lat', 'lon', 'lev'), may hold values from -0.2 to 0.2
Outputs:
- standard_deviation_score: float32 [128, 512, 8, 128], P('lat', 'lon', 'lev')
- temperature_end: float32 [128, 512, 8, 128], P('lat', 'lon', 'lev')
The draws below stay inside these ranges and needn't reach their ends.
All inputs are finite; a program needn't handle non-finite values.
Results may differ from the reference program's by a relative error of at most 0.00002.
Values sent between devices are 32-bit elements; how exact they have to be, the bound alone decides.
A program may use at most 128 MiB of HBM per device.

```python
import jax
import jax.numpy as jnp
from jax import lax

GRID_DEPTH = 128
GRID_WIDTH = 512
GRID_HEIGHT = 8
MEMBER_TOTAL = 128
STEPS = 4


def steps_of(key, shape, cuts, least, top_value):
    level = 1.0
    for dim, shards_of in cuts:
        draws = jax.random.uniform(jax.random.fold_in(jax.random.fold_in(key, 6), dim), (shards_of,), jnp.float32, least / len(cuts), top_value / len(cuts))
        level = level * jnp.repeat(jnp.exp(draws), shape[dim] // shards_of).reshape((-1,) + (1,) * (len(shape) - 1 - dim))
    return level


def setup_inputs(seed: int = 0) -> dict:
    key_of = jax.random.split(jax.random.key(seed), 4)
    return {
        "initial_heat": jnp.clip(0.5 + 1.5 * jax.random.uniform(key_of[0], (GRID_DEPTH, GRID_WIDTH, GRID_HEIGHT, MEMBER_TOTAL), jnp.float32) ** steps_of(key_of[0], (GRID_DEPTH, GRID_WIDTH, GRID_HEIGHT, MEMBER_TOTAL), ((0, 4), (1, 4), (2, 2)), -0.2, 0.2), 0.5, 2.0),
        "diffusivity_ratio": jnp.clip(0.03 + 0.120000007 * jax.random.uniform(key_of[1], (GRID_DEPTH, GRID_WIDTH, GRID_HEIGHT, MEMBER_TOTAL), jnp.float32) ** steps_of(key_of[1], (GRID_DEPTH, GRID_WIDTH, GRID_HEIGHT, MEMBER_TOTAL), ((0, 4), (1, 4), (2, 2)), -0.2, 0.2), 0.03, 0.15),
        "forcing_term": jnp.clip(jax.random.uniform(key_of[2], (GRID_DEPTH, GRID_WIDTH, GRID_HEIGHT, MEMBER_TOTAL), jnp.float32, -0.2, 0.2) * steps_of(key_of[2], (GRID_DEPTH, GRID_WIDTH, GRID_HEIGHT, MEMBER_TOTAL), ((0, 4), (1, 4), (2, 2)), -0.4, 0.0), -0.2, 0.2),
    }


def without_rim(values, dims):
    for dim in dims:
        values = lax.slice_in_dim(values, 1, values.shape[dim] - 1, axis=dim)
    return values

def shifted_cells(values, dim, start, dims):
    others = [other for other in dims if other != dim]
    values = without_rim(values, others)
    return lax.slice_in_dim(values, start, start + values.shape[dim] - 2, axis=dim)

def march_forward(extended_grid_state, diffusivity_ratio, forcing_term):
    middle = without_rim(extended_grid_state, (0, 1, 2))
    lower = [shifted_cells(extended_grid_state, dim, 0, (0, 1, 2)) for dim in (0, 1, 2)]
    upper = [shifted_cells(extended_grid_state, dim, 2, (0, 1, 2)) for dim in (0, 1, 2)]
    spread = lower[0] + upper[0] + lower[1] + upper[1] + lower[2] + upper[2] - 6.0 * middle
    return middle + diffusivity_ratio * spread + forcing_term

def reference(initial_heat, diffusivity_ratio, forcing_term):
    for step in range(STEPS):
        initial_heat = march_forward(jnp.pad(initial_heat, ((1, 1), (1, 1), (1, 1), (0, 0)), mode='wrap'), diffusivity_ratio, forcing_term)
    row_mean_estimate = lax.optimization_barrier(jnp.mean(initial_heat, axis=1, keepdims=True))
    deviations_from_mean = initial_heat - row_mean_estimate
    line_variance = lax.optimization_barrier(jnp.mean(deviations_from_mean * deviations_from_mean, axis=1, keepdims=True))
    standard_deviation_score = deviations_from_mean * lax.rsqrt(line_variance + 0.0001)
    return (standard_deviation_score, initial_heat)
```

```python
import functools

import jax
import jax.numpy as jnp
from jax import lax
from jax.experimental import pallas as pl
from jax.experimental.pallas import tpu as pltpu
from jax.sharding import PartitionSpec as P

STEPS = 4
PAD = 8
XBLOCK = 32
XCELLS = 16
MESH = pl.DeviceIdType.MESH


def march_kernel(
    sizes, chunks, rows,
    heat_in, ratio_in, forcing_in, raw, moments_out,
    field, ratio, forcing, xsend, xrecv, stats,
    load_heat, load_ratio, load_forcing,
    zsend_sem, zrecv_sem, xsend_sem, xrecv_sem, ysend_sem, yrecv_sem, stat_send, stat_recv,
):
    depth, width, height = sizes
    inner = pl.ds(PAD, width)
    places = {axis: lax.axis_index(axis) for axis in ("lat", "lon", "lev")}
    counts = {axis: lax.axis_size(axis) for axis in ("lat", "lon", "lev")}

    def beside(axis, offset):
        return {axis: lax.rem(places[axis] + offset + counts[axis], counts[axis])}

    def rows_of(c):
        return pl.ds(c * rows, rows)

    def load(c):
        return [
            pltpu.make_async_copy(source.at[rows_of(c)], target.at[rows_of(c)], sem.at[c])
            for source, target, sem in (
                (heat_in, raw, load_heat), (ratio_in, ratio, load_ratio), (forcing_in, forcing, load_forcing),
            )
        ]

    def zcopy(side, p, c):
        span = pl.ds(1 + c * rows, rows)
        return pltpu.make_async_remote_copy(
            src_ref=field.at[p, (1, height)[side], span, inner],
            dst_ref=field.at[p, (height + 1, 0)[side], span, inner],
            send_sem=zsend_sem.at[side, p, c], recv_sem=zrecv_sem.at[1 - side, p, c],
            device_id=beside("lev", (-1, 1)[side]), device_id_type=MESH,
        )

    def xcopy(side, p, c):
        return pltpu.make_async_remote_copy(
            src_ref=xsend.at[side, p, c], dst_ref=xrecv.at[1 - side, p, c],
            send_sem=xsend_sem.at[side, p, c], recv_sem=xrecv_sem.at[1 - side, p, c],
            device_id=beside("lon", (-1, 1)[side]), device_id_type=MESH,
        )

    def ycopy(side, p):
        return pltpu.make_async_remote_copy(
            src_ref=field.at[p, pl.ds(1, height), (1, depth)[side], inner],
            dst_ref=field.at[p, pl.ds(1, height), (depth + 1, 0)[side], inner],
            send_sem=ysend_sem.at[side, p], recv_sem=yrecv_sem.at[1 - side, p],
            device_id=beside("lat", (-1, 1)[side]), device_id_type=MESH,
        )

    def stat_copy(offset, c):
        return pltpu.make_async_remote_copy(
            src_ref=stats.at[0, c], dst_ref=stats.at[offset, c],
            send_sem=stat_send.at[offset - 1, c], recv_sem=stat_recv.at[offset - 1, c],
            device_id=beside("lon", offset), device_id_type=MESH,
        )

    def send(p, c):
        for side, end in ((0, 0), (1, chunks - 1)):
            @pl.when(c == end)
            def _():
                ycopy(side, p).start()
        for side in (0, 1):
            zcopy(side, p, c).start()
        for side in (0, 1):
            xcopy(side, p, c).start()

    def sent(p, c):
        for side, end in ((0, 0), (1, chunks - 1)):
            @pl.when(c == end)
            def _():
                ycopy(side, p).wait_send()
        for side in (0, 1):
            zcopy(side, p, c).wait_send()
            xcopy(side, p, c).wait_send()

    def arrived(p, c):
        for side, end in ((1, 0), (0, chunks - 1)):
            @pl.when(c == end)
            def _():
                ycopy(side, p).wait_recv()
        for side in (0, 1):
            xcopy(side, p, c).wait_recv()
        for side in (0, 1):
            zcopy(side, p, c).wait_recv()

    def pack(p, c, i):
        for z in range(height):
            for side, x in ((0, PAD), (1, PAD + width - 1)):
                xsend[side, p, c, pl.ds(i * height + z, 1), :] = field[p, z + 1, c * rows + i + 1, pl.ds(x, 1), :]

    def start_loads(c, carry):
        load(c)[0].start()
        return carry

    def start_others(c, carry):
        for copy in load(c)[1:]:
            copy.start()
        return carry

    barrier = pltpu.get_barrier_semaphore()
    greeted = [beside("lev", -1), beside("lev", 1), beside("lat", -1), beside("lat", 1)]
    greeted += [beside("lon", offset) for offset in range(1, counts["lon"])]
    for device in greeted:
        pl.semaphore_signal(barrier, inc=1, device_id=device, device_id_type=MESH)
    lax.fori_loop(0, chunks, start_loads, 0)

    def unpack(c):
        load(c)[0].wait()

        def row(i, carry):
            y = c * rows + i
            for z in range(height):
                field[0, z + 1, y + 1, inner, :] = raw[y, pl.ds(z, width, stride=height), :]
            pack(0, c, i)
            return carry

        lax.fori_loop(0, rows, row, 0)

    def unpack_send(c, carry):
        unpack(c)
        send(0, c)
        return carry

    unpack(0)
    pl.semaphore_wait(barrier, len(greeted))
    send(0, 0)
    lax.fori_loop(0, chunks, start_others, 0)
    lax.fori_loop(1, chunks, unpack_send, 0)

    def combine(c):
        for offset in range(1, counts["lon"]):
            stat_copy(offset, c).wait_recv()
        means = [stats[offset, c, 0] for offset in range(counts["lon"])]
        mean = sum(means[1:], means[0]) * (1.0 / counts["lon"])
        squares = sum([stats[offset, c, 1] for offset in range(1, counts["lon"])], stats[0, c, 1])
        apart = sum([(other - mean) * (other - mean) for other in means[1:]], (means[0] - mean) * (means[0] - mean))
        variance = (squares + width * apart) * (1.0 / (width * counts["lon"]))
        scale = lax.rsqrt(variance + 0.0001)
        for i in range(rows):
            for half in range(2):
                for kind, values in ((0, mean), (1, scale)):
                    moments_out[kind, c * rows + i, pl.ds(half * height, height), :] = values[i * height:(i + 1) * height]
        for offset in range(1, counts["lon"]):
            stat_copy(offset, c).wait_send()
        sent((STEPS - 1) % 2, c)

    def step(s, carry):
        p = lax.rem(s, 2)
        q = 1 - p

        def chunk(c, carry):
            @pl.when(s == 0)
            def _():
                for copy in load(c)[1:]:
                    copy.wait()

            @pl.when(s >= 1)
            def _():
                sent(q, c)

            arrived(p, c)

            def row(i, carry):
                y = c * rows + i
                for z in range(height):
                    for side, x in ((0, PAD - 1), (1, PAD + width)):
                        field[p, z + 1, y + 1, pl.ds(x, 1), :] = xrecv[side, p, c, pl.ds(i * height + z, 1), :]
                for x in range(0, width, XBLOCK):
                    here = pl.ds(PAD + x, XBLOCK)
                    planes = [field[p, z, y + 1, here, :] for z in range(height + 2)]
                    for z in range(height):
                        middle = planes[z + 1]
                        spread = (
                            field[p, z + 1, y, here, :] + field[p, z + 1, y + 2, here, :]
                            + field[p, z + 1, y + 1, pl.ds(PAD + x - 1, XBLOCK), :]
                            + field[p, z + 1, y + 1, pl.ds(PAD + x + 1, XBLOCK), :]
                            + planes[z] + planes[z + 2] - 6.0 * middle
                        )
                        cells = pl.ds(x * height + z, XBLOCK, stride=height)
                        field[q, z + 1, y + 1, here, :] = middle + ratio[y, cells, :] * spread + forcing[y, cells, :]
                pack(q, c, i)
                return carry

            lax.fori_loop(0, rows, row, 0)

            @pl.when(s < STEPS - 1)
            def _():
                send(q, c)

            @pl.when(s == STEPS - 1)
            def _():
                def finish(i, carry):
                    y = c * rows + i
                    for z in range(height):
                        line = field[q, z + 1, y + 1, inner, :]
                        raw[y, pl.ds(z, width, stride=height), :] = line
                        mean = jnp.sum(line, axis=0, keepdims=True) * (1.0 / width)
                        centred = line - mean
                        stats[0, c, 0, pl.ds(i * height + z, 1), :] = mean
                        stats[0, c, 1, pl.ds(i * height + z, 1), :] = jnp.sum(centred * centred, axis=0, keepdims=True)
                    return carry

                lax.fori_loop(0, rows, finish, 0)
                for offset in range(1, counts["lon"]):
                    stat_copy(offset, c).start()

                @pl.when(c >= 1)
                def _():
                    combine(c - 1)

            return carry

        lax.fori_loop(0, chunks, chunk, 0)
        return carry

    lax.fori_loop(0, STEPS, step, 0)


    combine(chunks - 1)


def swap_kernel(
    sizes, rows,
    heat_in, ratio_in, forcing_in, heat_out, moments_out,
    field, rim, core, ratio, ratio_far, forcing_far, back, stage,
    xsend, xrecv, csend, crecv, stats,
    load_sem, r_send, r_recv, u_send, u_recv, f_send, f_recv, b_send, b_recv,
    xsend_sem, xrecv_sem, ysend_sem, yrecv_sem, cxsend_sem, cxrecv_sem, cysend_sem, cyrecv_sem,
    stat_send, stat_recv,
):
    depth, width, height = sizes
    half, planes, inside = width // 2, 2 * height, height - 2
    chunks = depth // rows
    units = chunks // 2
    sent_at = height * half
    inner = pl.ds(PAD, half)
    forcing = heat_out
    places = {axis: lax.axis_index(axis) for axis in ("lat", "lon", "lev")}
    counts = {axis: lax.axis_size(axis) for axis in ("lat", "lon", "lev")}
    upper = places["lev"] == 1

    def beside(axis, offset):
        return {axis: lax.rem(places[axis] + offset + counts[axis], counts[axis])}

    def rows_of(c):
        return pl.ds(c * rows, rows)

    def chunk_of(u, side):
        return u + side * (chunks - 1 - 2 * u)

    def first_lanes(shape):
        return lax.broadcasted_iota(jnp.int32, shape, 1) < shape[1] // 2

    def turned(values):
        return pltpu.roll(values, values.shape[1] // 2, 1)

    def remote(source, target, send_sem, recv_sem, device):
        return pltpu.make_async_remote_copy(
            src_ref=source, dst_ref=target, send_sem=send_sem, recv_sem=recv_sem,
            device_id=device, device_id_type=MESH,
        )

    partner = beside("lev", 1)

    def load(kind, c, slot):
        source = (heat_in, ratio_in, forcing_in)[kind]
        return pltpu.make_async_copy(source.at[rows_of(c)], stage.at[kind, slot], load_sem.at[kind, slot])

    def ratio_copy(c):
        return remote(
            ratio.at[rows_of(c), pl.ds(sent_at, sent_at)], ratio_far.at[rows_of(c)], r_send.at[c], r_recv.at[c], partner
        )

    def forcing_copy(c):
        return remote(
            forcing.at[rows_of(c), pl.ds(sent_at, sent_at)], forcing_far.at[rows_of(c)], f_send.at[c], f_recv.at[c], partner
        )

    def rim_copy(end, c):
        return remote(
            rim.at[end, rows_of(c)], field.at[0, (height, planes - 1)[end], pl.ds(1 + c * rows, rows), inner],
            u_send.at[end, c], u_recv.at[end, c], partner,
        )

    def back_copy(c):
        return remote(
            field.at[STEPS % 2, pl.ds(height, height), pl.ds(1 + c * rows, rows), inner], back.at[:, rows_of(c)],
            b_send.at[c], b_recv.at[c], partner,
        )

    def xcopy(level, side, c):
        return remote(
            xsend.at[level, side, rows_of(c)], xrecv.at[level, 1 - side, rows_of(c)],
            xsend_sem.at[level, side, c], xrecv_sem.at[level, 1 - side, c], beside("lon", (-1, 1)[side]),
        )

    def ycopy(level, side):
        p = lax.rem(level, 2)
        return remote(
            field.at[p, :, (1, depth)[side], inner], field.at[p, :, (depth + 1, 0)[side], inner],
            ysend_sem.at[level, side], yrecv_sem.at[level, 1 - side], beside("lat", (-1, 1)[side]),
        )

    def core_xcopy(side, c):
        return remote(
            csend.at[side, rows_of(c)], crecv.at[1 - side, rows_of(c)],
            cxsend_sem.at[side, c], cxrecv_sem.at[1 - side, c], beside("lon", (-1, 1)[side]),
        )

    def core_ycopy(side):
        return remote(
            core.at[:, (1, depth)[side], inner], core.at[:, (depth + 1, 0)[side], inner],
            cysend_sem.at[side], cyrecv_sem.at[1 - side], beside("lat", (-1, 1)[side]),
        )

    def stat_copy(offset, c):
        return remote(
            stats.at[0, c], stats.at[offset, c], stat_send.at[offset - 1, c], stat_recv.at[offset - 1, c],
            beside("lon", offset),
        )

    def at_ends(c, action):
        for side, end in ((0, 0), (1, chunks - 1)):
            @pl.when(c == end)
            def _():
                action(side)

    def over(count, body):
        def step(i, carry):
            body(i)
            return carry

        lax.fori_loop(0, count, step, 0)


    def split(kind, slot, i, z, x):
        low = stage[kind, slot, i, pl.ds(x * height + z, XBLOCK, stride=height), :]
        high = stage[kind, slot, i, pl.ds((half + x) * height + z, XBLOCK, stride=height), :]
        mask = first_lanes(low.shape)
        one = jnp.where(mask, low, turned(high))
        two = jnp.where(mask, turned(low), high)
        return jnp.where(upper, two, one), jnp.where(upper, one, two)

    def split_into(target, kind, slot, c):
        def row(i):
            for z in range(height):
                for x in range(0, half, XBLOCK):
                    kept, sent = split(kind, slot, i, z, x)
                    target[c * rows + i, pl.ds(z * half + x, XBLOCK), :] = kept
                    target[c * rows + i, pl.ds(sent_at + z * half + x, XBLOCK), :] = sent

        over(rows, row)

    def split_heat(slot, c):
        def row(i):
            y = c * rows + i
            for z in range(height):
                for x in range(0, half, XBLOCK):
                    here = pl.ds(PAD + x, XBLOCK)
                    kept, sent = split(0, slot, i, z, x)
                    field[0, z, y + 1, here, :] = kept
                    if 0 < z < height - 1:
                        core[z - 1, y + 1, here, :] = sent
                        field[0, height + z, y + 1, here, :] = jnp.zeros_like(sent)
                    else:
                        rim[min(z, 1), y, pl.ds(x, XBLOCK), :] = sent
            for side, x in ((0, PAD), (1, PAD + half - 1)):
                csend[side, y] = jnp.zeros(csend.shape[2:], csend.dtype)
                for n in range(inside):
                    csend[side, y, pl.ds(n, 1), :] = core[n, y + 1, pl.ds(x, 1), :]

        over(rows, row)

    def prepare(u, side):
        c = chunk_of(u, side)
        load(1, c, side).wait()
        split_into(ratio, 1, side, c)

        @pl.when((u == 0) & (side == 0))
        def _():
            pl.semaphore_wait(barrier, len(greeted))

        ratio_copy(c).start()
        load(0, c, side).wait()
        split_heat(side, c)
        for end in (0, 1):
            rim_copy(end, c).start()
        for end in (0, 1):
            core_xcopy(end, c).start()
        at_ends(c, lambda end: core_ycopy(end).start())
        load(2, c, side).wait()
        split_into(forcing, 2, side, c)

        @pl.when(u < units - 1)
        def _():
            for kind in (1, 0, 2):
                load(kind, chunk_of(u + 1, side), side).start()

    def correct(u, side):
        c = chunk_of(u, side)
        at_ends(c, lambda end: core_ycopy(1 - end).wait_recv())
        for end in (0, 1):
            core_xcopy(end, c).wait_recv()

        def row(i):
            y = c * rows + i
            mask = first_lanes(crecv.shape[2:])
            left = turned(jnp.where(mask, csend[1, y], crecv[0, y]))
            right = turned(jnp.where(mask, crecv[1, y], csend[0, y]))
            for n in range(inside):
                core[n, y + 1, pl.ds(PAD - 1, 1), :] = left[n:n + 1]
                core[n, y + 1, pl.ds(PAD + half, 1), :] = right[n:n + 1]
            for x in range(0, half, XBLOCK):
                here = pl.ds(PAD + x, XBLOCK)
                middles = {n: core[n, y + 1, here, :] for n in range(inside)}
                for z in range(height):
                    parts = [middles[n] for n in (z - 2, z) if n in middles]
                    n = z - 1
                    if n in middles:
                        parts += [
                            core[n, y, here, :] + core[n, y + 2, here, :],
                            core[n, y + 1, pl.ds(PAD + x - 1, XBLOCK), :] + core[n, y + 1, pl.ds(PAD + x + 1, XBLOCK), :],
                            -6.0 * middles[n],
                        ]
                    cells = pl.ds(sent_at + z * half + x, XBLOCK)
                    forcing[y, cells, :] = forcing[y, cells, :] + ratio[y, cells, :] * sum(parts[1:], parts[0])

        over(rows, row)
        forcing_copy(c).start()

    barrier = pltpu.get_barrier_semaphore()
    greeted = [partner, beside("lat", -1), beside("lat", 1)]
    greeted += [beside("lon", offset) for offset in range(1, counts["lon"])]
    for device in greeted:
        pl.semaphore_signal(barrier, inc=1, device_id=device, device_id_type=MESH)
    for side in (0, 1):
        for kind in (1, 0, 2):
            load(kind, chunk_of(0, side), side).start()

    def inputs(u):
        @pl.when(u < units)
        def _():
            over(2, lambda side: prepare(u, side))

        @pl.when(u > 0)
        def _():
            over(2, lambda side: correct(u - 1, side))

    over(units + 1, inputs)


    def publish(level, c):
        p = lax.rem(level, 2)

        def row(i):
            y = c * rows + i
            for side, x in ((0, PAD), (1, PAD + half - 1)):
                for z in range(planes):
                    xsend[level, side, y, pl.ds(z, 1), :] = field[p, z, y + 1, pl.ds(x, 1), :]

        over(rows, row)
        for side in (0, 1):
            xcopy(level, side, c).start()
        at_ends(c, lambda side: ycopy(level, side).start())

    def arrive(u, side):
        c = chunk_of(u, side)
        ratio_copy(c).wait_recv()
        forcing_copy(c).wait_recv()
        for end in (0, 1):
            rim_copy(end, c).wait_recv()
        publish(0, c)

    def advance(s, u, side):
        c = chunk_of(u, side)
        level = s - 1
        p = lax.rem(level, 2)
        q = 1 - p
        at_ends(c, lambda end: ycopy(level, 1 - end).wait_recv())

        @pl.when(s >= 2)
        def _():
            at_ends(c, lambda end: ycopy(s - 2, end).wait_send())

        for end in (0, 1):
            xcopy(level, end, c).wait_recv()

        def row(i):
            y = c * rows + i
            mask = first_lanes(xrecv.shape[3:])
            left = turned(jnp.where(mask, xsend[level, 1, y], xrecv[level, 0, y]))
            right = turned(jnp.where(mask, xrecv[level, 1, y], xsend[level, 0, y]))
            for z in range(planes):
                field[p, z, y + 1, pl.ds(PAD - 1, 1), :] = left[z:z + 1]
                field[p, z, y + 1, pl.ds(PAD + half, 1), :] = right[z:z + 1]
            for x in range(0, half, XCELLS):
                here = pl.ds(PAD + x, XCELLS)
                middles = [field[p, z, y + 1, here, :] for z in range(planes)]
                for z in range(planes):
                    middle = middles[z]
                    spread = (
                        field[p, z, y, here, :] + field[p, z, y + 2, here, :]
                        + field[p, z, y + 1, pl.ds(PAD + x - 1, XCELLS), :]
                        + field[p, z, y + 1, pl.ds(PAD + x + 1, XCELLS), :]
                        + middles[z - 1] + middles[(z + 1) % planes]
                        - 6.0 * middle
                    )
                    if z < height:
                        cells = pl.ds(z * half + x, XCELLS)
                        scale, source = ratio[y, cells, :], forcing[y, cells, :]
                    else:
                        cells = pl.ds((z - height) * half + x, XCELLS)
                        scale, source = ratio_far[y, cells, :], forcing_far[y, cells, :]
                    field[q, z, y + 1, here, :] = middle + scale * spread + source

        over(rows, row)

        @pl.when(s < STEPS)
        def _():
            publish(s, c)

        @pl.when(s == STEPS)
        def _():
            back_copy(c).start()

    def wave(w):
        @pl.when(w < units)
        def _():
            over(2, lambda side: arrive(w, side))

        def step(i):
            u = w - 1 - i

            @pl.when((u >= 0) & (u < units))
            def _():
                over(2, lambda side: advance(i + 1, u, side))

        over(STEPS, step)

    over(units + STEPS, wave)


    def finish(c):
        back_copy(c).wait_recv()
        forcing_copy(c).wait_send()

        def row(i):
            y = c * rows + i
            for z in range(height):
                parts = []
                for x in range(0, half, XBLOCK):
                    here = pl.ds(PAD + x, XBLOCK)
                    kept, other = field[STEPS % 2, z, y + 1, here, :], back[z, y, pl.ds(x, XBLOCK), :]
                    if 0 < z < height - 1:
                        other = other + core[z - 1, y + 1, here, :]
                    mask = first_lanes(kept.shape)
                    one, two = jnp.where(upper, other, kept), jnp.where(upper, kept, other)
                    low = jnp.where(mask, one, turned(two))
                    high = jnp.where(mask, turned(one), two)
                    heat_out[y, pl.ds(x * height + z, XBLOCK, stride=height), :] = low
                    heat_out[y, pl.ds((half + x) * height + z, XBLOCK, stride=height), :] = high
                    parts += [low, high]
                line = jnp.concatenate(parts, axis=0)
                mean = jnp.sum(line, axis=0, keepdims=True) * (1.0 / width)
                centred = line - mean
                stats[0, c, 0, pl.ds(i * height + z, 1), :] = mean
                stats[0, c, 1, pl.ds(i * height + z, 1), :] = jnp.sum(centred * centred, axis=0, keepdims=True)

        over(rows, row)
        for offset in range(1, counts["lon"]):
            stat_copy(offset, c).start()

    def combine(c):
        for offset in range(1, counts["lon"]):
            stat_copy(offset, c).wait_recv()
        means = [stats[offset, c, 0] for offset in range(counts["lon"])]
        mean = sum(means[1:], means[0]) * (1.0 / counts["lon"])
        squares = sum([stats[offset, c, 1] for offset in range(1, counts["lon"])], stats[0, c, 1])
        apart = sum([(other - mean) * (other - mean) for other in means[1:]], (means[0] - mean) * (means[0] - mean))
        variance = (squares + width * apart) * (1.0 / (width * counts["lon"]))
        scale = lax.rsqrt(variance + 0.0001)
        for i in range(rows):
            for copy in range(2):
                for kind, values in ((0, mean), (1, scale)):
                    moments_out[kind, c * rows + i, pl.ds(copy * height, height), :] = values[i * height:(i + 1) * height]
        for offset in range(1, counts["lon"]):
            stat_copy(offset, c).wait_send()

    def ordered(i):
        return chunk_of(i // 2, lax.rem(i, 2))

    def ending(i):
        finish(ordered(i))

        @pl.when(i > 0)
        def _():
            combine(ordered(i - 1))

    over(chunks, ending)

    def drain(c):
        ratio_copy(c).wait_send()
        back_copy(c).wait_send()
        for side in (0, 1):
            rim_copy(side, c).wait_send()
            core_xcopy(side, c).wait_send()

        def level_sent(level):
            for side in (0, 1):
                xcopy(level, side, c).wait_send()

        over(STEPS, level_sent)

    over(chunks, drain)
    for side in (0, 1):
        core_ycopy(side).wait_send()
        ycopy(STEPS - 1, side).wait_send()
    combine(ordered(chunks - 1))


def swap(sizes, arrays):
    depth, width, height = sizes
    members = arrays[0].shape[-1]
    rows = 2
    chunks = depth // rows
    half = width // 2
    lon = lax.axis_size("lon")
    flat = (depth, width * height, members)
    f32 = jnp.float32
    dma = pltpu.SemaphoreType.DMA
    vmem = lambda *shape: pltpu.VMEM((*shape, members), f32)
    return pl.pallas_call(
        functools.partial(swap_kernel, sizes, rows),
        out_shape=(pltpu.VMEM(flat, f32), pltpu.VMEM((2, depth, 2 * height, members), f32)),
        in_specs=[pl.BlockSpec(memory_space=pl.ANY)] * 3,
        out_specs=(pl.BlockSpec(memory_space=pltpu.VMEM),) * 2,
        scratch_shapes=[
            vmem(2, 2 * height, depth + 2, half + 2 * PAD),
            vmem(2, depth, half),
            vmem(height - 2, depth + 2, half + 2 * PAD),
            vmem(depth, width * height),
            vmem(depth, half * height),
            vmem(depth, half * height),
            vmem(height, depth, half),
            vmem(3, 2, rows, width * height),
            vmem(STEPS, 2, depth, 2 * height), vmem(STEPS, 2, depth, 2 * height),
            vmem(2, depth, 8), vmem(2, depth, 8),
            vmem(lon, chunks, 2, rows * height),
            dma((3, 2)),
            dma((chunks,)), dma((chunks,)),
            dma((2, chunks)), dma((2, chunks)),
            dma((chunks,)), dma((chunks,)),
            dma((chunks,)), dma((chunks,)),
            dma((STEPS, 2, chunks)), dma((STEPS, 2, chunks)),
            dma((STEPS, 2)), dma((STEPS, 2)),
            dma((2, chunks)), dma((2, chunks)),
            dma((2,)), dma((2,)),
            dma((lon - 1, chunks)), dma((lon - 1, chunks)),
        ],
        compiler_params=pltpu.CompilerParams(
            collective_id=1, has_side_effects=True, vmem_limit_bytes=54 * 1024 * 1024
        ),
        name="swap",
    )(*arrays)


def march(sizes, arrays):
    depth, width, height = sizes
    members = arrays[0].shape[-1]
    rows = 2
    chunks = depth // rows
    lon = lax.axis_size("lon")
    flat = (depth, width * height, members)
    f32 = jnp.float32
    anywhere = pl.BlockSpec(memory_space=pl.ANY)
    dma = pltpu.SemaphoreType.DMA
    return pl.pallas_call(
        functools.partial(march_kernel, (depth, width, height), chunks, rows),
        out_shape=(pltpu.VMEM(flat, f32), pltpu.VMEM((2, depth, 2 * height, members), f32)),
        in_specs=[anywhere] * 3,
        out_specs=(pl.BlockSpec(memory_space=pltpu.VMEM),) * 2,
        scratch_shapes=[
            pltpu.VMEM((2, height + 2, depth + 2, width + 2 * PAD, members), f32),
            pltpu.VMEM(flat, f32),
            pltpu.VMEM(flat, f32),
            pltpu.VMEM((2, 2, chunks, rows * height, members), f32),
            pltpu.VMEM((2, 2, chunks, rows * height, members), f32),
            pltpu.VMEM((lon, chunks, 2, rows * height, members), f32),
            dma((chunks,)), dma((chunks,)), dma((chunks,)),
            dma((2, 2, chunks)), dma((2, 2, chunks)),
            dma((2, 2, chunks)), dma((2, 2, chunks)),
            dma((2, 2)), dma((2, 2)),
            dma((lon - 1, chunks)), dma((lon - 1, chunks)),
        ],
        compiler_params=pltpu.CompilerParams(
            collective_id=0, has_side_effects=True, vmem_limit_bytes=48 * 1024 * 1024
        ),
        name="march",
    )(*arrays)


def score_kernel(chunks, heat, moments, score, end, scaled, score_sem, end_sem):
    rows = heat.shape[0] // chunks
    finish = pltpu.make_async_copy(heat, end, end_sem)
    finish.start()

    def out_copy(c):
        span = pl.ds(c * rows, rows)
        return pltpu.make_async_copy(scaled.at[span], score.at[span], score_sem.at[c])

    def chunk(c, carry):
        def row(i, carry):
            y = c * rows + i
            mean, scale = moments[0, y], moments[1, y]
            values = heat[y]
            tall = values.reshape(values.shape[0] // mean.shape[0], *mean.shape)
            scaled[y] = ((tall - mean[None]) * scale[None]).reshape(values.shape)
            return carry

        lax.fori_loop(0, rows, row, 0)
        out_copy(c).start()
        return carry

    def drain(c, carry):
        out_copy(c).wait()
        return carry

    lax.fori_loop(0, chunks, chunk, 0)
    lax.fori_loop(0, chunks, drain, 0)
    finish.wait()


def local(initial_heat, diffusivity_ratio, forcing_term):
    depth, width, height, members = initial_heat.shape
    flat = (depth, width * height, members)
    f32 = jnp.float32
    anywhere = pl.BlockSpec(memory_space=pl.ANY)
    dma = pltpu.SemaphoreType.DMA
    arrays = [a.reshape(flat) for a in (initial_heat, diffusivity_ratio, forcing_term)]
    swaps = lax.axis_size("lev") == 2 and 3 <= height and 3 * height + 2 < 4 * STEPS
    swaps = swaps and depth % 4 == 0 and width % (2 * XBLOCK) == 0
    heat, moments = (swap if swaps else march)((depth, width, height), arrays)
    parts = min(8, depth)
    score, end = pl.pallas_call(
        functools.partial(score_kernel, parts),
        out_shape=(jax.ShapeDtypeStruct(flat, f32),) * 2,
        in_specs=[pl.BlockSpec(memory_space=pltpu.VMEM)] * 2,
        out_specs=(anywhere,) * 2,
        scratch_shapes=[pltpu.VMEM(flat, f32), dma((parts,)), dma(())],
        compiler_params=pltpu.CompilerParams(vmem_limit_bytes=24 * 1024 * 1024),
        name="score",
    )(heat, moments)
    return score.reshape(initial_heat.shape), end.reshape(initial_heat.shape)


def solution(mesh):
    placed = P("lat", "lon", "lev", None)
    return jax.shard_map(
        local, mesh=mesh, in_specs=(placed,) * 3, out_specs=(placed,) * 2, check_vma=False
    )
```

```python
import functools

import jax
import jax.numpy as jnp
from jax import lax
from jax.experimental import pallas as pl
from jax.experimental.pallas import tpu as pltpu
from jax.sharding import PartitionSpec as P

STEPS = 4
PAD = 8
XBLOCK = 32
XCELLS = 16
MESH = pl.DeviceIdType.MESH


def march_kernel(
    sizes, chunks, rows,
    heat_in, ratio_in, forcing_in, raw, moments_out,
    field, ratio, forcing, xsend, xrecv, stats,
    load_heat, load_ratio, load_forcing,
    zsend_sem, zrecv_sem, xsend_sem, xrecv_sem, ysend_sem, yrecv_sem, stat_send, stat_recv,
):
    depth, width, height = sizes
    inner = pl.ds(PAD, width)
    places = {axis: lax.axis_index(axis) for axis in ("lat", "lon", "lev")}
    counts = {axis: lax.axis_size(axis) for axis in ("lat", "lon", "lev")}

    def beside(axis, offset):
        return {axis: lax.rem(places[axis] + offset + counts[axis], counts[axis])}

    def rows_of(c):
        return pl.ds(c * rows, rows)

    def load(c):
        return [
            pltpu.make_async_copy(source.at[rows_of(c)], target.at[rows_of(c)], sem.at[c])
            for source, target, sem in (
                (heat_in, raw, load_heat), (ratio_in, ratio, load_ratio), (forcing_in, forcing, load_forcing),
            )
        ]

    def zcopy(side, p, c):
        span = pl.ds(1 + c * rows, rows)
        return pltpu.make_async_remote_copy(
            src_ref=field.at[p, (1, height)[side], span, inner],
            dst_ref=field.at[p, (height + 1, 0)[side], span, inner],
            send_sem=zsend_sem.at[side, p, c], recv_sem=zrecv_sem.at[1 - side, p, c],
            device_id=beside("lev", (-1, 1)[side]), device_id_type=MESH,
        )

    def xcopy(side, p, c):
        return pltpu.make_async_remote_copy(
            src_ref=xsend.at[side, p, c], dst_ref=xrecv.at[1 - side, p, c],
            send_sem=xsend_sem.at[side, p, c], recv_sem=xrecv_sem.at[1 - side, p, c],
            device_id=beside("lon", (-1, 1)[side]), device_id_type=MESH,
        )

    def ycopy(side, p):
        return pltpu.make_async_remote_copy(
            src_ref=field.at[p, pl.ds(1, height), (1, depth)[side], inner],
            dst_ref=field.at[p, pl.ds(1, height), (depth + 1, 0)[side], inner],
            send_sem=ysend_sem.at[side, p], recv_sem=yrecv_sem.at[1 - side, p],
            device_id=beside("lat", (-1, 1)[side]), device_id_type=MESH,
        )

    def stat_copy(offset, c):
        return pltpu.make_async_remote_copy(
            src_ref=stats.at[0, c], dst_ref=stats.at[offset, c],
            send_sem=stat_send.at[offset - 1, c], recv_sem=stat_recv.at[offset - 1, c],
            device_id=beside("lon", offset), device_id_type=MESH,
        )

    def send(p, c):
        for side, end in ((0, 0), (1, chunks - 1)):
            @pl.when(c == end)
            def _():
                ycopy(side, p).start()
        for side in (0, 1):
            zcopy(side, p, c).start()
        for side in (0, 1):
            xcopy(side, p, c).start()

    def sent(p, c):
        for side, end in ((0, 0), (1, chunks - 1)):
            @pl.when(c == end)
            def _():
                ycopy(side, p).wait_send()
        for side in (0, 1):
            zcopy(side, p, c).wait_send()
            xcopy(side, p, c).wait_send()

    def arrived(p, c):
        for side, end in ((1, 0), (0, chunks - 1)):
            @pl.when(c == end)
            def _():
                ycopy(side, p).wait_recv()
        for side in (0, 1):
            xcopy(side, p, c).wait_recv()
        for side in (0, 1):
            zcopy(side, p, c).wait_recv()

    def pack(p, c, i):
        for z in range(height):
            for side, x in ((0, PAD), (1, PAD + width - 1)):
                xsend[side, p, c, pl.ds(i * height + z, 1), :] = field[p, z + 1, c * rows + i + 1, pl.ds(x, 1), :]

    def start_loads(c, carry):
        load(c)[0].start()
        return carry

    def start_others(c, carry):
        for copy in load(c)[1:]:
            copy.start()
        return carry

    barrier = pltpu.get_barrier_semaphore()
    greeted = [beside("lev", -1), beside("lev", 1), beside("lat", -1), beside("lat", 1)]
    greeted += [beside("lon", offset) for offset in range(1, counts["lon"])]
    for device in greeted:
        pl.semaphore_signal(barrier, inc=1, device_id=device, device_id_type=MESH)
    lax.fori_loop(0, chunks, start_loads, 0)

    def unpack(c):
        load(c)[0].wait()

        def row(i, carry):
            y = c * rows + i
            for z in range(height):
                field[0, z + 1, y + 1, inner, :] = raw[y, pl.ds(z, width, stride=height), :]
            pack(0, c, i)
            return carry

        lax.fori_loop(0, rows, row, 0)

    def unpack_send(c, carry):
        unpack(c)
        send(0, c)
        return carry

    unpack(0)
    pl.semaphore_wait(barrier, len(greeted))
    send(0, 0)
    lax.fori_loop(0, chunks, start_others, 0)
    lax.fori_loop(1, chunks, unpack_send, 0)

    def combine(c):
        for offset in range(1, counts["lon"]):
            stat_copy(offset, c).wait_recv()
        means = [stats[offset, c, 0] for offset in range(counts["lon"])]
        mean = sum(means[1:], means[0]) * (1.0 / counts["lon"])
        squares = sum([stats[offset, c, 1] for offset in range(1, counts["lon"])], stats[0, c, 1])
        apart = sum([(other - mean) * (other - mean) for other in means[1:]], (means[0] - mean) * (means[0] - mean))
        variance = (squares + width * apart) * (1.0 / (width * counts["lon"]))
        scale = lax.rsqrt(variance + 0.0001)
        for i in range(rows):
            for half in range(2):
                for kind, values in ((0, mean), (1, scale)):
                    moments_out[kind, c * rows + i, pl.ds(half * height, height), :] = values[i * height:(i + 1) * height]
        for offset in range(1, counts["lon"]):
            stat_copy(offset, c).wait_send()
        sent((STEPS - 1) % 2, c)

    def step(s, carry):
        p = lax.rem(s, 2)
        q = 1 - p

        def chunk(c, carry):
            @pl.when(s == 0)
            def _():
                for copy in load(c)[1:]:
                    copy.wait()

            @pl.when(s >= 1)
            def _():
                sent(q, c)

            arrived(p, c)

            def row(i, carry):
                y = c * rows + i
                for z in range(height):
                    for side, x in ((0, PAD - 1), (1, PAD + width)):
                        field[p, z + 1, y + 1, pl.ds(x, 1), :] = xrecv[side, p, c, pl.ds(i * height + z, 1), :]
                for x in range(0, width, XBLOCK):
                    here = pl.ds(PAD + x, XBLOCK)
                    planes = [field[p, z, y + 1, here, :] for z in range(height + 2)]
                    for z in range(height):
                        middle = planes[z + 1]
                        spread = (
                            field[p, z + 1, y, here, :] + field[p, z + 1, y + 2, here, :]
                            + field[p, z + 1, y + 1, pl.ds(PAD + x - 1, XBLOCK), :]
                            + field[p, z + 1, y + 1, pl.ds(PAD + x + 1, XBLOCK), :]
                            + planes[z] + planes[z + 2] - 6.0 * middle
                        )
                        cells = pl.ds(x * height + z, XBLOCK, stride=height)
                        field[q, z + 1, y + 1, here, :] = middle + ratio[y, cells, :] * spread + forcing[y, cells, :]
                pack(q, c, i)
                return carry

            lax.fori_loop(0, rows, row, 0)

            @pl.when(s < STEPS - 1)
            def _():
                send(q, c)

            @pl.when(s == STEPS - 1)
            def _():
                def finish(i, carry):
                    y = c * rows + i
                    for z in range(height):
                        line = field[q, z + 1, y + 1, inner, :]
                        raw[y, pl.ds(z, width, stride=height), :] = line
                        mean = jnp.sum(line, axis=0, keepdims=True) * (1.0 / width)
                        centred = line - mean
                        stats[0, c, 0, pl.ds(i * height + z, 1), :] = mean
                        stats[0, c, 1, pl.ds(i * height + z, 1), :] = jnp.sum(centred * centred, axis=0, keepdims=True)
                    return carry

                lax.fori_loop(0, rows, finish, 0)
                for offset in range(1, counts["lon"]):
                    stat_copy(offset, c).start()

                @pl.when(c >= 1)
                def _():
                    combine(c - 1)

            return carry

        lax.fori_loop(0, chunks, chunk, 0)
        return carry

    lax.fori_loop(0, STEPS, step, 0)


    combine(chunks - 1)


def swap_kernel(
    sizes, rows,
    heat_in, ratio_in, forcing_in, heat_out, score_out,
    field, rim, core, ratio_far, forcing_far, back, stage,
    xsend, xrecv, csend, crecv, stats,
    load_sem, send_sem, ysend_sem, scale_recv, rim_recv, back_recv,
    xrecv_sem, yrecv_sem, cxrecv_sem, cyrecv_sem, stat_recv,
):
    depth, width, height = sizes
    half, planes, inside = width // 2, 2 * height, height - 2
    chunks = depth // rows
    units = chunks // 2
    sent_at = height * half
    inner = pl.ds(PAD, half)
    forcing, ratio = heat_out, score_out
    places = {axis: lax.axis_index(axis) for axis in ("lat", "lon", "lev")}
    counts = {axis: lax.axis_size(axis) for axis in ("lat", "lon", "lev")}
    upper = places["lev"] == 1

    def beside(axis, offset):
        return {axis: lax.rem(places[axis] + offset + counts[axis], counts[axis])}

    def rows_of(c):
        return pl.ds(c * rows, rows)

    def chunk_of(u, side):
        return u + side * (chunks - 1 - 2 * u)

    def first_lanes(shape):
        return lax.broadcasted_iota(jnp.int32, shape, 1) < shape[1] // 2

    def ordered(i):
        return chunk_of(i // 2, lax.rem(i, 2))

    def turned(values):
        return pltpu.roll(values, values.shape[1] // 2, 1)

    def remote(source, target, send_sem, recv_sem, device):
        return pltpu.make_async_remote_copy(
            src_ref=source, dst_ref=target, send_sem=send_sem, recv_sem=recv_sem,
            device_id=device, device_id_type=MESH,
        )

    partner = beside("lev", 1)

    def load(kind, c, slot):
        source = (heat_in, ratio_in, forcing_in)[kind]
        return pltpu.make_async_copy(source.at[rows_of(c)], stage.at[kind, slot], load_sem.at[kind, slot])

    def ratio_copy(u, span):
        cells = pl.ds(sent_at, sent_at)
        return remote(ratio.at[span, cells], ratio_far.at[span], send_sem.at[0], scale_recv.at[u], partner)

    def forcing_copy(u, span):
        cells = pl.ds(sent_at, sent_at)
        return remote(forcing.at[span, cells], forcing_far.at[span], send_sem.at[1], scale_recv.at[u], partner)

    def rim_copy(end, u, c):
        return remote(
            rim.at[end, rows_of(c)], field.at[0, (height, planes - 1)[end], pl.ds(1 + c * rows, rows), inner],
            send_sem.at[2], rim_recv.at[u], partner,
        )

    def back_copy(c):
        return remote(
            field.at[STEPS % 2, pl.ds(height, height), pl.ds(1 + c * rows, rows), inner], back.at[:, rows_of(c)],
            send_sem.at[3], back_recv.at[c], partner,
        )

    def xcopy(level, side, u):
        return remote(
            xsend.at[level, u, side], xrecv.at[level, u, 1 - side],
            send_sem.at[4], xrecv_sem.at[lax.rem(level, 2), u], beside("lon", (-1, 1)[side]),
        )

    def ycopy(level, side):
        p = lax.rem(level, 2)
        return remote(
            field.at[p, :, (1, depth)[side], inner], field.at[p, :, (depth + 1, 0)[side], inner],
            ysend_sem.at[p], yrecv_sem.at[p], beside("lat", (-1, 1)[side]),
        )

    def core_xcopy(side, u):
        return remote(
            csend.at[u, side], crecv.at[u, 1 - side], send_sem.at[5], cxrecv_sem.at[u], beside("lon", (-1, 1)[side])
        )

    def core_ycopy(side):
        return remote(
            core.at[:, (1, depth)[side], inner], core.at[:, (depth + 1, 0)[side], inner],
            send_sem.at[6], cyrecv_sem.at[0], beside("lat", (-1, 1)[side]),
        )

    def stat_copy(offset, i):
        c = ordered(i)
        return remote(
            stats.at[0, c], stats.at[offset, c], send_sem.at[7], stat_recv.at[lax.rem(i, 4)], beside("lon", offset)
        )

    def wait_all(ref, sem):
        pltpu.make_async_copy(ref, ref, sem).wait()

    def over(count, body):
        def step(i, carry):
            body(i)
            return carry

        lax.fori_loop(0, count, step, 0)


    def split(kind, slot, i, z, x):
        low = stage[kind, slot, i, pl.ds(x * height + z, XBLOCK, stride=height), :]
        high = stage[kind, slot, i, pl.ds((half + x) * height + z, XBLOCK, stride=height), :]
        mask = first_lanes(low.shape)
        one = jnp.where(mask, low, turned(high))
        two = jnp.where(mask, turned(low), high)
        return jnp.where(upper, two, one), jnp.where(upper, one, two)

    def split_into(target, kind, slot, c):
        def row(i):
            for z in range(height):
                for x in range(0, half, XBLOCK):
                    kept, sent = split(kind, slot, i, z, x)
                    target[c * rows + i, pl.ds(z * half + x, XBLOCK), :] = kept
                    target[c * rows + i, pl.ds(sent_at + z * half + x, XBLOCK), :] = sent

        over(rows, row)

    def split_heat(u, slot, c):
        def row(i):
            y = c * rows + i
            for z in range(height):
                for x in range(0, half, XBLOCK):
                    here = pl.ds(PAD + x, XBLOCK)
                    kept, sent = split(0, slot, i, z, x)
                    field[0, z, y + 1, here, :] = kept
                    if 0 < z < height - 1:
                        core[z - 1, y + 1, here, :] = sent
                        field[0, height + z, y + 1, here, :] = jnp.zeros_like(sent)
                    else:
                        rim[min(z, 1), y, pl.ds(x, XBLOCK), :] = sent
            for side, x in ((0, PAD), (1, PAD + half - 1)):
                csend[u, side, slot * rows + i] = jnp.zeros(csend.shape[3:], csend.dtype)
                for n in range(inside):
                    csend[u, side, slot * rows + i, pl.ds(n, 1), :] = core[n, y + 1, pl.ds(x, 1), :]

        over(rows, row)

    def prepare(u, side):
        c = chunk_of(u, side)
        load(1, c, side).wait()
        split_into(ratio, 1, side, c)

        @pl.when((u == 0) & (side == 0))
        def _():
            pl.semaphore_wait(barrier, len(greeted))

        ratio_copy(u, rows_of(c)).start()
        load(0, c, side).wait()
        split_heat(u, side, c)
        for end in (0, 1):
            rim_copy(end, u, c).start()

        @pl.when(side == 1)
        def _():
            for end in (0, 1):
                core_xcopy(end, u).start()

        @pl.when((side == 1) & (u == 0))
        def _():
            for end in (0, 1):
                core_ycopy(end).start()

        load(2, c, side).wait()
        split_into(forcing, 2, side, c)

        @pl.when(u < units - 1)
        def _():
            for kind in (1, 0, 2):
                load(kind, chunk_of(u + 1, side), side).start()

    def correct(u, side):
        c = chunk_of(u, side)

        @pl.when(side == 0)
        def _():
            wait_all(crecv.at[u], cxrecv_sem.at[u])

        @pl.when((side == 0) & (u == 0))
        def _():
            wait_all(core.at[:, pl.ds(0, 2), inner], cyrecv_sem.at[0])

        def row(i):
            y = c * rows + i
            k = side * rows + i
            mask = first_lanes(crecv.shape[3:])
            left = turned(jnp.where(mask, csend[u, 1, k], crecv[u, 0, k]))
            right = turned(jnp.where(mask, crecv[u, 1, k], csend[u, 0, k]))
            for n in range(inside):
                core[n, y + 1, pl.ds(PAD - 1, 1), :] = left[n:n + 1]
                core[n, y + 1, pl.ds(PAD + half, 1), :] = right[n:n + 1]
            for x in range(0, half, XBLOCK):
                here = pl.ds(PAD + x, XBLOCK)
                middles = {n: core[n, y + 1, here, :] for n in range(inside)}
                for z in range(height):
                    parts = [middles[n] for n in (z - 2, z) if n in middles]
                    n = z - 1
                    if n in middles:
                        parts += [
                            core[n, y, here, :] + core[n, y + 2, here, :],
                            core[n, y + 1, pl.ds(PAD + x - 1, XBLOCK), :] + core[n, y + 1, pl.ds(PAD + x + 1, XBLOCK), :],
                            -6.0 * middles[n],
                        ]
                    cells = pl.ds(sent_at + z * half + x, XBLOCK)
                    forcing[y, cells, :] = forcing[y, cells, :] + ratio[y, cells, :] * sum(parts[1:], parts[0])

        over(rows, row)
        forcing_copy(u, rows_of(c)).start()

    barrier = pltpu.get_barrier_semaphore()
    greeted = [partner, beside("lat", -1), beside("lat", 1)]
    greeted += [beside("lon", offset) for offset in range(1, counts["lon"])]
    for device in greeted:
        pl.semaphore_signal(barrier, inc=1, device_id=device, device_id_type=MESH)
    for side in (0, 1):
        for kind in (1, 0, 2):
            load(kind, chunk_of(0, side), side).start()

    def inputs(u):
        @pl.when(u < units)
        def _():
            over(2, lambda side: prepare(u, side))

        @pl.when(u > 0)
        def _():
            over(2, lambda side: correct(u - 1, side))

    over(units + 1, inputs)


    def publish(level, u):
        p = lax.rem(level, 2)

        def row(k):
            y = chunk_of(u, k // rows) * rows + lax.rem(k, rows)
            for side, x in ((0, PAD), (1, PAD + half - 1)):
                for z in range(planes):
                    xsend[level, u, side, k, pl.ds(z, 1), :] = field[p, z, y + 1, pl.ds(x, 1), :]

        over(2 * rows, row)
        for side in (0, 1):
            xcopy(level, side, u).start()

        @pl.when(u == 0)
        def _():
            for side in (0, 1):
                ycopy(level, side).start()

    def arrive(u):
        wait_all(ratio_far.at[pl.ds(0, 4 * rows)], scale_recv.at[u])
        wait_all(rim.at[:, pl.ds(0, 2 * rows)], rim_recv.at[u])
        publish(0, u)

    def advance(s, u):
        level = s - 1
        p = lax.rem(level, 2)
        q = 1 - p

        @pl.when(u == 0)
        def _():
            wait_all(field.at[p, :, pl.ds(0, 2), inner], yrecv_sem.at[p])

        @pl.when((u == 0) & (s >= 2))
        def _():
            wait_all(field.at[q, :, pl.ds(0, 2), inner], ysend_sem.at[q])

        wait_all(xrecv.at[level, u], xrecv_sem.at[p, u])
        over(2, lambda side: march_rows(level, p, q, u, side))

        @pl.when(s < STEPS)
        def _():
            publish(s, u)

        @pl.when(s == STEPS)
        def _():
            for side in (0, 1):
                back_copy(chunk_of(u, side)).start()

    def march_rows(level, p, q, u, side):
        c = chunk_of(u, side)

        def row(i):
            y = c * rows + i
            k = side * rows + i
            mask = first_lanes(xrecv.shape[4:])
            left = turned(jnp.where(mask, xsend[level, u, 1, k], xrecv[level, u, 0, k]))
            right = turned(jnp.where(mask, xrecv[level, u, 1, k], xsend[level, u, 0, k]))
            for z in range(planes):
                field[p, z, y + 1, pl.ds(PAD - 1, 1), :] = left[z:z + 1]
                field[p, z, y + 1, pl.ds(PAD + half, 1), :] = right[z:z + 1]
            for x in range(0, half, XCELLS):
                here = pl.ds(PAD + x, XCELLS)
                middles = [field[p, z, y + 1, here, :] for z in range(planes)]
                for z in range(planes):
                    middle = middles[z]
                    spread = (
                        field[p, z, y, here, :] + field[p, z, y + 2, here, :]
                        + field[p, z, y + 1, pl.ds(PAD + x - 1, XCELLS), :]
                        + field[p, z, y + 1, pl.ds(PAD + x + 1, XCELLS), :]
                        + middles[z - 1] + middles[(z + 1) % planes]
                        - 6.0 * middle
                    )
                    if z < height:
                        cells = pl.ds(z * half + x, XCELLS)
                        scale, source = ratio[y, cells, :], forcing[y, cells, :]
                    else:
                        cells = pl.ds((z - height) * half + x, XCELLS)
                        scale, source = ratio_far[y, cells, :], forcing_far[y, cells, :]
                    field[q, z, y + 1, here, :] = middle + scale * spread + source

        over(rows, row)

    def wave(w):
        @pl.when(w < units)
        def _():
            arrive(w)

        def step(i):
            u = w - 1 - i

            @pl.when((u >= 0) & (u < units))
            def _():
                advance(i + 1, u)

        over(STEPS, step)

    over(units + STEPS, wave)


    def finish(position):
        c = ordered(position)
        back_copy(c).wait_recv()

        def row(i):
            y = c * rows + i
            for z in range(height):
                parts = []
                for x in range(0, half, XBLOCK):
                    here = pl.ds(PAD + x, XBLOCK)
                    kept, other = field[STEPS % 2, z, y + 1, here, :], back[z, y, pl.ds(x, XBLOCK), :]
                    if 0 < z < height - 1:
                        other = other + core[z - 1, y + 1, here, :]
                    mask = first_lanes(kept.shape)
                    one, two = jnp.where(upper, other, kept), jnp.where(upper, kept, other)
                    low = jnp.where(mask, one, turned(two))
                    high = jnp.where(mask, turned(one), two)
                    heat_out[y, pl.ds(x * height + z, XBLOCK, stride=height), :] = low
                    heat_out[y, pl.ds((half + x) * height + z, XBLOCK, stride=height), :] = high
                    parts += [low, high]
                line = jnp.concatenate(parts, axis=0)
                mean = jnp.sum(line, axis=0, keepdims=True) * (1.0 / width)
                centred = line - mean
                stats[0, c, 0, pl.ds(i * height + z, 1), :] = mean
                stats[0, c, 1, pl.ds(i * height + z, 1), :] = jnp.sum(centred * centred, axis=0, keepdims=True)

        over(rows, row)
        for offset in range(1, counts["lon"]):
            stat_copy(offset, position).start()

    def combine(position):
        c = ordered(position)
        wait_all(stats.at[pl.ds(1, counts["lon"] - 1), c], stat_recv.at[lax.rem(position, 4)])
        means = [stats[offset, c, 0] for offset in range(counts["lon"])]
        mean = sum(means[1:], means[0]) * (1.0 / counts["lon"])
        squares = sum([stats[offset, c, 1] for offset in range(1, counts["lon"])], stats[0, c, 1])
        apart = sum([(other - mean) * (other - mean) for other in means[1:]], (means[0] - mean) * (means[0] - mean))
        variance = (squares + width * apart) * (1.0 / (width * counts["lon"]))
        scale = lax.rsqrt(variance + 0.0001)
        for i in range(rows):
            y = c * rows + i
            lines = slice(i * height, (i + 1) * height)
            pair_mean = jnp.concatenate([mean[lines]] * 2, axis=0)[None]
            pair_scale = jnp.concatenate([scale[lines]] * 2, axis=0)[None]
            values = heat_out[y]
            tall = values.reshape(half, 2 * height, values.shape[1])
            score_out[y] = ((tall - pair_mean) * pair_scale).reshape(values.shape)

    wait_all(ratio.at[:, pl.ds(sent_at, sent_at)], send_sem.at[0])
    wait_all(forcing.at[:, pl.ds(sent_at, sent_at)], send_sem.at[1])

    def ending(i):
        finish(i)

        @pl.when(i > 0)
        def _():
            combine(i - 1)

    over(chunks, ending)
    wait_all(rim, send_sem.at[2])
    wait_all(field.at[STEPS % 2, pl.ds(height, height), pl.ds(1, depth), inner], send_sem.at[3])
    wait_all(xsend, send_sem.at[4])
    wait_all(csend, send_sem.at[5])
    wait_all(core.at[:, pl.ds(0, 2), inner], send_sem.at[6])
    wait_all(field.at[(STEPS - 1) % 2, :, pl.ds(0, 2), inner], ysend_sem.at[(STEPS - 1) % 2])
    wait_all(stats.at[pl.ds(1, counts["lon"] - 1)], send_sem.at[7])
    combine(chunks - 1)


def swap(sizes, arrays):
    depth, width, height = sizes
    members = arrays[0].shape[-1]
    rows = 2
    chunks = depth // rows
    units = chunks // 2
    half = width // 2
    lon = lax.axis_size("lon")
    flat = (depth, width * height, members)
    f32 = jnp.float32
    dma = pltpu.SemaphoreType.DMA
    vmem = lambda *shape: pltpu.VMEM((*shape, members), f32)
    return pl.pallas_call(
        functools.partial(swap_kernel, sizes, rows),
        out_shape=(pltpu.VMEM(flat, f32),) * 2,
        in_specs=[pl.BlockSpec(memory_space=pl.ANY)] * 3,
        out_specs=(pl.BlockSpec(memory_space=pltpu.VMEM),) * 2,
        scratch_shapes=[
            vmem(2, 2 * height, depth + 2, half + 2 * PAD),
            vmem(2, depth, half),
            vmem(height - 2, depth + 2, half + 2 * PAD),
            vmem(depth, half * height),
            vmem(depth, half * height),
            vmem(height, depth, half),
            vmem(3, 2, rows, width * height),
            vmem(STEPS, units, 2, 2 * rows, 2 * height), vmem(STEPS, units, 2, 2 * rows, 2 * height),
            vmem(units, 2, 2 * rows, 8), vmem(units, 2, 2 * rows, 8),
            vmem(lon, chunks, 2, rows * height),
            dma((3, 2)), dma((8,)), dma((2,)),
            dma((units,)), dma((units,)), dma((chunks,)),
            dma((2, units)), dma((2,)), dma((units,)), dma((1,)), dma((4,)),
        ],
        compiler_params=pltpu.CompilerParams(
            collective_id=1, has_side_effects=True, vmem_limit_bytes=47 * 1024 * 1024
        ),
        name="swap",
    )(*arrays)


def march(sizes, arrays):
    depth, width, height = sizes
    members = arrays[0].shape[-1]
    rows = 2
    chunks = depth // rows
    lon = lax.axis_size("lon")
    flat = (depth, width * height, members)
    f32 = jnp.float32
    anywhere = pl.BlockSpec(memory_space=pl.ANY)
    dma = pltpu.SemaphoreType.DMA
    return pl.pallas_call(
        functools.partial(march_kernel, (depth, width, height), chunks, rows),
        out_shape=(pltpu.VMEM(flat, f32), pltpu.VMEM((2, depth, 2 * height, members), f32)),
        in_specs=[anywhere] * 3,
        out_specs=(pl.BlockSpec(memory_space=pltpu.VMEM),) * 2,
        scratch_shapes=[
            pltpu.VMEM((2, height + 2, depth + 2, width + 2 * PAD, members), f32),
            pltpu.VMEM(flat, f32),
            pltpu.VMEM(flat, f32),
            pltpu.VMEM((2, 2, chunks, rows * height, members), f32),
            pltpu.VMEM((2, 2, chunks, rows * height, members), f32),
            pltpu.VMEM((lon, chunks, 2, rows * height, members), f32),
            dma((chunks,)), dma((chunks,)), dma((chunks,)),
            dma((2, 2, chunks)), dma((2, 2, chunks)),
            dma((2, 2, chunks)), dma((2, 2, chunks)),
            dma((2, 2)), dma((2, 2)),
            dma((lon - 1, chunks)), dma((lon - 1, chunks)),
        ],
        compiler_params=pltpu.CompilerParams(
            collective_id=0, has_side_effects=True, vmem_limit_bytes=48 * 1024 * 1024
        ),
        name="march",
    )(*arrays)


def copy_kernel(chunks, heat, scored, score, end, sem):
    rows = heat.shape[0] // chunks
    copies = []
    for c in range(chunks):
        span = pl.ds(c * rows, rows)
        copies.append(pltpu.make_async_copy(heat.at[span], end.at[span], sem.at[0, c]))
        copies.append(pltpu.make_async_copy(scored.at[span], score.at[span], sem.at[1, c]))
    for copy in copies:
        copy.start()
    for copy in copies:
        copy.wait()


def score_kernel(chunks, heat, moments, score, end, scaled, score_sem, end_sem):
    rows = heat.shape[0] // chunks
    finish = pltpu.make_async_copy(heat, end, end_sem)
    finish.start()

    def out_copy(c):
        span = pl.ds(c * rows, rows)
        return pltpu.make_async_copy(scaled.at[span], score.at[span], score_sem.at[c])

    def chunk(c, carry):
        def row(i, carry):
            y = c * rows + i
            mean, scale = moments[0, y], moments[1, y]
            values = heat[y]
            tall = values.reshape(values.shape[0] // mean.shape[0], *mean.shape)
            scaled[y] = ((tall - mean[None]) * scale[None]).reshape(values.shape)
            return carry

        lax.fori_loop(0, rows, row, 0)
        out_copy(c).start()
        return carry

    def drain(c, carry):
        out_copy(c).wait()
        return carry

    lax.fori_loop(0, chunks, chunk, 0)
    lax.fori_loop(0, chunks, drain, 0)
    finish.wait()


def local(initial_heat, diffusivity_ratio, forcing_term):
    depth, width, height, members = initial_heat.shape
    flat = (depth, width * height, members)
    f32 = jnp.float32
    anywhere = pl.BlockSpec(memory_space=pl.ANY)
    dma = pltpu.SemaphoreType.DMA
    arrays = [a.reshape(flat) for a in (initial_heat, diffusivity_ratio, forcing_term)]
    swaps = lax.axis_size("lev") == 2 and 3 <= height and 3 * height + 2 < 4 * STEPS
    swaps = swaps and depth % 4 == 0 and width % (2 * XBLOCK) == 0
    sizes = (depth, width, height)
    common = dict(out_shape=(jax.ShapeDtypeStruct(flat, f32),) * 2, out_specs=(anywhere,) * 2)
    inputs = [pl.BlockSpec(memory_space=pltpu.VMEM)] * 2
    if swaps:
        parts = min(4, depth)
        score, end = pl.pallas_call(
            functools.partial(copy_kernel, parts), **common, in_specs=inputs,
            scratch_shapes=[dma((2, parts))],
            compiler_params=pltpu.CompilerParams(vmem_limit_bytes=8 * 1024 * 1024),
            name="emit",
        )(*swap(sizes, arrays))
    else:
        parts = min(8, depth)
        score, end = pl.pallas_call(
            functools.partial(score_kernel, parts), **common, in_specs=inputs,
            scratch_shapes=[pltpu.VMEM(flat, f32), dma((parts,)), dma(())],
            compiler_params=pltpu.CompilerParams(vmem_limit_bytes=24 * 1024 * 1024),
            name="score",
        )(*march(sizes, arrays))
    return score.reshape(initial_heat.shape), end.reshape(initial_heat.shape)


def solution(mesh):
    placed = P("lat", "lon", "lev", None)
    return jax.shard_map(
        local, mesh=mesh, in_specs=(placed,) * 3, out_specs=(placed,) * 2, check_vma=False
    )
```

```python
import functools

import jax
import jax.numpy as jnp
from jax import lax
from jax.experimental import pallas as pl
from jax.experimental.pallas import tpu as pltpu
from jax.sharding import PartitionSpec as P

STEPS = 4
PAD = 8
XBLOCK = 32
XCELLS = 16
MESH = pl.DeviceIdType.MESH


def march_kernel(
    sizes, chunks, rows,
    heat_in, ratio_in, forcing_in, raw, moments_out,
    field, ratio, forcing, xsend, xrecv, stats,
    load_heat, load_ratio, load_forcing,
    zsend_sem, zrecv_sem, xsend_sem, xrecv_sem, ysend_sem, yrecv_sem, stat_send, stat_recv,
):
    depth, width, height = sizes
    inner = pl.ds(PAD, width)
    places = {axis: lax.axis_index(axis) for axis in ("lat", "lon", "lev")}
    counts = {axis: lax.axis_size(axis) for axis in ("lat", "lon", "lev")}

    def beside(axis, offset):
        return {axis: lax.rem(places[axis] + offset + counts[axis], counts[axis])}

    def rows_of(c):
        return pl.ds(c * rows, rows)

    def load(c):
        return [
            pltpu.make_async_copy(source.at[rows_of(c)], target.at[rows_of(c)], sem.at[c])
            for source, target, sem in (
                (heat_in, raw, load_heat), (ratio_in, ratio, load_ratio), (forcing_in, forcing, load_forcing),
            )
        ]

    def zcopy(side, p, c):
        span = pl.ds(1 + c * rows, rows)
        return pltpu.make_async_remote_copy(
            src_ref=field.at[p, (1, height)[side], span, inner],
            dst_ref=field.at[p, (height + 1, 0)[side], span, inner],
            send_sem=zsend_sem.at[side, p, c], recv_sem=zrecv_sem.at[1 - side, p, c],
            device_id=beside("lev", (-1, 1)[side]), device_id_type=MESH,
        )

    def xcopy(side, p, c):
        return pltpu.make_async_remote_copy(
            src_ref=xsend.at[side, p, c], dst_ref=xrecv.at[1 - side, p, c],
            send_sem=xsend_sem.at[side, p, c], recv_sem=xrecv_sem.at[1 - side, p, c],
            device_id=beside("lon", (-1, 1)[side]), device_id_type=MESH,
        )

    def ycopy(side, p):
        return pltpu.make_async_remote_copy(
            src_ref=field.at[p, pl.ds(1, height), (1, depth)[side], inner],
            dst_ref=field.at[p, pl.ds(1, height), (depth + 1, 0)[side], inner],
            send_sem=ysend_sem.at[side, p], recv_sem=yrecv_sem.at[1 - side, p],
            device_id=beside("lat", (-1, 1)[side]), device_id_type=MESH,
        )

    def stat_copy(offset, c):
        return pltpu.make_async_remote_copy(
            src_ref=stats.at[0, c], dst_ref=stats.at[offset, c],
            send_sem=stat_send.at[offset - 1, c], recv_sem=stat_recv.at[offset - 1, c],
            device_id=beside("lon", offset), device_id_type=MESH,
        )

    def send(p, c):
        for side, end in ((0, 0), (1, chunks - 1)):
            @pl.when(c == end)
            def _():
                ycopy(side, p).start()
        for side in (0, 1):
            zcopy(side, p, c).start()
        for side in (0, 1):
            xcopy(side, p, c).start()

    def sent(p, c):
        for side, end in ((0, 0), (1, chunks - 1)):
            @pl.when(c == end)
            def _():
                ycopy(side, p).wait_send()
        for side in (0, 1):
            zcopy(side, p, c).wait_send()
            xcopy(side, p, c).wait_send()

    def arrived(p, c):
        for side, end in ((1, 0), (0, chunks - 1)):
            @pl.when(c == end)
            def _():
                ycopy(side, p).wait_recv()
        for side in (0, 1):
            xcopy(side, p, c).wait_recv()
        for side in (0, 1):
            zcopy(side, p, c).wait_recv()

    def pack(p, c, i):
        for z in range(height):
            for side, x in ((0, PAD), (1, PAD + width - 1)):
                xsend[side, p, c, pl.ds(i * height + z, 1), :] = field[p, z + 1, c * rows + i + 1, pl.ds(x, 1), :]

    def start_loads(c, carry):
        load(c)[0].start()
        return carry

    def start_others(c, carry):
        for copy in load(c)[1:]:
            copy.start()
        return carry

    barrier = pltpu.get_barrier_semaphore()
    greeted = [beside("lev", -1), beside("lev", 1), beside("lat", -1), beside("lat", 1)]
    greeted += [beside("lon", offset) for offset in range(1, counts["lon"])]
    for device in greeted:
        pl.semaphore_signal(barrier, inc=1, device_id=device, device_id_type=MESH)
    lax.fori_loop(0, chunks, start_loads, 0)

    def unpack(c):
        load(c)[0].wait()

        def row(i, carry):
            y = c * rows + i
            for z in range(height):
                field[0, z + 1, y + 1, inner, :] = raw[y, pl.ds(z, width, stride=height), :]
            pack(0, c, i)
            return carry

        lax.fori_loop(0, rows, row, 0)

    def unpack_send(c, carry):
        unpack(c)
        send(0, c)
        return carry

    unpack(0)
    pl.semaphore_wait(barrier, len(greeted))
    send(0, 0)
    lax.fori_loop(0, chunks, start_others, 0)
    lax.fori_loop(1, chunks, unpack_send, 0)

    def combine(c):
        for offset in range(1, counts["lon"]):
            stat_copy(offset, c).wait_recv()
        means = [stats[offset, c, 0] for offset in range(counts["lon"])]
        mean = sum(means[1:], means[0]) * (1.0 / counts["lon"])
        squares = sum([stats[offset, c, 1] for offset in range(1, counts["lon"])], stats[0, c, 1])
        apart = sum([(other - mean) * (other - mean) for other in means[1:]], (means[0] - mean) * (means[0] - mean))
        variance = (squares + width * apart) * (1.0 / (width * counts["lon"]))
        scale = lax.rsqrt(variance + 0.0001)
        for i in range(rows):
            for half in range(2):
                for kind, values in ((0, mean), (1, scale)):
                    moments_out[kind, c * rows + i, pl.ds(half * height, height), :] = values[i * height:(i + 1) * height]
        for offset in range(1, counts["lon"]):
            stat_copy(offset, c).wait_send()
        sent((STEPS - 1) % 2, c)

    def step(s, carry):
        p = lax.rem(s, 2)
        q = 1 - p

        def chunk(c, carry):
            @pl.when(s == 0)
            def _():
                for copy in load(c)[1:]:
                    copy.wait()

            @pl.when(s >= 1)
            def _():
                sent(q, c)

            arrived(p, c)

            def row(i, carry):
                y = c * rows + i
                for z in range(height):
                    for side, x in ((0, PAD - 1), (1, PAD + width)):
                        field[p, z + 1, y + 1, pl.ds(x, 1), :] = xrecv[side, p, c, pl.ds(i * height + z, 1), :]
                for x in range(0, width, XBLOCK):
                    here = pl.ds(PAD + x, XBLOCK)
                    planes = [field[p, z, y + 1, here, :] for z in range(height + 2)]
                    for z in range(height):
                        middle = planes[z + 1]
                        spread = (
                            field[p, z + 1, y, here, :] + field[p, z + 1, y + 2, here, :]
                            + field[p, z + 1, y + 1, pl.ds(PAD + x - 1, XBLOCK), :]
                            + field[p, z + 1, y + 1, pl.ds(PAD + x + 1, XBLOCK), :]
                            + planes[z] + planes[z + 2] - 6.0 * middle
                        )
                        cells = pl.ds(x * height + z, XBLOCK, stride=height)
                        field[q, z + 1, y + 1, here, :] = middle + ratio[y, cells, :] * spread + forcing[y, cells, :]
                pack(q, c, i)
                return carry

            lax.fori_loop(0, rows, row, 0)

            @pl.when(s < STEPS - 1)
            def _():
                send(q, c)

            @pl.when(s == STEPS - 1)
            def _():
                def finish(i, carry):
                    y = c * rows + i
                    for z in range(height):
                        line = field[q, z + 1, y + 1, inner, :]
                        raw[y, pl.ds(z, width, stride=height), :] = line
                        mean = jnp.sum(line, axis=0, keepdims=True) * (1.0 / width)
                        centred = line - mean
                        stats[0, c, 0, pl.ds(i * height + z, 1), :] = mean
                        stats[0, c, 1, pl.ds(i * height + z, 1), :] = jnp.sum(centred * centred, axis=0, keepdims=True)
                    return carry

                lax.fori_loop(0, rows, finish, 0)
                for offset in range(1, counts["lon"]):
                    stat_copy(offset, c).start()

                @pl.when(c >= 1)
                def _():
                    combine(c - 1)

            return carry

        lax.fori_loop(0, chunks, chunk, 0)
        return carry

    lax.fori_loop(0, STEPS, step, 0)


    combine(chunks - 1)


def swap_kernel(
    sizes, rows,
    heat_in, ratio_in, forcing_in, heat_out, score_out,
    field, rim, core, ratio_far, forcing_far, back, stage,
    xsend, xrecv, csend, crecv, ends, ends_far, stats, moments,
    load_sem, send_sem, ysend_sem, scale_recv, rim_recv, inner_recv, ends_recv, outer_recv,
    xrecv_sem, yrecv_sem, cxrecv_sem, cyrecv_sem, stat_recv,
):
    depth, width, height = sizes
    half, planes, inside = width // 2, 2 * height, height - 2
    chunks = depth // rows
    units = chunks // 2
    sent_at = height * half
    inner = pl.ds(PAD, half)
    forcing, ratio = heat_out, score_out
    places = {axis: lax.axis_index(axis) for axis in ("lat", "lon", "lev")}
    counts = {axis: lax.axis_size(axis) for axis in ("lat", "lon", "lev")}
    upper = places["lev"] == 1

    def beside(axis, offset):
        return {axis: lax.rem(places[axis] + offset + counts[axis], counts[axis])}

    def rows_of(c):
        return pl.ds(c * rows, rows)

    def chunk_of(u, side):
        return u + side * (chunks - 1 - 2 * u)

    def first_lanes(shape):
        return lax.broadcasted_iota(jnp.int32, shape, 1) < shape[1] // 2

    def turned(values):
        return pltpu.roll(values, values.shape[1] // 2, 1)

    def remote(source, target, send_sem, recv_sem, device):
        return pltpu.make_async_remote_copy(
            src_ref=source, dst_ref=target, send_sem=send_sem, recv_sem=recv_sem,
            device_id=device, device_id_type=MESH,
        )

    partner = beside("lev", 1)

    def load(kind, c, slot):
        source = (heat_in, ratio_in, forcing_in)[kind]
        return pltpu.make_async_copy(source.at[rows_of(c)], stage.at[kind, slot], load_sem.at[kind, slot])

    def ratio_copy(u, span):
        cells = pl.ds(sent_at, sent_at)
        return remote(ratio.at[span, cells], ratio_far.at[span], send_sem.at[0], scale_recv.at[u], partner)

    def forcing_copy(u, span):
        cells = pl.ds(sent_at, sent_at)
        return remote(forcing.at[span, cells], forcing_far.at[span], send_sem.at[1], scale_recv.at[u], partner)

    def rim_copy(end, u, c):
        return remote(
            rim.at[end, rows_of(c)], field.at[0, (height, planes - 1)[end], pl.ds(1 + c * rows, rows), inner],
            send_sem.at[2], rim_recv.at[u], partner,
        )

    def inner_copy(u, c):
        return remote(
            field.at[STEPS % 2, pl.ds(height + 1, inside), pl.ds(1 + c * rows, rows), inner],
            back.at[pl.ds(1, inside), rows_of(c)], send_sem.at[3], inner_recv.at[u], partner,
        )

    def outer_copy(end, u, c):
        return remote(
            field.at[STEPS % 2, (height, planes - 1)[end], pl.ds(1 + c * rows, rows), inner],
            back.at[(0, height - 1)[end], rows_of(c)], send_sem.at[3], outer_recv.at[u], partner,
        )

    def ends_copy(u):
        return remote(ends.at[1, u], ends_far.at[u], send_sem.at[8], ends_recv.at[u], partner)

    def xcopy(level, side, u):
        return remote(
            xsend.at[level, u, side], xrecv.at[level, u, 1 - side],
            send_sem.at[4], xrecv_sem.at[lax.rem(level, 2), u], beside("lon", (-1, 1)[side]),
        )

    def ycopy(level, side):
        p = lax.rem(level, 2)
        return remote(
            field.at[p, :, (1, depth)[side], inner], field.at[p, :, (depth + 1, 0)[side], inner],
            ysend_sem.at[p], yrecv_sem.at[p], beside("lat", (-1, 1)[side]),
        )

    def core_xcopy(side, u):
        return remote(
            csend.at[u, side], crecv.at[u, 1 - side], send_sem.at[5], cxrecv_sem.at[u], beside("lon", (-1, 1)[side])
        )

    def core_ycopy(side):
        return remote(
            core.at[:, (1, depth)[side], inner], core.at[:, (depth + 1, 0)[side], inner],
            send_sem.at[6], cyrecv_sem.at[0], beside("lat", (-1, 1)[side]),
        )

    def stat_copy(offset, u):
        return remote(
            stats.at[0, u], stats.at[offset, u], send_sem.at[7], stat_recv.at[lax.rem(u, 2)], beside("lon", offset)
        )

    def wait_all(ref, sem):
        pltpu.make_async_copy(ref, ref, sem).wait()

    def over(count, body):
        def step(i, carry):
            body(i)
            return carry

        lax.fori_loop(0, count, step, 0)


    def split(kind, slot, i, z, x):
        low = stage[kind, slot, i, pl.ds(x * height + z, XBLOCK, stride=height), :]
        high = stage[kind, slot, i, pl.ds((half + x) * height + z, XBLOCK, stride=height), :]
        mask = first_lanes(low.shape)
        one = jnp.where(mask, low, turned(high))
        two = jnp.where(mask, turned(low), high)
        return jnp.where(upper, two, one), jnp.where(upper, one, two)

    def split_into(target, kind, slot, c):
        def row(i):
            for z in range(height):
                for x in range(0, half, XBLOCK):
                    kept, sent = split(kind, slot, i, z, x)
                    target[c * rows + i, pl.ds(z * half + x, XBLOCK), :] = kept
                    target[c * rows + i, pl.ds(sent_at + z * half + x, XBLOCK), :] = sent

        over(rows, row)

    def split_heat(u, slot, c):
        def row(i):
            y = c * rows + i
            for z in range(height):
                for x in range(0, half, XBLOCK):
                    here = pl.ds(PAD + x, XBLOCK)
                    kept, sent = split(0, slot, i, z, x)
                    field[0, z, y + 1, here, :] = kept
                    if 0 < z < height - 1:
                        core[z - 1, y + 1, here, :] = sent
                        field[0, height + z, y + 1, here, :] = jnp.zeros_like(sent)
                    else:
                        rim[min(z, 1), y, pl.ds(x, XBLOCK), :] = sent
            for side, x in ((0, PAD), (1, PAD + half - 1)):
                csend[u, side, slot * rows + i] = jnp.zeros(csend.shape[3:], csend.dtype)
                for n in range(inside):
                    csend[u, side, slot * rows + i, pl.ds(n, 1), :] = core[n, y + 1, pl.ds(x, 1), :]

        over(rows, row)

    def prepare(u, side):
        c = chunk_of(u, side)
        load(1, c, side).wait()
        split_into(ratio, 1, side, c)

        @pl.when((u == 0) & (side == 0))
        def _():
            pl.semaphore_wait(barrier, len(greeted))

        ratio_copy(u, rows_of(c)).start()
        load(0, c, side).wait()
        split_heat(u, side, c)
        for end in (0, 1):
            rim_copy(end, u, c).start()

        @pl.when(side == 1)
        def _():
            for end in (0, 1):
                core_xcopy(end, u).start()

        @pl.when((side == 1) & (u == 0))
        def _():
            for end in (0, 1):
                core_ycopy(end).start()

        load(2, c, side).wait()
        split_into(forcing, 2, side, c)

        @pl.when(u < units - 1)
        def _():
            for kind in (1, 0, 2):
                load(kind, chunk_of(u + 1, side), side).start()

    def correct(u, side):
        c = chunk_of(u, side)

        @pl.when(side == 0)
        def _():
            wait_all(crecv.at[u], cxrecv_sem.at[u])

        @pl.when((side == 0) & (u == 0))
        def _():
            wait_all(core.at[:, pl.ds(0, 2), inner], cyrecv_sem.at[0])

        def row(i):
            y = c * rows + i
            k = side * rows + i
            mask = first_lanes(crecv.shape[3:])
            left = turned(jnp.where(mask, csend[u, 1, k], crecv[u, 0, k]))
            right = turned(jnp.where(mask, crecv[u, 1, k], csend[u, 0, k]))
            for n in range(inside):
                core[n, y + 1, pl.ds(PAD - 1, 1), :] = left[n:n + 1]
                core[n, y + 1, pl.ds(PAD + half, 1), :] = right[n:n + 1]
            for x in range(0, half, XBLOCK):
                here = pl.ds(PAD + x, XBLOCK)
                middles = {n: core[n, y + 1, here, :] for n in range(inside)}
                for z in range(height):
                    parts = [middles[n] for n in (z - 2, z) if n in middles]
                    n = z - 1
                    if n in middles:
                        parts += [
                            core[n, y, here, :] + core[n, y + 2, here, :],
                            core[n, y + 1, pl.ds(PAD + x - 1, XBLOCK), :] + core[n, y + 1, pl.ds(PAD + x + 1, XBLOCK), :],
                            -6.0 * middles[n],
                        ]
                    cells = pl.ds(sent_at + z * half + x, XBLOCK)
                    forcing[y, cells, :] = forcing[y, cells, :] + ratio[y, cells, :] * sum(parts[1:], parts[0])

        over(rows, row)
        forcing_copy(u, rows_of(c)).start()

    barrier = pltpu.get_barrier_semaphore()
    greeted = [partner, beside("lat", -1), beside("lat", 1)]
    greeted += [beside("lon", offset) for offset in range(1, counts["lon"])]
    for device in greeted:
        pl.semaphore_signal(barrier, inc=1, device_id=device, device_id_type=MESH)
    for side in (0, 1):
        for kind in (1, 0, 2):
            load(kind, chunk_of(0, side), side).start()

    def inputs(u):
        @pl.when(u < units)
        def _():
            over(2, lambda side: prepare(u, side))

        @pl.when(u > 0)
        def _():
            over(2, lambda side: correct(u - 1, side))

    over(units + 1, inputs)


    def publish(level, u):
        p = lax.rem(level, 2)

        def row(k):
            y = row_of(u, k)
            for side, x in ((0, PAD), (1, PAD + half - 1)):
                for z in range(planes):
                    xsend[level, u, side, k, pl.ds(z, 1), :] = field[p, z, y + 1, pl.ds(x, 1), :]

        over(2 * rows, row)
        for side in (0, 1):
            xcopy(level, side, u).start()

        @pl.when(u == 0)
        def _():
            for side in (0, 1):
                ycopy(level, side).start()

    def arrive(u):
        wait_all(ratio_far.at[pl.ds(0, 4 * rows)], scale_recv.at[u])
        wait_all(rim.at[:, pl.ds(0, 2 * rows)], rim_recv.at[u])
        publish(0, u)

    def advance(s, u):
        level = s - 1
        p = lax.rem(level, 2)
        q = 1 - p

        @pl.when(u == 0)
        def _():
            wait_all(field.at[p, :, pl.ds(0, 2), inner], yrecv_sem.at[p])

        @pl.when((u == 0) & (s >= 2))
        def _():
            wait_all(field.at[q, :, pl.ds(0, 2), inner], ysend_sem.at[q])

        wait_all(xrecv.at[level, u], xrecv_sem.at[p, u])
        over(2, lambda side: march_rows(level, p, q, u, side))

        @pl.when(s < STEPS)
        def _():
            publish(s, u)

        @pl.when(s == STEPS)
        def _():
            for side in (0, 1):
                inner_copy(u, chunk_of(u, side)).start()
            over(2 * rows, lambda k: end_moments(u, k))
            ends_copy(u).start()
            for side in (0, 1):
                for end in (0, 1):
                    outer_copy(end, u, chunk_of(u, side)).start()

    def row_of(u, k):
        return chunk_of(u, k // rows) * rows + lax.rem(k, rows)

    def end_moments(u, k):
        for whose in (0, 1):
            for end in (0, 1):
                line = field[STEPS % 2, whose * height + end * (height - 1), row_of(u, k) + 1, inner, :]
                mean = both_halves(jnp.sum(line, axis=0, keepdims=True)) * (1.0 / width)
                centred = line - mean
                ends[whose, u, 0, pl.ds(2 * k + end, 1), :] = mean
                squares = both_halves(jnp.sum(centred * centred, axis=0, keepdims=True))
                ends[whose, u, 1, pl.ds(2 * k + end, 1), :] = squares

    def both_halves(sums):
        tall = jnp.broadcast_to(sums, (8, sums.shape[1]))
        return (tall + turned(tall))[:1]

    def march_rows(level, p, q, u, side):
        c = chunk_of(u, side)

        def row(i):
            y = c * rows + i
            k = side * rows + i
            mask = first_lanes(xrecv.shape[4:])
            left = turned(jnp.where(mask, xsend[level, u, 1, k], xrecv[level, u, 0, k]))
            right = turned(jnp.where(mask, xrecv[level, u, 1, k], xsend[level, u, 0, k]))
            for z in range(planes):
                field[p, z, y + 1, pl.ds(PAD - 1, 1), :] = left[z:z + 1]
                field[p, z, y + 1, pl.ds(PAD + half, 1), :] = right[z:z + 1]
            for x in range(0, half, XCELLS):
                here = pl.ds(PAD + x, XCELLS)
                middles = [field[p, z, y + 1, here, :] for z in range(planes)]
                for z in range(planes):
                    middle = middles[z]
                    spread = (
                        field[p, z, y, here, :] + field[p, z, y + 2, here, :]
                        + field[p, z, y + 1, pl.ds(PAD + x - 1, XCELLS), :]
                        + field[p, z, y + 1, pl.ds(PAD + x + 1, XCELLS), :]
                        + middles[z - 1] + middles[(z + 1) % planes]
                        - 6.0 * middle
                    )
                    if z < height:
                        cells = pl.ds(z * half + x, XCELLS)
                        scale, source = ratio[y, cells, :], forcing[y, cells, :]
                    else:
                        cells = pl.ds((z - height) * half + x, XCELLS)
                        scale, source = ratio_far[y, cells, :], forcing_far[y, cells, :]
                    field[q, z, y + 1, here, :] = middle + scale * spread + source

        over(rows, row)

    def wave(w):
        @pl.when(w < units)
        def _():
            arrive(w)

        def step(i):
            u = w - 1 - i

            @pl.when((u >= 0) & (u < units))
            def _():
                advance(i + 1, u)

        over(STEPS, step)

    over(units + STEPS, wave)


    def join(y, z, x):
        here = pl.ds(PAD + x, XBLOCK)
        kept, other = field[STEPS % 2, z, y + 1, here, :], back[z, y, pl.ds(x, XBLOCK), :]
        if 0 < z < height - 1:
            other = other + core[z - 1, y + 1, here, :]
        mask = first_lanes(kept.shape)
        one, two = jnp.where(upper, other, kept), jnp.where(upper, kept, other)
        low = jnp.where(mask, one, turned(two))
        high = jnp.where(mask, turned(one), two)
        heat_out[y, pl.ds(x * height + z, XBLOCK, stride=height), :] = low
        heat_out[y, pl.ds((half + x) * height + z, XBLOCK, stride=height), :] = high
        return [low, high]

    def join_inner(u, k):
        y = row_of(u, k)
        for z in range(1, height - 1):
            line = jnp.concatenate(sum([join(y, z, x) for x in range(0, half, XBLOCK)], []), axis=0)
            mean = jnp.sum(line, axis=0, keepdims=True) * (1.0 / width)
            centred = line - mean
            stats[0, u, 0, pl.ds(k * height + z, 1), :] = mean
            stats[0, u, 1, pl.ds(k * height + z, 1), :] = jnp.sum(centred * centred, axis=0, keepdims=True)

    def share_moments(u):
        mask = first_lanes(ends_far.shape[2:])
        for kind in (0, 1):
            mine, far = ends[0, u, kind], ends_far[u, kind]
            lines = jnp.where(upper, jnp.where(mask, far, mine), jnp.where(mask, mine, far))
            for k in range(2 * rows):
                for end in (0, 1):
                    at = k * height + end * (height - 1)
                    stats[0, u, kind, pl.ds(at, 1), :] = lines[2 * k + end:2 * k + end + 1]
        for offset in range(1, counts["lon"]):
            stat_copy(offset, u).start()

    def combine(u):
        wait_all(stats.at[pl.ds(1, counts["lon"] - 1), u], stat_recv.at[lax.rem(u, 2)])
        means = [stats[offset, u, 0] for offset in range(counts["lon"])]
        mean = sum(means[1:], means[0]) * (1.0 / counts["lon"])
        squares = sum([stats[offset, u, 1] for offset in range(1, counts["lon"])], stats[0, u, 1])
        apart = sum([(other - mean) * (other - mean) for other in means[1:]], (means[0] - mean) * (means[0] - mean))
        variance = (squares + width * apart) * (1.0 / (width * counts["lon"]))
        scale = lax.rsqrt(variance + 0.0001)
        for k in range(2 * rows):
            for copy in range(2):
                for kind, values in ((0, mean), (1, scale)):
                    moments[kind, k, pl.ds(copy * height, height), :] = values[k * height:(k + 1) * height]

    def join_outer(u, k):
        y = row_of(u, k)
        for z in (0, height - 1):
            for x in range(0, half, XBLOCK):
                join(y, z, x)
        values = heat_out[y]
        tall = values.reshape(half, 2 * height, values.shape[1])
        score_out[y] = ((tall - moments[0, k][None]) * moments[1, k][None]).reshape(values.shape)

    wait_all(ratio.at[:, pl.ds(sent_at, sent_at)], send_sem.at[0])
    wait_all(forcing.at[:, pl.ds(sent_at, sent_at)], send_sem.at[1])

    def finish(u):
        wait_all(back.at[pl.ds(0, inside), pl.ds(0, 2 * rows)], inner_recv.at[u])
        over(2 * rows, lambda k: join_inner(u, k))
        wait_all(ends_far.at[u], ends_recv.at[u])
        share_moments(u)
        combine(u)
        wait_all(back.at[pl.ds(0, 2), pl.ds(0, 2 * rows)], outer_recv.at[u])
        over(2 * rows, lambda k: join_outer(u, k))

    over(units, finish)
    wait_all(rim, send_sem.at[2])
    wait_all(field.at[STEPS % 2, pl.ds(height, height), pl.ds(1, depth), inner], send_sem.at[3])
    wait_all(xsend, send_sem.at[4])
    wait_all(csend, send_sem.at[5])
    wait_all(core.at[:, pl.ds(0, 2), inner], send_sem.at[6])
    wait_all(field.at[(STEPS - 1) % 2, :, pl.ds(0, 2), inner], ysend_sem.at[(STEPS - 1) % 2])
    wait_all(stats.at[pl.ds(1, counts["lon"] - 1)], send_sem.at[7])
    wait_all(ends_far, send_sem.at[8])


def swap(sizes, arrays):
    depth, width, height = sizes
    members = arrays[0].shape[-1]
    rows = 2
    chunks = depth // rows
    units = chunks // 2
    half = width // 2
    lon = lax.axis_size("lon")
    flat = (depth, width * height, members)
    f32 = jnp.float32
    dma = pltpu.SemaphoreType.DMA
    vmem = lambda *shape: pltpu.VMEM((*shape, members), f32)
    return pl.pallas_call(
        functools.partial(swap_kernel, sizes, rows),
        out_shape=(pltpu.VMEM(flat, f32),) * 2,
        in_specs=[pl.BlockSpec(memory_space=pl.ANY)] * 3,
        out_specs=(pl.BlockSpec(memory_space=pltpu.VMEM),) * 2,
        scratch_shapes=[
            vmem(2, 2 * height, depth + 2, half + 2 * PAD),
            vmem(2, depth, half),
            vmem(height - 2, depth + 2, half + 2 * PAD),
            vmem(depth, half * height),
            vmem(depth, half * height),
            vmem(height, depth, half),
            vmem(3, 2, rows, width * height),
            vmem(STEPS, units, 2, 2 * rows, 2 * height), vmem(STEPS, units, 2, 2 * rows, 2 * height),
            vmem(units, 2, 2 * rows, 8), vmem(units, 2, 2 * rows, 8),
            vmem(2, units, 2, 4 * rows), vmem(units, 2, 4 * rows),
            vmem(lon, units, 2, 2 * rows * height), vmem(2, 2 * rows, 2 * height),
            dma((3, 2)), dma((9,)), dma((2,)),
            dma((units,)), dma((units,)), dma((units,)), dma((units,)), dma((units,)),
            dma((2, units)), dma((2,)), dma((units,)), dma((1,)), dma((2,)),
        ],
        compiler_params=pltpu.CompilerParams(
            collective_id=1, has_side_effects=True, vmem_limit_bytes=47 * 1024 * 1024
        ),
        name="swap",
    )(*arrays)


def march(sizes, arrays):
    depth, width, height = sizes
    members = arrays[0].shape[-1]
    rows = 2
    chunks = depth // rows
    lon = lax.axis_size("lon")
    flat = (depth, width * height, members)
    f32 = jnp.float32
    anywhere = pl.BlockSpec(memory_space=pl.ANY)
    dma = pltpu.SemaphoreType.DMA
    return pl.pallas_call(
        functools.partial(march_kernel, (depth, width, height), chunks, rows),
        out_shape=(pltpu.VMEM(flat, f32), pltpu.VMEM((2, depth, 2 * height, members), f32)),
        in_specs=[anywhere] * 3,
        out_specs=(pl.BlockSpec(memory_space=pltpu.VMEM),) * 2,
        scratch_shapes=[
            pltpu.VMEM((2, height + 2, depth + 2, width + 2 * PAD, members), f32),
            pltpu.VMEM(flat, f32),
            pltpu.VMEM(flat, f32),
            pltpu.VMEM((2, 2, chunks, rows * height, members), f32),
            pltpu.VMEM((2, 2, chunks, rows * height, members), f32),
            pltpu.VMEM((lon, chunks, 2, rows * height, members), f32),
            dma((chunks,)), dma((chunks,)), dma((chunks,)),
            dma((2, 2, chunks)), dma((2, 2, chunks)),
            dma((2, 2, chunks)), dma((2, 2, chunks)),
            dma((2, 2)), dma((2, 2)),
            dma((lon - 1, chunks)), dma((lon - 1, chunks)),
        ],
        compiler_params=pltpu.CompilerParams(
            collective_id=0, has_side_effects=True, vmem_limit_bytes=48 * 1024 * 1024
        ),
        name="march",
    )(*arrays)


def copy_kernel(chunks, heat, scored, score, end, sem):
    rows = heat.shape[0] // chunks
    copies = []
    for c in range(chunks):
        span = pl.ds(c * rows, rows)
        copies.append(pltpu.make_async_copy(heat.at[span], end.at[span], sem.at[0, c]))
        copies.append(pltpu.make_async_copy(scored.at[span], score.at[span], sem.at[1, c]))
    for copy in copies:
        copy.start()
    for copy in copies:
        copy.wait()


def score_kernel(chunks, heat, moments, score, end, scaled, score_sem, end_sem):
    rows = heat.shape[0] // chunks
    finish = pltpu.make_async_copy(heat, end, end_sem)
    finish.start()

    def out_copy(c):
        span = pl.ds(c * rows, rows)
        return pltpu.make_async_copy(scaled.at[span], score.at[span], score_sem.at[c])

    def chunk(c, carry):
        def row(i, carry):
            y = c * rows + i
            mean, scale = moments[0, y], moments[1, y]
            values = heat[y]
            tall = values.reshape(values.shape[0] // mean.shape[0], *mean.shape)
            scaled[y] = ((tall - mean[None]) * scale[None]).reshape(values.shape)
            return carry

        lax.fori_loop(0, rows, row, 0)
        out_copy(c).start()
        return carry

    def drain(c, carry):
        out_copy(c).wait()
        return carry

    lax.fori_loop(0, chunks, chunk, 0)
    lax.fori_loop(0, chunks, drain, 0)
    finish.wait()


def local(initial_heat, diffusivity_ratio, forcing_term):
    depth, width, height, members = initial_heat.shape
    flat = (depth, width * height, members)
    f32 = jnp.float32
    anywhere = pl.BlockSpec(memory_space=pl.ANY)
    dma = pltpu.SemaphoreType.DMA
    arrays = [a.reshape(flat) for a in (initial_heat, diffusivity_ratio, forcing_term)]
    swaps = lax.axis_size("lev") == 2 and 3 <= height and 3 * height + 2 < 4 * STEPS
    swaps = swaps and depth % 4 == 0 and width % (2 * XBLOCK) == 0
    sizes = (depth, width, height)
    common = dict(out_shape=(jax.ShapeDtypeStruct(flat, f32),) * 2, out_specs=(anywhere,) * 2)
    inputs = [pl.BlockSpec(memory_space=pltpu.VMEM)] * 2
    if swaps:
        parts = min(4, depth)
        score, end = pl.pallas_call(
            functools.partial(copy_kernel, parts), **common, in_specs=inputs,
            scratch_shapes=[dma((2, parts))],
            compiler_params=pltpu.CompilerParams(vmem_limit_bytes=8 * 1024 * 1024),
            name="emit",
        )(*swap(sizes, arrays))
    else:
        parts = min(8, depth)
        score, end = pl.pallas_call(
            functools.partial(score_kernel, parts), **common, in_specs=inputs,
            scratch_shapes=[pltpu.VMEM(flat, f32), dma((parts,)), dma(())],
            compiler_params=pltpu.CompilerParams(vmem_limit_bytes=24 * 1024 * 1024),
            name="score",
        )(*march(sizes, arrays))
    return score.reshape(initial_heat.shape), end.reshape(initial_heat.shape)


def solution(mesh):
    placed = P("lat", "lon", "lev", None)
    return jax.shard_map(
        local, mesh=mesh, in_specs=(placed,) * 3, out_specs=(placed,) * 2, check_vma=False
    )
```

```python
import functools

import jax
import jax.numpy as jnp
from jax import lax
from jax.experimental import pallas as pl
from jax.experimental.pallas import tpu as pltpu
from jax.sharding import PartitionSpec as P

STEPS = 4
PAD = 8
XBLOCK = 32
XCELLS = 16
MESH = pl.DeviceIdType.MESH


def march_kernel(
    sizes, chunks, rows,
    heat_in, ratio_in, forcing_in, raw, moments_out,
    field, ratio, forcing, xsend, xrecv, stats,
    load_heat, load_ratio, load_forcing,
    zsend_sem, zrecv_sem, xsend_sem, xrecv_sem, ysend_sem, yrecv_sem, stat_send, stat_recv,
):
    depth, width, height = sizes
    inner = pl.ds(PAD, width)
    places = {axis: lax.axis_index(axis) for axis in ("lat", "lon", "lev")}
    counts = {axis: lax.axis_size(axis) for axis in ("lat", "lon", "lev")}

    def beside(axis, offset):
        return {axis: lax.rem(places[axis] + offset + counts[axis], counts[axis])}

    def rows_of(c):
        return pl.ds(c * rows, rows)

    def load(c):
        return [
            pltpu.make_async_copy(source.at[rows_of(c)], target.at[rows_of(c)], sem.at[c])
            for source, target, sem in (
                (heat_in, raw, load_heat), (ratio_in, ratio, load_ratio), (forcing_in, forcing, load_forcing),
            )
        ]

    def zcopy(side, p, c):
        span = pl.ds(1 + c * rows, rows)
        return pltpu.make_async_remote_copy(
            src_ref=field.at[p, (1, height)[side], span, inner],
            dst_ref=field.at[p, (height + 1, 0)[side], span, inner],
            send_sem=zsend_sem.at[side, p, c], recv_sem=zrecv_sem.at[1 - side, p, c],
            device_id=beside("lev", (-1, 1)[side]), device_id_type=MESH,
        )

    def xcopy(side, p, c):
        return pltpu.make_async_remote_copy(
            src_ref=xsend.at[side, p, c], dst_ref=xrecv.at[1 - side, p, c],
            send_sem=xsend_sem.at[side, p, c], recv_sem=xrecv_sem.at[1 - side, p, c],
            device_id=beside("lon", (-1, 1)[side]), device_id_type=MESH,
        )

    def ycopy(side, p):
        return pltpu.make_async_remote_copy(
            src_ref=field.at[p, pl.ds(1, height), (1, depth)[side], inner],
            dst_ref=field.at[p, pl.ds(1, height), (depth + 1, 0)[side], inner],
            send_sem=ysend_sem.at[side, p], recv_sem=yrecv_sem.at[1 - side, p],
            device_id=beside("lat", (-1, 1)[side]), device_id_type=MESH,
        )

    def stat_copy(offset, c):
        return pltpu.make_async_remote_copy(
            src_ref=stats.at[0, c], dst_ref=stats.at[offset, c],
            send_sem=stat_send.at[offset - 1, c], recv_sem=stat_recv.at[offset - 1, c],
            device_id=beside("lon", offset), device_id_type=MESH,
        )

    def send(p, c):
        for side, end in ((0, 0), (1, chunks - 1)):
            @pl.when(c == end)
            def _():
                ycopy(side, p).start()
        for side in (0, 1):
            zcopy(side, p, c).start()
        for side in (0, 1):
            xcopy(side, p, c).start()

    def sent(p, c):
        for side, end in ((0, 0), (1, chunks - 1)):
            @pl.when(c == end)
            def _():
                ycopy(side, p).wait_send()
        for side in (0, 1):
            zcopy(side, p, c).wait_send()
            xcopy(side, p, c).wait_send()

    def arrived(p, c):
        for side, end in ((1, 0), (0, chunks - 1)):
            @pl.when(c == end)
            def _():
                ycopy(side, p).wait_recv()
        for side in (0, 1):
            xcopy(side, p, c).wait_recv()
        for side in (0, 1):
            zcopy(side, p, c).wait_recv()

    def pack(p, c, i):
        for z in range(height):
            for side, x in ((0, PAD), (1, PAD + width - 1)):
                xsend[side, p, c, pl.ds(i * height + z, 1), :] = field[p, z + 1, c * rows + i + 1, pl.ds(x, 1), :]

    def start_loads(c, carry):
        load(c)[0].start()
        return carry

    def start_others(c, carry):
        for copy in load(c)[1:]:
            copy.start()
        return carry

    barrier = pltpu.get_barrier_semaphore()
    greeted = [beside("lev", -1), beside("lev", 1), beside("lat", -1), beside("lat", 1)]
    greeted += [beside("lon", offset) for offset in range(1, counts["lon"])]
    for device in greeted:
        pl.semaphore_signal(barrier, inc=1, device_id=device, device_id_type=MESH)
    lax.fori_loop(0, chunks, start_loads, 0)

    def unpack(c):
        load(c)[0].wait()

        def row(i, carry):
            y = c * rows + i
            for z in range(height):
                field[0, z + 1, y + 1, inner, :] = raw[y, pl.ds(z, width, stride=height), :]
            pack(0, c, i)
            return carry

        lax.fori_loop(0, rows, row, 0)

    def unpack_send(c, carry):
        unpack(c)
        send(0, c)
        return carry

    unpack(0)
    pl.semaphore_wait(barrier, len(greeted))
    send(0, 0)
    lax.fori_loop(0, chunks, start_others, 0)
    lax.fori_loop(1, chunks, unpack_send, 0)

    def combine(c):
        for offset in range(1, counts["lon"]):
            stat_copy(offset, c).wait_recv()
        means = [stats[offset, c, 0] for offset in range(counts["lon"])]
        mean = sum(means[1:], means[0]) * (1.0 / counts["lon"])
        squares = sum([stats[offset, c, 1] for offset in range(1, counts["lon"])], stats[0, c, 1])
        apart = sum([(other - mean) * (other - mean) for other in means[1:]], (means[0] - mean) * (means[0] - mean))
        variance = (squares + width * apart) * (1.0 / (width * counts["lon"]))
        scale = lax.rsqrt(variance + 0.0001)
        for i in range(rows):
            for half in range(2):
                for kind, values in ((0, mean), (1, scale)):
                    moments_out[kind, c * rows + i, pl.ds(half * height, height), :] = values[i * height:(i + 1) * height]
        for offset in range(1, counts["lon"]):
            stat_copy(offset, c).wait_send()
        sent((STEPS - 1) % 2, c)

    def step(s, carry):
        p = lax.rem(s, 2)
        q = 1 - p

        def chunk(c, carry):
            @pl.when(s == 0)
            def _():
                for copy in load(c)[1:]:
                    copy.wait()

            @pl.when(s >= 1)
            def _():
                sent(q, c)

            arrived(p, c)

            def row(i, carry):
                y = c * rows + i
                for z in range(height):
                    for side, x in ((0, PAD - 1), (1, PAD + width)):
                        field[p, z + 1, y + 1, pl.ds(x, 1), :] = xrecv[side, p, c, pl.ds(i * height + z, 1), :]
                for x in range(0, width, XBLOCK):
                    here = pl.ds(PAD + x, XBLOCK)
                    planes = [field[p, z, y + 1, here, :] for z in range(height + 2)]
                    for z in range(height):
                        middle = planes[z + 1]
                        spread = (
                            field[p, z + 1, y, here, :] + field[p, z + 1, y + 2, here, :]
                            + field[p, z + 1, y + 1, pl.ds(PAD + x - 1, XBLOCK), :]
                            + field[p, z + 1, y + 1, pl.ds(PAD + x + 1, XBLOCK), :]
                            + planes[z] + planes[z + 2] - 6.0 * middle
                        )
                        cells = pl.ds(x * height + z, XBLOCK, stride=height)
                        field[q, z + 1, y + 1, here, :] = middle + ratio[y, cells, :] * spread + forcing[y, cells, :]
                pack(q, c, i)
                return carry

            lax.fori_loop(0, rows, row, 0)

            @pl.when(s < STEPS - 1)
            def _():
                send(q, c)

            @pl.when(s == STEPS - 1)
            def _():
                def finish(i, carry):
                    y = c * rows + i
                    for z in range(height):
                        line = field[q, z + 1, y + 1, inner, :]
                        raw[y, pl.ds(z, width, stride=height), :] = line
                        mean = jnp.sum(line, axis=0, keepdims=True) * (1.0 / width)
                        centred = line - mean
                        stats[0, c, 0, pl.ds(i * height + z, 1), :] = mean
                        stats[0, c, 1, pl.ds(i * height + z, 1), :] = jnp.sum(centred * centred, axis=0, keepdims=True)
                    return carry

                lax.fori_loop(0, rows, finish, 0)
                for offset in range(1, counts["lon"]):
                    stat_copy(offset, c).start()

                @pl.when(c >= 1)
                def _():
                    combine(c - 1)

            return carry

        lax.fori_loop(0, chunks, chunk, 0)
        return carry

    lax.fori_loop(0, STEPS, step, 0)


    combine(chunks - 1)


def swap_kernel(
    sizes, rows,
    heat_in, ratio_in, forcing_in, heat_out, score_out, seam_far, seam_near, seam_rows, moments,
    field, rim, core, ratio_far, forcing_far, back, stage,
    xsend, xrecv, csend, crecv, ends, ends_far, stats,
    load_sem, send_sem, ysend_sem, scale_recv, rim_recv, inner_recv, ends_recv, outer_recv,
    xrecv_sem, yrecv_sem, cxrecv_sem, cyrecv_sem, stat_recv, seam_sem,
):
    depth, width, height = sizes
    half, planes, inside = width // 2, 2 * height, height - 2
    chunks = depth // rows
    units = chunks // 2
    sent_at = height * half
    inner = pl.ds(PAD, half)
    forcing, ratio = heat_out, score_out
    places = {axis: lax.axis_index(axis) for axis in ("lat", "lon", "lev")}
    counts = {axis: lax.axis_size(axis) for axis in ("lat", "lon", "lev")}
    upper = places["lev"] == 1

    def beside(axis, offset):
        return {axis: lax.rem(places[axis] + offset + counts[axis], counts[axis])}

    def rows_of(c):
        return pl.ds(c * rows, rows)

    def chunk_of(u, side):
        return u + side * (chunks - 1 - 2 * u)

    def first_lanes(shape):
        return lax.broadcasted_iota(jnp.int32, shape, 1) < shape[1] // 2

    def turned(values):
        return pltpu.roll(values, values.shape[1] // 2, 1)

    def remote(source, target, send_sem, recv_sem, device):
        return pltpu.make_async_remote_copy(
            src_ref=source, dst_ref=target, send_sem=send_sem, recv_sem=recv_sem,
            device_id=device, device_id_type=MESH,
        )

    partner = beside("lev", 1)

    def load(kind, c, slot):
        source = (heat_in, ratio_in, forcing_in)[kind]
        return pltpu.make_async_copy(source.at[rows_of(c)], stage.at[kind, slot], load_sem.at[kind, slot])

    def ratio_copy(u, span):
        cells = pl.ds(sent_at, sent_at)
        return remote(ratio.at[span, cells], ratio_far.at[span], send_sem.at[0], scale_recv.at[u], partner)

    def forcing_copy(u, span):
        cells = pl.ds(sent_at, sent_at)
        return remote(forcing.at[span, cells], forcing_far.at[span], send_sem.at[1], scale_recv.at[u], partner)

    def rim_copy(end, u, c):
        return remote(
            rim.at[end, rows_of(c)], field.at[0, (height, planes - 1)[end], pl.ds(1 + c * rows, rows), inner],
            send_sem.at[2], rim_recv.at[u], partner,
        )

    def inner_copy(u, c):
        return remote(
            field.at[STEPS % 2, pl.ds(height + 1, inside), pl.ds(1 + c * rows, rows), inner],
            back.at[pl.ds(1, inside), rows_of(c)], send_sem.at[3], inner_recv.at[u], partner,
        )

    def outer_copy(end, u, c):
        return remote(
            field.at[STEPS % 2, (height, planes - 1)[end], pl.ds(1 + c * rows, rows), inner],
            back.at[(0, height - 1)[end], rows_of(c)], send_sem.at[9], outer_recv.at[u], partner,
        )

    def ends_copy(u):
        return remote(ends.at[1, u], ends_far.at[u], send_sem.at[8], ends_recv.at[u], partner)

    def xcopy(level, side, u):
        return remote(
            xsend.at[level, u, side], xrecv.at[level, u, 1 - side],
            send_sem.at[4], xrecv_sem.at[lax.rem(level, 2), u], beside("lon", (-1, 1)[side]),
        )

    def ycopy(level, side):
        p = lax.rem(level, 2)
        return remote(
            field.at[p, :, (1, depth)[side], inner], field.at[p, :, (depth + 1, 0)[side], inner],
            ysend_sem.at[p], yrecv_sem.at[p], beside("lat", (-1, 1)[side]),
        )

    def core_xcopy(side, u):
        return remote(
            csend.at[u, side], crecv.at[u, 1 - side], send_sem.at[5], cxrecv_sem.at[u], beside("lon", (-1, 1)[side])
        )

    def core_ycopy(side):
        return remote(
            core.at[:, (1, depth)[side], inner], core.at[:, (depth + 1, 0)[side], inner],
            send_sem.at[6], cyrecv_sem.at[0], beside("lat", (-1, 1)[side]),
        )

    def stat_copy(offset, u):
        return remote(
            stats.at[0, u], stats.at[offset, u], send_sem.at[7], stat_recv.at[lax.rem(u, 2)], beside("lon", offset)
        )

    def wait_all(ref, sem):
        pltpu.make_async_copy(ref, ref, sem).wait()

    def over(count, body):
        def step(i, carry):
            body(i)
            return carry

        lax.fori_loop(0, count, step, 0)


    def split(kind, slot, i, z, x):
        low = stage[kind, slot, i, pl.ds(x * height + z, XBLOCK, stride=height), :]
        high = stage[kind, slot, i, pl.ds((half + x) * height + z, XBLOCK, stride=height), :]
        mask = first_lanes(low.shape)
        one = jnp.where(mask, low, turned(high))
        two = jnp.where(mask, turned(low), high)
        return jnp.where(upper, two, one), jnp.where(upper, one, two)

    def split_into(target, kind, slot, c):
        def row(i):
            for z in range(height):
                for x in range(0, half, XBLOCK):
                    kept, sent = split(kind, slot, i, z, x)
                    target[c * rows + i, pl.ds(z * half + x, XBLOCK), :] = kept
                    target[c * rows + i, pl.ds(sent_at + z * half + x, XBLOCK), :] = sent

        over(rows, row)

    def split_heat(u, slot, c):
        def row(i):
            y = c * rows + i
            for z in range(height):
                for x in range(0, half, XBLOCK):
                    here = pl.ds(PAD + x, XBLOCK)
                    kept, sent = split(0, slot, i, z, x)
                    field[0, z, y + 1, here, :] = kept
                    if 0 < z < height - 1:
                        core[z - 1, y + 1, here, :] = sent
                        field[0, height + z, y + 1, here, :] = jnp.zeros_like(sent)
                    else:
                        rim[min(z, 1), y, pl.ds(x, XBLOCK), :] = sent
            for side, x in ((0, PAD), (1, PAD + half - 1)):
                csend[u, side, slot * rows + i] = jnp.zeros(csend.shape[3:], csend.dtype)
                for n in range(inside):
                    csend[u, side, slot * rows + i, pl.ds(n, 1), :] = core[n, y + 1, pl.ds(x, 1), :]

        over(rows, row)

    def prepare(u, side):
        c = chunk_of(u, side)
        load(1, c, side).wait()
        split_into(ratio, 1, side, c)

        @pl.when((u == 0) & (side == 0))
        def _():
            pl.semaphore_wait(barrier, len(greeted))

        ratio_copy(u, rows_of(c)).start()
        load(0, c, side).wait()
        split_heat(u, side, c)
        for end in (0, 1):
            rim_copy(end, u, c).start()

        @pl.when(side == 1)
        def _():
            for end in (0, 1):
                core_xcopy(end, u).start()

        @pl.when((side == 1) & (u == 0))
        def _():
            for end in (0, 1):
                core_ycopy(end).start()

        load(2, c, side).wait()
        split_into(forcing, 2, side, c)

        @pl.when(u < units - 1)
        def _():
            for kind in (1, 0, 2):
                load(kind, chunk_of(u + 1, side), side).start()

    def correct(u, side):
        c = chunk_of(u, side)

        @pl.when(side == 0)
        def _():
            wait_all(crecv.at[u], cxrecv_sem.at[u])

        @pl.when((side == 0) & (u == 0))
        def _():
            wait_all(core.at[:, pl.ds(0, 2), inner], cyrecv_sem.at[0])

        def row(i):
            y = c * rows + i
            k = side * rows + i
            mask = first_lanes(crecv.shape[3:])
            left = turned(jnp.where(mask, csend[u, 1, k], crecv[u, 0, k]))
            right = turned(jnp.where(mask, crecv[u, 1, k], csend[u, 0, k]))
            for n in range(inside):
                core[n, y + 1, pl.ds(PAD - 1, 1), :] = left[n:n + 1]
                core[n, y + 1, pl.ds(PAD + half, 1), :] = right[n:n + 1]
            for x in range(0, half, XBLOCK):
                here = pl.ds(PAD + x, XBLOCK)
                middles = {n: core[n, y + 1, here, :] for n in range(inside)}
                for z in range(height):
                    parts = [middles[n] for n in (z - 2, z) if n in middles]
                    n = z - 1
                    if n in middles:
                        parts += [
                            core[n, y, here, :] + core[n, y + 2, here, :],
                            core[n, y + 1, pl.ds(PAD + x - 1, XBLOCK), :] + core[n, y + 1, pl.ds(PAD + x + 1, XBLOCK), :],
                            -6.0 * middles[n],
                        ]
                    cells = pl.ds(sent_at + z * half + x, XBLOCK)
                    forcing[y, cells, :] = forcing[y, cells, :] + ratio[y, cells, :] * sum(parts[1:], parts[0])

        over(rows, row)
        forcing_copy(u, rows_of(c)).start()

    barrier = pltpu.get_barrier_semaphore()
    greeted = [partner, beside("lat", -1), beside("lat", 1)]
    greeted += [beside("lon", offset) for offset in range(1, counts["lon"])]
    for device in greeted:
        pl.semaphore_signal(barrier, inc=1, device_id=device, device_id_type=MESH)
    for side in (0, 1):
        for kind in (1, 0, 2):
            load(kind, chunk_of(0, side), side).start()

    def inputs(u):
        @pl.when(u < units)
        def _():
            over(2, lambda side: prepare(u, side))

        @pl.when(u > 0)
        def _():
            over(2, lambda side: correct(u - 1, side))

    over(units + 1, inputs)


    def publish(level, u):
        p = lax.rem(level, 2)

        def row(k):
            y = row_of(u, k)
            for side, x in ((0, PAD), (1, PAD + half - 1)):
                for z in range(planes):
                    xsend[level, u, side, k, pl.ds(z, 1), :] = field[p, z, y + 1, pl.ds(x, 1), :]

        over(2 * rows, row)
        for side in (0, 1):
            xcopy(level, side, u).start()

        @pl.when(u == 0)
        def _():
            for side in (0, 1):
                ycopy(level, side).start()

    def arrive(u):
        wait_all(ratio_far.at[pl.ds(0, 4 * rows)], scale_recv.at[u])
        wait_all(rim.at[:, pl.ds(0, 2 * rows)], rim_recv.at[u])
        publish(0, u)

    def advance(s, u):
        level = s - 1
        p = lax.rem(level, 2)
        q = 1 - p

        @pl.when(u == 0)
        def _():
            wait_all(field.at[p, :, pl.ds(0, 2), inner], yrecv_sem.at[p])

        @pl.when((u == 0) & (s >= 2))
        def _():
            wait_all(field.at[q, :, pl.ds(0, 2), inner], ysend_sem.at[q])

        wait_all(xrecv.at[level, u], xrecv_sem.at[p, u])
        over(2, lambda side: march_rows(level, p, q, u, side))

        @pl.when(s < STEPS)
        def _():
            publish(s, u)

        @pl.when(s == STEPS)
        def _():
            for side in (0, 1):
                inner_copy(u, chunk_of(u, side)).start()
            over(2 * rows, lambda k: end_moments(u, k))
            ends_copy(u).start()

        @pl.when((s == STEPS) & (u > 0))
        def _():
            for side in (0, 1):
                for end in (0, 1):
                    outer_copy(end, u - 1, chunk_of(u - 1, side)).start()

        @pl.when((s == STEPS) & (u == units - 1))
        def _():
            over(2 * rows, lambda k: keep_seam(u, k))
            for end in (0, 1):
                seam_copy(end).start()

    def keep_seam(u, k):
        for end in (0, 1):
            seam_near[end, k] = field[STEPS % 2, end * (height - 1), row_of(u, k) + 1, inner, :]

    def seam_copy(end):
        span = pl.ds((units - 1) * rows + 1, 2 * rows)
        plane = field.at[STEPS % 2, (height, planes - 1)[end], span, inner]
        return pltpu.make_async_copy(plane, seam_far.at[end], seam_sem.at[end])

    def row_of(u, k):
        return chunk_of(u, k // rows) * rows + lax.rem(k, rows)

    def end_moments(u, k):
        for whose in (0, 1):
            for end in (0, 1):
                line = field[STEPS % 2, whose * height + end * (height - 1), row_of(u, k) + 1, inner, :]
                mean = both_halves(jnp.sum(line, axis=0, keepdims=True)) * (1.0 / width)
                centred = line - mean
                ends[whose, u, 0, pl.ds(2 * k + end, 1), :] = mean
                squares = both_halves(jnp.sum(centred * centred, axis=0, keepdims=True))
                ends[whose, u, 1, pl.ds(2 * k + end, 1), :] = squares

    def both_halves(sums):
        tall = jnp.broadcast_to(sums, (8, sums.shape[1]))
        return (tall + turned(tall))[:1]

    def march_rows(level, p, q, u, side):
        c = chunk_of(u, side)

        def row(i):
            y = c * rows + i
            k = side * rows + i
            mask = first_lanes(xrecv.shape[4:])
            left = turned(jnp.where(mask, xsend[level, u, 1, k], xrecv[level, u, 0, k]))
            right = turned(jnp.where(mask, xrecv[level, u, 1, k], xsend[level, u, 0, k]))
            for z in range(planes):
                field[p, z, y + 1, pl.ds(PAD - 1, 1), :] = left[z:z + 1]
                field[p, z, y + 1, pl.ds(PAD + half, 1), :] = right[z:z + 1]
            for x in range(0, half, XCELLS):
                here = pl.ds(PAD + x, XCELLS)
                middles = [field[p, z, y + 1, here, :] for z in range(planes)]
                for z in range(planes):
                    middle = middles[z]
                    spread = (
                        field[p, z, y, here, :] + field[p, z, y + 2, here, :]
                        + field[p, z, y + 1, pl.ds(PAD + x - 1, XCELLS), :]
                        + field[p, z, y + 1, pl.ds(PAD + x + 1, XCELLS), :]
                        + middles[z - 1] + middles[(z + 1) % planes]
                        - 6.0 * middle
                    )
                    if z < height:
                        cells = pl.ds(z * half + x, XCELLS)
                        scale, source = ratio[y, cells, :], forcing[y, cells, :]
                    else:
                        cells = pl.ds((z - height) * half + x, XCELLS)
                        scale, source = ratio_far[y, cells, :], forcing_far[y, cells, :]
                    field[q, z, y + 1, here, :] = middle + scale * spread + source

        over(rows, row)

    def wave(w):
        @pl.when(w < units)
        def _():
            arrive(w)

        def step(i):
            u = w - 1 - i

            @pl.when((u >= 0) & (u < units))
            def _():
                advance(i + 1, u)

        over(STEPS, step)

    over(units + STEPS, wave)


    def join(y, z, x):
        here = pl.ds(PAD + x, XBLOCK)
        kept, other = field[STEPS % 2, z, y + 1, here, :], back[z, y, pl.ds(x, XBLOCK), :]
        if 0 < z < height - 1:
            other = other + core[z - 1, y + 1, here, :]
        mask = first_lanes(kept.shape)
        one, two = jnp.where(upper, other, kept), jnp.where(upper, kept, other)
        low = jnp.where(mask, one, turned(two))
        high = jnp.where(mask, turned(one), two)
        heat_out[y, pl.ds(x * height + z, XBLOCK, stride=height), :] = low
        heat_out[y, pl.ds((half + x) * height + z, XBLOCK, stride=height), :] = high
        return [low, high]

    def join_inner(u, k):
        y = row_of(u, k)
        for z in range(1, height - 1):
            line = jnp.concatenate(sum([join(y, z, x) for x in range(0, half, XBLOCK)], []), axis=0)
            mean = jnp.sum(line, axis=0, keepdims=True) * (1.0 / width)
            centred = line - mean
            stats[0, u, 0, pl.ds(k * height + z, 1), :] = mean
            stats[0, u, 1, pl.ds(k * height + z, 1), :] = jnp.sum(centred * centred, axis=0, keepdims=True)

    def share_moments(u):
        mask = first_lanes(ends_far.shape[2:])
        for kind in (0, 1):
            mine, far = ends[0, u, kind], ends_far[u, kind]
            lines = jnp.where(upper, jnp.where(mask, far, mine), jnp.where(mask, mine, far))
            for k in range(2 * rows):
                for end in (0, 1):
                    at = k * height + end * (height - 1)
                    stats[0, u, kind, pl.ds(at, 1), :] = lines[2 * k + end:2 * k + end + 1]
        for offset in range(1, counts["lon"]):
            stat_copy(offset, u).start()

    def combine(u):
        wait_all(stats.at[pl.ds(1, counts["lon"] - 1), u], stat_recv.at[lax.rem(u, 2)])
        means = [stats[offset, u, 0] for offset in range(counts["lon"])]
        mean = sum(means[1:], means[0]) * (1.0 / counts["lon"])
        squares = sum([stats[offset, u, 1] for offset in range(1, counts["lon"])], stats[0, u, 1])
        apart = sum([(other - mean) * (other - mean) for other in means[1:]], (means[0] - mean) * (means[0] - mean))
        variance = (squares + width * apart) * (1.0 / (width * counts["lon"]))
        scale = lax.rsqrt(variance + 0.0001)
        for k in range(2 * rows):
            for copy in range(2):
                for kind, values in ((0, mean), (1, scale)):
                    moments[u, kind, k, pl.ds(copy * height, height), :] = values[k * height:(k + 1) * height]

    def join_outer(u, k):
        y = row_of(u, k)
        for z in (0, height - 1):
            for x in range(0, half, XBLOCK):
                join(y, z, x)
        values = heat_out[y]
        tall = values.reshape(half, 2 * height, values.shape[1])
        score_out[y] = ((tall - moments[u, 0, k][None]) * moments[u, 1, k][None]).reshape(values.shape)

    wait_all(ratio.at[:, pl.ds(sent_at, sent_at)], send_sem.at[0])
    wait_all(forcing.at[:, pl.ds(sent_at, sent_at)], send_sem.at[1])

    def finish(u):
        wait_all(back.at[pl.ds(0, inside), pl.ds(0, 2 * rows)], inner_recv.at[u])
        over(2 * rows, lambda k: join_inner(u, k))
        wait_all(ends_far.at[u], ends_recv.at[u])
        share_moments(u)
        combine(u)

        @pl.when(u > 0)
        def _():
            wait_all(back.at[pl.ds(0, 2), pl.ds(0, 2 * rows)], outer_recv.at[u - 1])
            over(2 * rows, lambda k: join_outer(u - 1, k))

    over(units, finish)

    def seam_row(k):
        seam_rows[k] = heat_out[row_of(units - 1, k)]

    over(2 * rows, seam_row)
    wait_all(rim, send_sem.at[2])
    for end in (0, 1):
        seam_copy(end).wait()
    wait_all(field.at[STEPS % 2, pl.ds(height + 1, inside), pl.ds(1, depth), inner], send_sem.at[3])
    wait_all(field.at[STEPS % 2, pl.ds(height, 2), pl.ds(1, depth - 2 * rows), inner], send_sem.at[9])
    wait_all(xsend, send_sem.at[4])
    wait_all(csend, send_sem.at[5])
    wait_all(core.at[:, pl.ds(0, 2), inner], send_sem.at[6])
    wait_all(field.at[(STEPS - 1) % 2, :, pl.ds(0, 2), inner], ysend_sem.at[(STEPS - 1) % 2])
    wait_all(stats.at[pl.ds(1, counts["lon"] - 1)], send_sem.at[7])
    wait_all(ends_far, send_sem.at[8])


def swap(sizes, arrays):
    depth, width, height = sizes
    members = arrays[0].shape[-1]
    rows = 2
    chunks = depth // rows
    units = chunks // 2
    half = width // 2
    lon = lax.axis_size("lon")
    flat = (depth, width * height, members)
    f32 = jnp.float32
    dma = pltpu.SemaphoreType.DMA
    vmem = lambda *shape: pltpu.VMEM((*shape, members), f32)
    return pl.pallas_call(
        functools.partial(swap_kernel, sizes, rows),
        out_shape=(
            pltpu.VMEM(flat, f32), pltpu.VMEM(flat, f32),
            jax.ShapeDtypeStruct((2, 2 * rows, half, members), f32), vmem(2, 2 * rows, half),
            vmem(2 * rows, width * height), vmem(units, 2, 2 * rows, 2 * height),
        ),
        in_specs=[pl.BlockSpec(memory_space=pl.ANY)] * 3,
        out_specs=tuple(pl.BlockSpec(memory_space=pltpu.HBM if i == 2 else pltpu.VMEM) for i in range(6)),
        scratch_shapes=[
            vmem(2, 2 * height, depth + 2, half + 2 * PAD),
            vmem(2, depth, half),
            vmem(height - 2, depth + 2, half + 2 * PAD),
            vmem(depth, half * height),
            vmem(depth, half * height),
            vmem(height, depth, half),
            vmem(3, 2, rows, width * height),
            vmem(STEPS, units, 2, 2 * rows, 2 * height), vmem(STEPS, units, 2, 2 * rows, 2 * height),
            vmem(units, 2, 2 * rows, 8), vmem(units, 2, 2 * rows, 8),
            vmem(2, units, 2, 4 * rows), vmem(units, 2, 4 * rows),
            vmem(lon, units, 2, 2 * rows * height),
            dma((3, 2)), dma((10,)), dma((2,)),
            dma((units,)), dma((units,)), dma((units,)), dma((units,)), dma((units,)),
            dma((2, units)), dma((2,)), dma((units,)), dma((1,)), dma((2,)), dma((2,)),
        ],
        compiler_params=pltpu.CompilerParams(
            collective_id=1, has_side_effects=True, vmem_limit_bytes=46 * 1024 * 1024
        ),
        name="swap",
    )(*arrays)


def march(sizes, arrays):
    depth, width, height = sizes
    members = arrays[0].shape[-1]
    rows = 2
    chunks = depth // rows
    lon = lax.axis_size("lon")
    flat = (depth, width * height, members)
    f32 = jnp.float32
    anywhere = pl.BlockSpec(memory_space=pl.ANY)
    dma = pltpu.SemaphoreType.DMA
    return pl.pallas_call(
        functools.partial(march_kernel, (depth, width, height), chunks, rows),
        out_shape=(pltpu.VMEM(flat, f32), pltpu.VMEM((2, depth, 2 * height, members), f32)),
        in_specs=[anywhere] * 3,
        out_specs=(pl.BlockSpec(memory_space=pltpu.VMEM),) * 2,
        scratch_shapes=[
            pltpu.VMEM((2, height + 2, depth + 2, width + 2 * PAD, members), f32),
            pltpu.VMEM(flat, f32),
            pltpu.VMEM(flat, f32),
            pltpu.VMEM((2, 2, chunks, rows * height, members), f32),
            pltpu.VMEM((2, 2, chunks, rows * height, members), f32),
            pltpu.VMEM((lon, chunks, 2, rows * height, members), f32),
            dma((chunks,)), dma((chunks,)), dma((chunks,)),
            dma((2, 2, chunks)), dma((2, 2, chunks)),
            dma((2, 2, chunks)), dma((2, 2, chunks)),
            dma((2, 2)), dma((2, 2)),
            dma((lon - 1, chunks)), dma((lon - 1, chunks)),
        ],
        compiler_params=pltpu.CompilerParams(
            collective_id=0, has_side_effects=True, vmem_limit_bytes=48 * 1024 * 1024
        ),
        name="march",
    )(*arrays)


def copy_kernel(chunks, heat, scored, score, end, sem):
    rows = heat.shape[0] // chunks
    copies = []
    for c in range(chunks):
        span = pl.ds(c * rows, rows)
        copies.append(pltpu.make_async_copy(heat.at[span], end.at[span], sem.at[0, c]))
        copies.append(pltpu.make_async_copy(scored.at[span], score.at[span], sem.at[1, c]))
    for copy in copies:
        copy.start()
    for copy in copies:
        copy.wait()


def seam_kernel(sizes, far, near, rows_in, moments, score_in, end_in, score, end, joined, scored, sem):
    width, height, first = sizes
    half = width // 2
    unit = moments.shape[0] - 1
    upper = lax.axis_index("lev") == 1

    def out_copies(k):
        return [
            pltpu.make_async_copy(source.at[k], target.at[first + k], sem.at[kind, k])
            for kind, (source, target) in enumerate(((joined, end), (scored, score)))
        ]

    def row(k, carry):
        joined[k] = rows_in[k]
        for side, z in ((0, 0), (1, height - 1)):
            for x in range(0, half, XBLOCK):
                kept, other = near[side, k, pl.ds(x, XBLOCK), :], far[side, k, pl.ds(x, XBLOCK), :]
                mask = lax.broadcasted_iota(jnp.int32, kept.shape, 1) < kept.shape[1] // 2
                one, two = jnp.where(upper, other, kept), jnp.where(upper, kept, other)
                turn = kept.shape[1] // 2
                joined[k, pl.ds(x * height + z, XBLOCK, stride=height), :] = jnp.where(mask, one, pltpu.roll(two, turn, 1))
                joined[k, pl.ds((half + x) * height + z, XBLOCK, stride=height), :] = jnp.where(
                    mask, pltpu.roll(one, turn, 1), two
                )
        out_copies(k)[0].start()
        values = joined[k]
        tall = values.reshape(half, 2 * height, values.shape[1])
        scored[k] = ((tall - moments[unit, 0, k][None]) * moments[unit, 1, k][None]).reshape(values.shape)
        out_copies(k)[1].start()
        return carry

    lax.fori_loop(0, joined.shape[0], row, 0)
    for k in range(joined.shape[0]):
        for copy in out_copies(k):
            copy.wait()


def score_kernel(chunks, heat, moments, score, end, scaled, score_sem, end_sem):
    rows = heat.shape[0] // chunks
    finish = pltpu.make_async_copy(heat, end, end_sem)
    finish.start()

    def out_copy(c):
        span = pl.ds(c * rows, rows)
        return pltpu.make_async_copy(scaled.at[span], score.at[span], score_sem.at[c])

    def chunk(c, carry):
        def row(i, carry):
            y = c * rows + i
            mean, scale = moments[0, y], moments[1, y]
            values = heat[y]
            tall = values.reshape(values.shape[0] // mean.shape[0], *mean.shape)
            scaled[y] = ((tall - mean[None]) * scale[None]).reshape(values.shape)
            return carry

        lax.fori_loop(0, rows, row, 0)
        out_copy(c).start()
        return carry

    def drain(c, carry):
        out_copy(c).wait()
        return carry

    lax.fori_loop(0, chunks, chunk, 0)
    lax.fori_loop(0, chunks, drain, 0)
    finish.wait()


def local(initial_heat, diffusivity_ratio, forcing_term):
    depth, width, height, members = initial_heat.shape
    flat = (depth, width * height, members)
    f32 = jnp.float32
    anywhere = pl.BlockSpec(memory_space=pl.ANY)
    dma = pltpu.SemaphoreType.DMA
    arrays = [a.reshape(flat) for a in (initial_heat, diffusivity_ratio, forcing_term)]
    swaps = lax.axis_size("lev") == 2 and 3 <= height and 3 * height + 2 < 4 * STEPS
    swaps = swaps and depth % 4 == 0 and width % (2 * XBLOCK) == 0
    sizes = (depth, width, height)
    common = dict(out_shape=(jax.ShapeDtypeStruct(flat, f32),) * 2, out_specs=(anywhere,) * 2)
    inputs = [pl.BlockSpec(memory_space=pltpu.VMEM)] * 2
    if swaps:
        heat, scored, far, near, seam_rows, moments = swap(sizes, arrays)
        far = lax.ppermute(far, "lev", [(0, 1), (1, 0)])
        parts = min(4, depth)
        in_hbm = pl.BlockSpec(memory_space=pltpu.HBM)
        score, end = pl.pallas_call(
            functools.partial(copy_kernel, parts), out_shape=common["out_shape"], out_specs=(in_hbm,) * 2,
            in_specs=inputs, scratch_shapes=[dma((2, parts))],
            cost_estimate=pl.CostEstimate(flops=60000000, bytes_accessed=4 * heat.nbytes, transcendentals=0),
            compiler_params=pltpu.CompilerParams(vmem_limit_bytes=8 * 1024 * 1024),
            name="emit",
        )(heat, scored)
        taken = seam_rows.shape[0]
        score, end = pl.pallas_call(
            functools.partial(seam_kernel, (width, height, (depth - taken) // 2)),
            out_shape=common["out_shape"], out_specs=(in_hbm,) * 2,
            in_specs=[pl.BlockSpec(memory_space=pltpu.VMEM)] * 4 + [in_hbm] * 2,
            scratch_shapes=[pltpu.VMEM(seam_rows.shape, f32)] * 2 + [dma((2, taken))],
            input_output_aliases={4: 0, 5: 1},
            compiler_params=pltpu.CompilerParams(vmem_limit_bytes=8 * 1024 * 1024),
            name="seam",
        )(far, near, seam_rows, moments, score, end)
    else:
        parts = min(8, depth)
        score, end = pl.pallas_call(
            functools.partial(score_kernel, parts), **common, in_specs=inputs,
            scratch_shapes=[pltpu.VMEM(flat, f32), dma((parts,)), dma(())],
            compiler_params=pltpu.CompilerParams(vmem_limit_bytes=24 * 1024 * 1024),
            name="score",
        )(*march(sizes, arrays))
    return score.reshape(initial_heat.shape), end.reshape(initial_heat.shape)


def solution(mesh):
    placed = P("lat", "lon", "lev", None)
    return jax.shard_map(
        local, mesh=mesh, in_specs=(placed,) * 3, out_specs=(placed,) * 2, check_vma=False
    )
```

```python
import functools

import jax
import jax.numpy as jnp
from jax import lax
from jax.experimental import pallas as pl
from jax.experimental.pallas import tpu as pltpu
from jax.sharding import PartitionSpec as P

STEPS = 4
PAD = 8
XBLOCK = 32
XCELLS = 16
MESH = pl.DeviceIdType.MESH


def march_kernel(
    sizes, chunks, rows,
    heat_in, ratio_in, forcing_in, raw, moments_out,
    field, ratio, forcing, xsend, xrecv, stats,
    load_heat, load_ratio, load_forcing,
    zsend_sem, zrecv_sem, xsend_sem, xrecv_sem, ysend_sem, yrecv_sem, stat_send, stat_recv,
):
    depth, width, height = sizes
    inner = pl.ds(PAD, width)
    places = {axis: lax.axis_index(axis) for axis in ("lat", "lon", "lev")}
    counts = {axis: lax.axis_size(axis) for axis in ("lat", "lon", "lev")}

    def beside(axis, offset):
        return {axis: lax.rem(places[axis] + offset + counts[axis], counts[axis])}

    def rows_of(c):
        return pl.ds(c * rows, rows)

    def load(c):
        return [
            pltpu.make_async_copy(source.at[rows_of(c)], target.at[rows_of(c)], sem.at[c])
            for source, target, sem in (
                (heat_in, raw, load_heat), (ratio_in, ratio, load_ratio), (forcing_in, forcing, load_forcing),
            )
        ]

    def zcopy(side, p, c):
        span = pl.ds(1 + c * rows, rows)
        return pltpu.make_async_remote_copy(
            src_ref=field.at[p, (1, height)[side], span, inner],
            dst_ref=field.at[p, (height + 1, 0)[side], span, inner],
            send_sem=zsend_sem.at[side, p, c], recv_sem=zrecv_sem.at[1 - side, p, c],
            device_id=beside("lev", (-1, 1)[side]), device_id_type=MESH,
        )

    def xcopy(side, p, c):
        return pltpu.make_async_remote_copy(
            src_ref=xsend.at[side, p, c], dst_ref=xrecv.at[1 - side, p, c],
            send_sem=xsend_sem.at[side, p, c], recv_sem=xrecv_sem.at[1 - side, p, c],
            device_id=beside("lon", (-1, 1)[side]), device_id_type=MESH,
        )

    def ycopy(side, p):
        return pltpu.make_async_remote_copy(
            src_ref=field.at[p, pl.ds(1, height), (1, depth)[side], inner],
            dst_ref=field.at[p, pl.ds(1, height), (depth + 1, 0)[side], inner],
            send_sem=ysend_sem.at[side, p], recv_sem=yrecv_sem.at[1 - side, p],
            device_id=beside("lat", (-1, 1)[side]), device_id_type=MESH,
        )

    def stat_copy(offset, c):
        return pltpu.make_async_remote_copy(
            src_ref=stats.at[0, c], dst_ref=stats.at[offset, c],
            send_sem=stat_send.at[offset - 1, c], recv_sem=stat_recv.at[offset - 1, c],
            device_id=beside("lon", offset), device_id_type=MESH,
        )

    def send(p, c):
        for side, end in ((0, 0), (1, chunks - 1)):
            @pl.when(c == end)
            def _():
                ycopy(side, p).start()
        for side in (0, 1):
            zcopy(side, p, c).start()
        for side in (0, 1):
            xcopy(side, p, c).start()

    def sent(p, c):
        for side, end in ((0, 0), (1, chunks - 1)):
            @pl.when(c == end)
            def _():
                ycopy(side, p).wait_send()
        for side in (0, 1):
            zcopy(side, p, c).wait_send()
            xcopy(side, p, c).wait_send()

    def arrived(p, c):
        for side, end in ((1, 0), (0, chunks - 1)):
            @pl.when(c == end)
            def _():
                ycopy(side, p).wait_recv()
        for side in (0, 1):
            xcopy(side, p, c).wait_recv()
        for side in (0, 1):
            zcopy(side, p, c).wait_recv()

    def pack(p, c, i):
        for z in range(height):
            for side, x in ((0, PAD), (1, PAD + width - 1)):
                xsend[side, p, c, pl.ds(i * height + z, 1), :] = field[p, z + 1, c * rows + i + 1, pl.ds(x, 1), :]

    def start_loads(c, carry):
        load(c)[0].start()
        return carry

    def start_others(c, carry):
        for copy in load(c)[1:]:
            copy.start()
        return carry

    barrier = pltpu.get_barrier_semaphore()
    greeted = [beside("lev", -1), beside("lev", 1), beside("lat", -1), beside("lat", 1)]
    greeted += [beside("lon", offset) for offset in range(1, counts["lon"])]
    for device in greeted:
        pl.semaphore_signal(barrier, inc=1, device_id=device, device_id_type=MESH)
    lax.fori_loop(0, chunks, start_loads, 0)

    def unpack(c):
        load(c)[0].wait()

        def row(i, carry):
            y = c * rows + i
            for z in range(height):
                field[0, z + 1, y + 1, inner, :] = raw[y, pl.ds(z, width, stride=height), :]
            pack(0, c, i)
            return carry

        lax.fori_loop(0, rows, row, 0)

    def unpack_send(c, carry):
        unpack(c)
        send(0, c)
        return carry

    unpack(0)
    pl.semaphore_wait(barrier, len(greeted))
    send(0, 0)
    lax.fori_loop(0, chunks, start_others, 0)
    lax.fori_loop(1, chunks, unpack_send, 0)

    def combine(c):
        for offset in range(1, counts["lon"]):
            stat_copy(offset, c).wait_recv()
        means = [stats[offset, c, 0] for offset in range(counts["lon"])]
        mean = sum(means[1:], means[0]) * (1.0 / counts["lon"])
        squares = sum([stats[offset, c, 1] for offset in range(1, counts["lon"])], stats[0, c, 1])
        apart = sum([(other - mean) * (other - mean) for other in means[1:]], (means[0] - mean) * (means[0] - mean))
        variance = (squares + width * apart) * (1.0 / (width * counts["lon"]))
        scale = lax.rsqrt(variance + 0.0001)
        for i in range(rows):
            for half in range(2):
                for kind, values in ((0, mean), (1, scale)):
                    moments_out[kind, c * rows + i, pl.ds(half * height, height), :] = values[i * height:(i + 1) * height]
        for offset in range(1, counts["lon"]):
            stat_copy(offset, c).wait_send()
        sent((STEPS - 1) % 2, c)

    def step(s, carry):
        p = lax.rem(s, 2)
        q = 1 - p

        def chunk(c, carry):
            @pl.when(s == 0)
            def _():
                for copy in load(c)[1:]:
                    copy.wait()

            @pl.when(s >= 1)
            def _():
                sent(q, c)

            arrived(p, c)

            def row(i, carry):
                y = c * rows + i
                for z in range(height):
                    for side, x in ((0, PAD - 1), (1, PAD + width)):
                        field[p, z + 1, y + 1, pl.ds(x, 1), :] = xrecv[side, p, c, pl.ds(i * height + z, 1), :]
                for x in range(0, width, XBLOCK):
                    here = pl.ds(PAD + x, XBLOCK)
                    planes = [field[p, z, y + 1, here, :] for z in range(height + 2)]
                    for z in range(height):
                        middle = planes[z + 1]
                        spread = (
                            field[p, z + 1, y, here, :] + field[p, z + 1, y + 2, here, :]
                            + field[p, z + 1, y + 1, pl.ds(PAD + x - 1, XBLOCK), :]
                            + field[p, z + 1, y + 1, pl.ds(PAD + x + 1, XBLOCK), :]
                            + planes[z] + planes[z + 2] - 6.0 * middle
                        )
                        cells = pl.ds(x * height + z, XBLOCK, stride=height)
                        field[q, z + 1, y + 1, here, :] = middle + ratio[y, cells, :] * spread + forcing[y, cells, :]
                pack(q, c, i)
                return carry

            lax.fori_loop(0, rows, row, 0)

            @pl.when(s < STEPS - 1)
            def _():
                send(q, c)

            @pl.when(s == STEPS - 1)
            def _():
                def finish(i, carry):
                    y = c * rows + i
                    for z in range(height):
                        line = field[q, z + 1, y + 1, inner, :]
                        raw[y, pl.ds(z, width, stride=height), :] = line
                        mean = jnp.sum(line, axis=0, keepdims=True) * (1.0 / width)
                        centred = line - mean
                        stats[0, c, 0, pl.ds(i * height + z, 1), :] = mean
                        stats[0, c, 1, pl.ds(i * height + z, 1), :] = jnp.sum(centred * centred, axis=0, keepdims=True)
                    return carry

                lax.fori_loop(0, rows, finish, 0)
                for offset in range(1, counts["lon"]):
                    stat_copy(offset, c).start()

                @pl.when(c >= 1)
                def _():
                    combine(c - 1)

            return carry

        lax.fori_loop(0, chunks, chunk, 0)
        return carry

    lax.fori_loop(0, STEPS, step, 0)


    combine(chunks - 1)


def swap_kernel(
    sizes, rows,
    heat_in, ratio_in, forcing_in, heat_out, score_out, seam_far, seam_near, seam_rows, moments,
    field, rim, core, ratio_far, forcing_far, back, stage,
    xsend, xrecv, csend, crecv, ends, ends_far, stats,
    load_sem, send_sem, ysend_sem, scale_recv, rim_recv, inner_recv, ends_recv, outer_recv,
    xrecv_sem, yrecv_sem, cxrecv_sem, cyrecv_sem, stat_recv, seam_sem, hello,
):
    depth, width, height = sizes
    half, planes, inside = width // 2, 2 * height, height - 2
    chunks = depth // rows
    units = chunks // 2
    sent_at = height * half
    inner = pl.ds(PAD, half)
    forcing, ratio = heat_out, score_out
    places = {axis: lax.axis_index(axis) for axis in ("lat", "lon", "lev")}
    counts = {axis: lax.axis_size(axis) for axis in ("lat", "lon", "lev")}
    upper = places["lev"] == 1

    def beside(axis, offset):
        return {axis: lax.rem(places[axis] + offset + counts[axis], counts[axis])}

    def rows_of(c):
        return pl.ds(c * rows, rows)

    def chunk_of(u, side):
        return u + side * (chunks - 1 - 2 * u)

    def first_lanes(shape):
        return lax.broadcasted_iota(jnp.int32, shape, 1) < shape[1] // 2

    def turned(values):
        return pltpu.roll(values, values.shape[1] // 2, 1)

    def remote(source, target, send_sem, recv_sem, device):
        return pltpu.make_async_remote_copy(
            src_ref=source, dst_ref=target, send_sem=send_sem, recv_sem=recv_sem,
            device_id=device, device_id_type=MESH,
        )

    partner = beside("lev", 1)

    def load(kind, c, slot):
        source = (heat_in, ratio_in, forcing_in)[kind]
        return pltpu.make_async_copy(source.at[rows_of(c)], stage.at[kind, slot], load_sem.at[kind, slot])

    def ratio_copy(u, span):
        cells = pl.ds(sent_at, sent_at)
        return remote(ratio.at[span, cells], ratio_far.at[span], send_sem.at[0], scale_recv.at[u], partner)

    def forcing_copy(u, span):
        cells = pl.ds(sent_at, sent_at)
        return remote(forcing.at[span, cells], forcing_far.at[span], send_sem.at[1], scale_recv.at[u], partner)

    def rim_copy(end, u, c):
        return remote(
            rim.at[end, rows_of(c)], field.at[0, (height, planes - 1)[end], pl.ds(1 + c * rows, rows), inner],
            send_sem.at[2], rim_recv.at[u], partner,
        )

    def inner_copy(u, c):
        return remote(
            field.at[STEPS % 2, pl.ds(height + 1, inside), pl.ds(1 + c * rows, rows), inner],
            back.at[pl.ds(1, inside), rows_of(c)], send_sem.at[3], inner_recv.at[u], partner,
        )

    def outer_copy(end, u, c):
        return remote(
            field.at[STEPS % 2, (height, planes - 1)[end], pl.ds(1 + c * rows, rows), inner],
            back.at[(0, height - 1)[end], rows_of(c)], send_sem.at[9], outer_recv.at[u], partner,
        )

    def ends_copy(u):
        return remote(ends.at[1, u], ends_far.at[u], send_sem.at[8], ends_recv.at[u], partner)

    def xcopy(level, side, u):
        return remote(
            xsend.at[level, u, side], xrecv.at[level, u, 1 - side],
            send_sem.at[4], xrecv_sem.at[lax.rem(level, 2), u], beside("lon", (-1, 1)[side]),
        )

    def ycopy(level, side):
        p = lax.rem(level, 2)
        return remote(
            field.at[p, :, (1, depth)[side], inner], field.at[p, :, (depth + 1, 0)[side], inner],
            ysend_sem.at[p], yrecv_sem.at[p], beside("lat", (-1, 1)[side]),
        )

    def core_xcopy(side, u):
        return remote(
            csend.at[u, side], crecv.at[u, 1 - side], send_sem.at[5], cxrecv_sem.at[u], beside("lon", (-1, 1)[side])
        )

    def core_ycopy(side):
        return remote(
            core.at[:, (1, depth)[side], inner], core.at[:, (depth + 1, 0)[side], inner],
            send_sem.at[6], cyrecv_sem.at[0], beside("lat", (-1, 1)[side]),
        )

    def stat_copy(offset, u):
        return remote(
            stats.at[0, u], stats.at[offset, u], send_sem.at[7], stat_recv.at[lax.rem(u, 2)], beside("lon", offset)
        )

    def wait_all(ref, sem):
        pltpu.make_async_copy(ref, ref, sem).wait()

    def over(count, body):
        def step(i, carry):
            body(i)
            return carry

        lax.fori_loop(0, count, step, 0)


    def split(kind, slot, i, z, x):
        low = stage[kind, slot, i, pl.ds(x * height + z, XBLOCK, stride=height), :]
        high = stage[kind, slot, i, pl.ds((half + x) * height + z, XBLOCK, stride=height), :]
        mask = first_lanes(low.shape)
        one = jnp.where(mask, low, turned(high))
        two = jnp.where(mask, turned(low), high)
        return jnp.where(upper, two, one), jnp.where(upper, one, two)

    def split_into(target, kind, slot, c):
        def row(i):
            for z in range(height):
                for x in range(0, half, XBLOCK):
                    kept, sent = split(kind, slot, i, z, x)
                    target[c * rows + i, pl.ds(z * half + x, XBLOCK), :] = kept
                    target[c * rows + i, pl.ds(sent_at + z * half + x, XBLOCK), :] = sent

        over(rows, row)

    def split_heat(u, slot, c):
        def row(i):
            y = c * rows + i
            for z in range(height):
                for x in range(0, half, XBLOCK):
                    here = pl.ds(PAD + x, XBLOCK)
                    kept, sent = split(0, slot, i, z, x)
                    field[0, z, y + 1, here, :] = kept
                    if 0 < z < height - 1:
                        core[z - 1, y + 1, here, :] = sent
                        field[0, height + z, y + 1, here, :] = jnp.zeros_like(sent)
                    else:
                        rim[min(z, 1), y, pl.ds(x, XBLOCK), :] = sent
            for side, x in ((0, PAD), (1, PAD + half - 1)):
                csend[u, side, slot * rows + i] = jnp.zeros(csend.shape[3:], csend.dtype)
                for n in range(inside):
                    csend[u, side, slot * rows + i, pl.ds(n, 1), :] = core[n, y + 1, pl.ds(x, 1), :]

        over(rows, row)

    def prepare(u, side):
        c = chunk_of(u, side)
        load(1, c, side).wait()
        split_into(ratio, 1, side, c)

        @pl.when((u == 0) & (side == 0) & jnp.logical_not(upper))
        def _():
            pl.semaphore_wait(barrier, 1)
            pl.semaphore_signal(hello.at[0], inc=1, device_id=partner, device_id_type=MESH)

        @pl.when((u == 0) & (side == 0) & upper)
        def _():
            pl.semaphore_wait(hello.at[0], 1)
            for device in around:
                pl.semaphore_signal(barrier, inc=1, device_id=device, device_id_type=MESH)

        ratio_copy(u, rows_of(c)).start()
        load(0, c, side).wait()
        split_heat(u, side, c)
        for end in (0, 1):
            rim_copy(end, u, c).start()

        @pl.when((u == 0) & (side == 1) & upper)
        def _():
            pl.semaphore_wait(barrier, len(around))
            pl.semaphore_signal(hello.at[1], inc=1, device_id=partner, device_id_type=MESH)

        @pl.when((u == 0) & (side == 1) & jnp.logical_not(upper))
        def _():
            pl.semaphore_wait(hello.at[1], 1)

        @pl.when(side == 1)
        def _():
            for end in (0, 1):
                core_xcopy(end, u).start()

        @pl.when((side == 1) & (u == 0))
        def _():
            for end in (0, 1):
                core_ycopy(end).start()

        load(2, c, side).wait()
        split_into(forcing, 2, side, c)

        @pl.when(u < units - 1)
        def _():
            for kind in (1, 0, 2):
                load(kind, chunk_of(u + 1, side), side).start()

    def correct(u, side):
        c = chunk_of(u, side)

        @pl.when(side == 0)
        def _():
            wait_all(crecv.at[u], cxrecv_sem.at[u])

        @pl.when((side == 0) & (u == 0))
        def _():
            wait_all(core.at[:, pl.ds(0, 2), inner], cyrecv_sem.at[0])

        def row(i):
            y = c * rows + i
            k = side * rows + i
            mask = first_lanes(crecv.shape[3:])
            left = turned(jnp.where(mask, csend[u, 1, k], crecv[u, 0, k]))
            right = turned(jnp.where(mask, crecv[u, 1, k], csend[u, 0, k]))
            for n in range(inside):
                core[n, y + 1, pl.ds(PAD - 1, 1), :] = left[n:n + 1]
                core[n, y + 1, pl.ds(PAD + half, 1), :] = right[n:n + 1]
            for x in range(0, half, XBLOCK):
                here = pl.ds(PAD + x, XBLOCK)
                middles = {n: core[n, y + 1, here, :] for n in range(inside)}
                for z in range(height):
                    parts = [middles[n] for n in (z - 2, z) if n in middles]
                    n = z - 1
                    if n in middles:
                        parts += [
                            core[n, y, here, :] + core[n, y + 2, here, :],
                            core[n, y + 1, pl.ds(PAD + x - 1, XBLOCK), :] + core[n, y + 1, pl.ds(PAD + x + 1, XBLOCK), :],
                            -6.0 * middles[n],
                        ]
                    cells = pl.ds(sent_at + z * half + x, XBLOCK)
                    forcing[y, cells, :] = forcing[y, cells, :] + ratio[y, cells, :] * sum(parts[1:], parts[0])

        over(rows, row)
        forcing_copy(u, rows_of(c)).start()

    barrier = pltpu.get_barrier_semaphore()
    around = [beside("lat", -1), beside("lat", 1)]
    around += [beside("lon", offset) for offset in range(1, counts["lon"])]

    @pl.when(upper)
    def _():
        pl.semaphore_signal(barrier, inc=1, device_id=partner, device_id_type=MESH)

    for side in (0, 1):
        for kind in (1, 0, 2):
            load(kind, chunk_of(0, side), side).start()

    def inputs(u):
        @pl.when(u < units)
        def _():
            over(2, lambda side: prepare(u, side))

        @pl.when(u > 0)
        def _():
            over(2, lambda side: correct(u - 1, side))

    over(units + 1, inputs)


    def publish(level, u):
        p = lax.rem(level, 2)

        def row(k):
            y = row_of(u, k)
            for side, x in ((0, PAD), (1, PAD + half - 1)):
                for z in range(planes):
                    xsend[level, u, side, k, pl.ds(z, 1), :] = field[p, z, y + 1, pl.ds(x, 1), :]

        over(2 * rows, row)
        for side in (0, 1):
            xcopy(level, side, u).start()

        @pl.when(u == 0)
        def _():
            for side in (0, 1):
                ycopy(level, side).start()

    def arrive(u):
        wait_all(ratio_far.at[pl.ds(0, 4 * rows)], scale_recv.at[u])
        wait_all(rim.at[:, pl.ds(0, 2 * rows)], rim_recv.at[u])
        publish(0, u)

    def advance(s, u):
        level = s - 1
        p = lax.rem(level, 2)
        q = 1 - p

        @pl.when(u == 0)
        def _():
            wait_all(field.at[p, :, pl.ds(0, 2), inner], yrecv_sem.at[p])

        @pl.when((u == 0) & (s >= 2))
        def _():
            wait_all(field.at[q, :, pl.ds(0, 2), inner], ysend_sem.at[q])

        wait_all(xrecv.at[level, u], xrecv_sem.at[p, u])
        over(2, lambda side: march_rows(level, p, q, u, side))

        @pl.when(s < STEPS)
        def _():
            publish(s, u)

        @pl.when(s == STEPS)
        def _():
            for side in (0, 1):
                inner_copy(u, chunk_of(u, side)).start()
            over(2 * rows, lambda k: end_moments(u, k))
            ends_copy(u).start()

        @pl.when((s == STEPS) & (u > 0))
        def _():
            for side in (0, 1):
                for end in (0, 1):
                    outer_copy(end, u - 1, chunk_of(u - 1, side)).start()

        @pl.when((s == STEPS) & (u == units - 1))
        def _():
            over(2 * rows, lambda k: keep_seam(u, k))
            for end in (0, 1):
                seam_copy(end).start()

    def keep_seam(u, k):
        for end in (0, 1):
            seam_near[end, k] = field[STEPS % 2, end * (height - 1), row_of(u, k) + 1, inner, :]

    def seam_copy(end):
        span = pl.ds((units - 1) * rows + 1, 2 * rows)
        plane = field.at[STEPS % 2, (height, planes - 1)[end], span, inner]
        return pltpu.make_async_copy(plane, seam_far.at[end], seam_sem.at[end])

    def row_of(u, k):
        return chunk_of(u, k // rows) * rows + lax.rem(k, rows)

    def end_moments(u, k):
        for whose in (0, 1):
            for end in (0, 1):
                line = field[STEPS % 2, whose * height + end * (height - 1), row_of(u, k) + 1, inner, :]
                mean = both_halves(jnp.sum(line, axis=0, keepdims=True)) * (1.0 / width)
                centred = line - mean
                squares = both_halves(jnp.sum(centred * centred, axis=0, keepdims=True))
                ends[whose, u, pl.ds(2 * k + end, 1), :] = jnp.where(first_lanes(mean.shape), mean, squares)

    def both_halves(sums):
        tall = jnp.broadcast_to(sums, (8, sums.shape[1]))
        return (tall + turned(tall))[:1]

    def march_rows(level, p, q, u, side):
        c = chunk_of(u, side)

        def row(i):
            y = c * rows + i
            k = side * rows + i
            mask = first_lanes(xrecv.shape[4:])
            left = turned(jnp.where(mask, xsend[level, u, 1, k], xrecv[level, u, 0, k]))
            right = turned(jnp.where(mask, xrecv[level, u, 1, k], xsend[level, u, 0, k]))
            for z in range(planes):
                field[p, z, y + 1, pl.ds(PAD - 1, 1), :] = left[z:z + 1]
                field[p, z, y + 1, pl.ds(PAD + half, 1), :] = right[z:z + 1]
            for x in range(0, half, XCELLS):
                here = pl.ds(PAD + x, XCELLS)
                middles = [field[p, z, y + 1, here, :] for z in range(planes)]
                for z in range(planes):
                    middle = middles[z]
                    spread = (
                        field[p, z, y, here, :] + field[p, z, y + 2, here, :]
                        + field[p, z, y + 1, pl.ds(PAD + x - 1, XCELLS), :]
                        + field[p, z, y + 1, pl.ds(PAD + x + 1, XCELLS), :]
                        + middles[z - 1] + middles[(z + 1) % planes]
                        - 6.0 * middle
                    )
                    if z < height:
                        cells = pl.ds(z * half + x, XCELLS)
                        scale, source = ratio[y, cells, :], forcing[y, cells, :]
                    else:
                        cells = pl.ds((z - height) * half + x, XCELLS)
                        scale, source = ratio_far[y, cells, :], forcing_far[y, cells, :]
                    field[q, z, y + 1, here, :] = middle + scale * spread + source

        over(rows, row)

    def wave(w):
        @pl.when(w < units)
        def _():
            arrive(w)

        def step(i):
            u = w - 1 - i

            @pl.when((u >= 0) & (u < units))
            def _():
                advance(i + 1, u)

        over(STEPS, step)

    over(units + STEPS, wave)


    def join(y, z, x):
        here = pl.ds(PAD + x, XBLOCK)
        kept, other = field[STEPS % 2, z, y + 1, here, :], back[z, y, pl.ds(x, XBLOCK), :]
        if 0 < z < height - 1:
            other = other + core[z - 1, y + 1, here, :]
        mask = first_lanes(kept.shape)
        one, two = jnp.where(upper, other, kept), jnp.where(upper, kept, other)
        low = jnp.where(mask, one, turned(two))
        high = jnp.where(mask, turned(one), two)
        heat_out[y, pl.ds(x * height + z, XBLOCK, stride=height), :] = low
        heat_out[y, pl.ds((half + x) * height + z, XBLOCK, stride=height), :] = high
        return [low, high]

    def join_inner(u, k):
        y = row_of(u, k)
        for z in range(1, height - 1):
            line = jnp.concatenate(sum([join(y, z, x) for x in range(0, half, XBLOCK)], []), axis=0)
            mean = jnp.sum(line, axis=0, keepdims=True) * (1.0 / width)
            centred = line - mean
            stats[0, u, 0, pl.ds(k * height + z, 1), :] = mean
            stats[0, u, 1, pl.ds(k * height + z, 1), :] = jnp.sum(centred * centred, axis=0, keepdims=True)

    def share_moments(u):
        mask = first_lanes(ends_far.shape[1:])
        mine, far = ends[0, u], ends_far[u]
        one, two = jnp.where(upper, far, mine), jnp.where(upper, mine, far)
        for kind, lines in ((0, jnp.where(mask, one, turned(two))), (1, jnp.where(mask, turned(one), two))):
            for k in range(2 * rows):
                for end in (0, 1):
                    at = k * height + end * (height - 1)
                    stats[0, u, kind, pl.ds(at, 1), :] = lines[2 * k + end:2 * k + end + 1]
        for offset in range(1, counts["lon"]):
            stat_copy(offset, u).start()

    def combine(u):
        wait_all(stats.at[pl.ds(1, counts["lon"] - 1), u], stat_recv.at[lax.rem(u, 2)])
        means = [stats[offset, u, 0] for offset in range(counts["lon"])]
        mean = sum(means[1:], means[0]) * (1.0 / counts["lon"])
        squares = sum([stats[offset, u, 1] for offset in range(1, counts["lon"])], stats[0, u, 1])
        apart = sum([(other - mean) * (other - mean) for other in means[1:]], (means[0] - mean) * (means[0] - mean))
        variance = (squares + width * apart) * (1.0 / (width * counts["lon"]))
        scale = lax.rsqrt(variance + 0.0001)
        for k in range(2 * rows):
            for copy in range(2):
                for kind, values in ((0, mean), (1, scale)):
                    moments[u, kind, k, pl.ds(copy * height, height), :] = values[k * height:(k + 1) * height]

    def join_outer(u, k):
        y = row_of(u, k)
        for z in (0, height - 1):
            for x in range(0, half, XBLOCK):
                join(y, z, x)
        values = heat_out[y]
        tall = values.reshape(half, 2 * height, values.shape[1])
        score_out[y] = ((tall - moments[u, 0, k][None]) * moments[u, 1, k][None]).reshape(values.shape)

    wait_all(ratio.at[:, pl.ds(sent_at, sent_at)], send_sem.at[0])
    wait_all(forcing.at[:, pl.ds(sent_at, sent_at)], send_sem.at[1])

    def finish(u):
        wait_all(back.at[pl.ds(0, inside), pl.ds(0, 2 * rows)], inner_recv.at[u])
        over(2 * rows, lambda k: join_inner(u, k))
        wait_all(ends_far.at[u], ends_recv.at[u])
        share_moments(u)
        combine(u)

        @pl.when(u > 0)
        def _():
            wait_all(back.at[pl.ds(0, 2), pl.ds(0, 2 * rows)], outer_recv.at[u - 1])
            over(2 * rows, lambda k: join_outer(u - 1, k))

    over(units, finish)

    def seam_row(k):
        seam_rows[k] = heat_out[row_of(units - 1, k)]

    over(2 * rows, seam_row)
    wait_all(rim, send_sem.at[2])
    for end in (0, 1):
        seam_copy(end).wait()
    wait_all(field.at[STEPS % 2, pl.ds(height + 1, inside), pl.ds(1, depth), inner], send_sem.at[3])
    wait_all(field.at[STEPS % 2, pl.ds(height, 2), pl.ds(1, depth - 2 * rows), inner], send_sem.at[9])
    wait_all(xsend, send_sem.at[4])
    wait_all(csend, send_sem.at[5])
    wait_all(core.at[:, pl.ds(0, 2), inner], send_sem.at[6])
    wait_all(field.at[(STEPS - 1) % 2, :, pl.ds(0, 2), inner], ysend_sem.at[(STEPS - 1) % 2])
    wait_all(stats.at[pl.ds(1, counts["lon"] - 1)], send_sem.at[7])
    wait_all(ends_far, send_sem.at[8])


def swap(sizes, arrays):
    depth, width, height = sizes
    members = arrays[0].shape[-1]
    rows = 2
    chunks = depth // rows
    units = chunks // 2
    half = width // 2
    lon = lax.axis_size("lon")
    flat = (depth, width * height, members)
    f32 = jnp.float32
    dma = pltpu.SemaphoreType.DMA
    vmem = lambda *shape: pltpu.VMEM((*shape, members), f32)
    return pl.pallas_call(
        functools.partial(swap_kernel, sizes, rows),
        out_shape=(
            pltpu.VMEM(flat, f32), pltpu.VMEM(flat, f32),
            jax.ShapeDtypeStruct((2, 2 * rows, half, members), f32), vmem(2, 2 * rows, half),
            vmem(2 * rows, width * height), vmem(units, 2, 2 * rows, 2 * height),
        ),
        in_specs=[pl.BlockSpec(memory_space=pl.ANY)] * 3,
        out_specs=tuple(pl.BlockSpec(memory_space=pltpu.HBM if i == 2 else pltpu.VMEM) for i in range(6)),
        scratch_shapes=[
            vmem(2, 2 * height, depth + 2, half + 2 * PAD),
            vmem(2, depth, half),
            vmem(height - 2, depth + 2, half + 2 * PAD),
            vmem(depth, half * height),
            vmem(depth, half * height),
            vmem(height, depth, half),
            vmem(3, 2, rows, width * height),
            vmem(STEPS, units, 2, 2 * rows, 2 * height), vmem(STEPS, units, 2, 2 * rows, 2 * height),
            vmem(units, 2, 2 * rows, 8), vmem(units, 2, 2 * rows, 8),
            vmem(2, units, 4 * rows), vmem(units, 4 * rows),
            vmem(lon, units, 2, 2 * rows * height),
            dma((3, 2)), dma((10,)), dma((2,)),
            dma((units,)), dma((units,)), dma((units,)), dma((units,)), dma((units,)),
            dma((2, units)), dma((2,)), dma((units,)), dma((1,)), dma((2,)), dma((2,)), pltpu.SemaphoreType.REGULAR((2,)),
        ],
        compiler_params=pltpu.CompilerParams(
            collective_id=1, has_side_effects=True, vmem_limit_bytes=46 * 1024 * 1024
        ),
        name="swap",
    )(*arrays)


def march(sizes, arrays):
    depth, width, height = sizes
    members = arrays[0].shape[-1]
    rows = 2
    chunks = depth // rows
    lon = lax.axis_size("lon")
    flat = (depth, width * height, members)
    f32 = jnp.float32
    anywhere = pl.BlockSpec(memory_space=pl.ANY)
    dma = pltpu.SemaphoreType.DMA
    return pl.pallas_call(
        functools.partial(march_kernel, (depth, width, height), chunks, rows),
        out_shape=(pltpu.VMEM(flat, f32), pltpu.VMEM((2, depth, 2 * height, members), f32)),
        in_specs=[anywhere] * 3,
        out_specs=(pl.BlockSpec(memory_space=pltpu.VMEM),) * 2,
        scratch_shapes=[
            pltpu.VMEM((2, height + 2, depth + 2, width + 2 * PAD, members), f32),
            pltpu.VMEM(flat, f32),
            pltpu.VMEM(flat, f32),
            pltpu.VMEM((2, 2, chunks, rows * height, members), f32),
            pltpu.VMEM((2, 2, chunks, rows * height, members), f32),
            pltpu.VMEM((lon, chunks, 2, rows * height, members), f32),
            dma((chunks,)), dma((chunks,)), dma((chunks,)),
            dma((2, 2, chunks)), dma((2, 2, chunks)),
            dma((2, 2, chunks)), dma((2, 2, chunks)),
            dma((2, 2)), dma((2, 2)),
            dma((lon - 1, chunks)), dma((lon - 1, chunks)),
        ],
        compiler_params=pltpu.CompilerParams(
            collective_id=0, has_side_effects=True, vmem_limit_bytes=48 * 1024 * 1024
        ),
        name="march",
    )(*arrays)


def copy_kernel(chunks, heat, scored, score, end, sem):
    rows = heat.shape[0] // chunks
    copies = []
    for c in range(chunks):
        span = pl.ds(c * rows, rows)
        copies.append(pltpu.make_async_copy(heat.at[span], end.at[span], sem.at[0, c]))
        copies.append(pltpu.make_async_copy(scored.at[span], score.at[span], sem.at[1, c]))
    for copy in copies:
        copy.start()
    for copy in copies:
        copy.wait()


def seam_kernel(sizes, far, near, rows_in, moments, score_in, end_in, score, end, joined, scored, sem):
    width, height, first = sizes
    half = width // 2
    unit = moments.shape[0] - 1
    upper = lax.axis_index("lev") == 1

    def out_copies(k):
        return [
            pltpu.make_async_copy(source.at[k], target.at[first + k], sem.at[kind, k])
            for kind, (source, target) in enumerate(((joined, end), (scored, score)))
        ]

    def row(k, carry):
        joined[k] = rows_in[k]
        for side, z in ((0, 0), (1, height - 1)):
            for x in range(0, half, XBLOCK):
                kept, other = near[side, k, pl.ds(x, XBLOCK), :], far[side, k, pl.ds(x, XBLOCK), :]
                mask = lax.broadcasted_iota(jnp.int32, kept.shape, 1) < kept.shape[1] // 2
                one, two = jnp.where(upper, other, kept), jnp.where(upper, kept, other)
                turn = kept.shape[1] // 2
                joined[k, pl.ds(x * height + z, XBLOCK, stride=height), :] = jnp.where(mask, one, pltpu.roll(two, turn, 1))
                joined[k, pl.ds((half + x) * height + z, XBLOCK, stride=height), :] = jnp.where(
                    mask, pltpu.roll(one, turn, 1), two
                )
        out_copies(k)[0].start()
        values = joined[k]
        tall = values.reshape(half, 2 * height, values.shape[1])
        scored[k] = ((tall - moments[unit, 0, k][None]) * moments[unit, 1, k][None]).reshape(values.shape)
        out_copies(k)[1].start()
        return carry

    lax.fori_loop(0, joined.shape[0], row, 0)
    for k in range(joined.shape[0]):
        for copy in out_copies(k):
            copy.wait()


def score_kernel(chunks, heat, moments, score, end, scaled, score_sem, end_sem):
    rows = heat.shape[0] // chunks
    finish = pltpu.make_async_copy(heat, end, end_sem)
    finish.start()

    def out_copy(c):
        span = pl.ds(c * rows, rows)
        return pltpu.make_async_copy(scaled.at[span], score.at[span], score_sem.at[c])

    def chunk(c, carry):
        def row(i, carry):
            y = c * rows + i
            mean, scale = moments[0, y], moments[1, y]
            values = heat[y]
            tall = values.reshape(values.shape[0] // mean.shape[0], *mean.shape)
            scaled[y] = ((tall - mean[None]) * scale[None]).reshape(values.shape)
            return carry

        lax.fori_loop(0, rows, row, 0)
        out_copy(c).start()
        return carry

    def drain(c, carry):
        out_copy(c).wait()
        return carry

    lax.fori_loop(0, chunks, chunk, 0)
    lax.fori_loop(0, chunks, drain, 0)
    finish.wait()


def local(initial_heat, diffusivity_ratio, forcing_term):
    depth, width, height, members = initial_heat.shape
    flat = (depth, width * height, members)
    f32 = jnp.float32
    anywhere = pl.BlockSpec(memory_space=pl.ANY)
    dma = pltpu.SemaphoreType.DMA
    arrays = [a.reshape(flat) for a in (initial_heat, diffusivity_ratio, forcing_term)]
    swaps = lax.axis_size("lev") == 2 and 3 <= height and 3 * height + 2 < 4 * STEPS
    swaps = swaps and depth % 4 == 0 and width % (2 * XBLOCK) == 0
    sizes = (depth, width, height)
    common = dict(out_shape=(jax.ShapeDtypeStruct(flat, f32),) * 2, out_specs=(anywhere,) * 2)
    inputs = [pl.BlockSpec(memory_space=pltpu.VMEM)] * 2
    if swaps:
        heat, scored, far, near, seam_rows, moments = swap(sizes, arrays)
        far = lax.ppermute(far, "lev", [(0, 1), (1, 0)])
        parts = min(4, depth)
        in_hbm = pl.BlockSpec(memory_space=pltpu.HBM)
        score, end = pl.pallas_call(
            functools.partial(copy_kernel, parts), out_shape=common["out_shape"], out_specs=(in_hbm,) * 2,
            in_specs=inputs, scratch_shapes=[dma((2, parts))],
            cost_estimate=pl.CostEstimate(flops=60000000, bytes_accessed=4 * heat.nbytes, transcendentals=0),
            compiler_params=pltpu.CompilerParams(vmem_limit_bytes=8 * 1024 * 1024),
            name="emit",
        )(heat, scored)
        taken = seam_rows.shape[0]
        score, end = pl.pallas_call(
            functools.partial(seam_kernel, (width, height, (depth - taken) // 2)),
            out_shape=common["out_shape"], out_specs=(in_hbm,) * 2,
            in_specs=[pl.BlockSpec(memory_space=pltpu.VMEM)] * 4 + [in_hbm] * 2,
            scratch_shapes=[pltpu.VMEM(seam_rows.shape, f32)] * 2 + [dma((2, taken))],
            input_output_aliases={4: 0, 5: 1},
            compiler_params=pltpu.CompilerParams(vmem_limit_bytes=8 * 1024 * 1024),
            name="seam",
        )(far, near, seam_rows, moments, score, end)
    else:
        parts = min(8, depth)
        score, end = pl.pallas_call(
            functools.partial(score_kernel, parts), **common, in_specs=inputs,
            scratch_shapes=[pltpu.VMEM(flat, f32), dma((parts,)), dma(())],
            compiler_params=pltpu.CompilerParams(vmem_limit_bytes=24 * 1024 * 1024),
            name="score",
        )(*march(sizes, arrays))
    return score.reshape(initial_heat.shape), end.reshape(initial_heat.shape)


def solution(mesh):
    placed = P("lat", "lon", "lev", None)
    return jax.shard_map(
        local, mesh=mesh, in_specs=(placed,) * 3, out_specs=(placed,) * 2, check_vma=False
    )
```

```python
import functools

import jax
import jax.numpy as jnp
from jax import lax
from jax.experimental import pallas as pl
from jax.experimental.pallas import tpu as pltpu
from jax.sharding import PartitionSpec as P

STEPS = 4
PAD = 8
XBLOCK = 32
XCELLS = 16
MESH = pl.DeviceIdType.MESH


def march_kernel(
    sizes, chunks, rows,
    heat_in, ratio_in, forcing_in, raw, moments_out,
    field, ratio, forcing, xsend, xrecv, stats,
    load_heat, load_ratio, load_forcing,
    zsend_sem, zrecv_sem, xsend_sem, xrecv_sem, ysend_sem, yrecv_sem, stat_send, stat_recv,
):
    depth, width, height = sizes
    inner = pl.ds(PAD, width)
    places = {axis: lax.axis_index(axis) for axis in ("lat", "lon", "lev")}
    counts = {axis: lax.axis_size(axis) for axis in ("lat", "lon", "lev")}

    def beside(axis, offset):
        return {axis: lax.rem(places[axis] + offset + counts[axis], counts[axis])}

    def rows_of(c):
        return pl.ds(c * rows, rows)

    def load(c):
        return [
            pltpu.make_async_copy(source.at[rows_of(c)], target.at[rows_of(c)], sem.at[c])
            for source, target, sem in (
                (heat_in, raw, load_heat), (ratio_in, ratio, load_ratio), (forcing_in, forcing, load_forcing),
            )
        ]

    def zcopy(side, p, c):
        span = pl.ds(1 + c * rows, rows)
        return pltpu.make_async_remote_copy(
            src_ref=field.at[p, (1, height)[side], span, inner],
            dst_ref=field.at[p, (height + 1, 0)[side], span, inner],
            send_sem=zsend_sem.at[side, p, c], recv_sem=zrecv_sem.at[1 - side, p, c],
            device_id=beside("lev", (-1, 1)[side]), device_id_type=MESH,
        )

    def xcopy(side, p, c):
        return pltpu.make_async_remote_copy(
            src_ref=xsend.at[side, p, c], dst_ref=xrecv.at[1 - side, p, c],
            send_sem=xsend_sem.at[side, p, c], recv_sem=xrecv_sem.at[1 - side, p, c],
            device_id=beside("lon", (-1, 1)[side]), device_id_type=MESH,
        )

    def ycopy(side, p):
        return pltpu.make_async_remote_copy(
            src_ref=field.at[p, pl.ds(1, height), (1, depth)[side], inner],
            dst_ref=field.at[p, pl.ds(1, height), (depth + 1, 0)[side], inner],
            send_sem=ysend_sem.at[side, p], recv_sem=yrecv_sem.at[1 - side, p],
            device_id=beside("lat", (-1, 1)[side]), device_id_type=MESH,
        )

    def stat_copy(offset, c):
        return pltpu.make_async_remote_copy(
            src_ref=stats.at[0, c], dst_ref=stats.at[offset, c],
            send_sem=stat_send.at[offset - 1, c], recv_sem=stat_recv.at[offset - 1, c],
            device_id=beside("lon", offset), device_id_type=MESH,
        )

    def send(p, c):
        for side, end in ((0, 0), (1, chunks - 1)):
            @pl.when(c == end)
            def _():
                ycopy(side, p).start()
        for side in (0, 1):
            zcopy(side, p, c).start()
        for side in (0, 1):
            xcopy(side, p, c).start()

    def sent(p, c):
        for side, end in ((0, 0), (1, chunks - 1)):
            @pl.when(c == end)
            def _():
                ycopy(side, p).wait_send()
        for side in (0, 1):
            zcopy(side, p, c).wait_send()
            xcopy(side, p, c).wait_send()

    def arrived(p, c):
        for side, end in ((1, 0), (0, chunks - 1)):
            @pl.when(c == end)
            def _():
                ycopy(side, p).wait_recv()
        for side in (0, 1):
            xcopy(side, p, c).wait_recv()
        for side in (0, 1):
            zcopy(side, p, c).wait_recv()

    def pack(p, c, i):
        for z in range(height):
            for side, x in ((0, PAD), (1, PAD + width - 1)):
                xsend[side, p, c, pl.ds(i * height + z, 1), :] = field[p, z + 1, c * rows + i + 1, pl.ds(x, 1), :]

    def start_loads(c, carry):
        load(c)[0].start()
        return carry

    def start_others(c, carry):
        for copy in load(c)[1:]:
            copy.start()
        return carry

    barrier = pltpu.get_barrier_semaphore()
    greeted = [beside("lev", -1), beside("lev", 1), beside("lat", -1), beside("lat", 1)]
    greeted += [beside("lon", offset) for offset in range(1, counts["lon"])]
    for device in greeted:
        pl.semaphore_signal(barrier, inc=1, device_id=device, device_id_type=MESH)
    lax.fori_loop(0, chunks, start_loads, 0)

    def unpack(c):
        load(c)[0].wait()

        def row(i, carry):
            y = c * rows + i
            for z in range(height):
                field[0, z + 1, y + 1, inner, :] = raw[y, pl.ds(z, width, stride=height), :]
            pack(0, c, i)
            return carry

        lax.fori_loop(0, rows, row, 0)

    def unpack_send(c, carry):
        unpack(c)
        send(0, c)
        return carry

    unpack(0)
    pl.semaphore_wait(barrier, len(greeted))
    send(0, 0)
    lax.fori_loop(0, chunks, start_others, 0)
    lax.fori_loop(1, chunks, unpack_send, 0)

    def combine(c):
        for offset in range(1, counts["lon"]):
            stat_copy(offset, c).wait_recv()
        means = [stats[offset, c, 0] for offset in range(counts["lon"])]
        mean = sum(means[1:], means[0]) * (1.0 / counts["lon"])
        squares = sum([stats[offset, c, 1] for offset in range(1, counts["lon"])], stats[0, c, 1])
        apart = sum([(other - mean) * (other - mean) for other in means[1:]], (means[0] - mean) * (means[0] - mean))
        variance = (squares + width * apart) * (1.0 / (width * counts["lon"]))
        scale = lax.rsqrt(variance + 0.0001)
        for i in range(rows):
            for half in range(2):
                for kind, values in ((0, mean), (1, scale)):
                    moments_out[kind, c * rows + i, pl.ds(half * height, height), :] = values[i * height:(i + 1) * height]
        for offset in range(1, counts["lon"]):
            stat_copy(offset, c).wait_send()
        sent((STEPS - 1) % 2, c)

    def step(s, carry):
        p = lax.rem(s, 2)
        q = 1 - p

        def chunk(c, carry):
            @pl.when(s == 0)
            def _():
                for copy in load(c)[1:]:
                    copy.wait()

            @pl.when(s >= 1)
            def _():
                sent(q, c)

            arrived(p, c)

            def row(i, carry):
                y = c * rows + i
                for z in range(height):
                    for side, x in ((0, PAD - 1), (1, PAD + width)):
                        field[p, z + 1, y + 1, pl.ds(x, 1), :] = xrecv[side, p, c, pl.ds(i * height + z, 1), :]
                for x in range(0, width, XBLOCK):
                    here = pl.ds(PAD + x, XBLOCK)
                    planes = [field[p, z, y + 1, here, :] for z in range(height + 2)]
                    for z in range(height):
                        middle = planes[z + 1]
                        spread = (
                            field[p, z + 1, y, here, :] + field[p, z + 1, y + 2, here, :]
                            + field[p, z + 1, y + 1, pl.ds(PAD + x - 1, XBLOCK), :]
                            + field[p, z + 1, y + 1, pl.ds(PAD + x + 1, XBLOCK), :]
                            + planes[z] + planes[z + 2] - 6.0 * middle
                        )
                        cells = pl.ds(x * height + z, XBLOCK, stride=height)
                        field[q, z + 1, y + 1, here, :] = middle + ratio[y, cells, :] * spread + forcing[y, cells, :]
                pack(q, c, i)
                return carry

            lax.fori_loop(0, rows, row, 0)

            @pl.when(s < STEPS - 1)
            def _():
                send(q, c)

            @pl.when(s == STEPS - 1)
            def _():
                def finish(i, carry):
                    y = c * rows + i
                    for z in range(height):
                        line = field[q, z + 1, y + 1, inner, :]
                        raw[y, pl.ds(z, width, stride=height), :] = line
                        mean = jnp.sum(line, axis=0, keepdims=True) * (1.0 / width)
                        centred = line - mean
                        stats[0, c, 0, pl.ds(i * height + z, 1), :] = mean
                        stats[0, c, 1, pl.ds(i * height + z, 1), :] = jnp.sum(centred * centred, axis=0, keepdims=True)
                    return carry

                lax.fori_loop(0, rows, finish, 0)
                for offset in range(1, counts["lon"]):
                    stat_copy(offset, c).start()

                @pl.when(c >= 1)
                def _():
                    combine(c - 1)

            return carry

        lax.fori_loop(0, chunks, chunk, 0)
        return carry

    lax.fori_loop(0, STEPS, step, 0)


    combine(chunks - 1)


def swap_kernel(
    sizes, rows,
    heat_in, ratio_in, forcing_in, heat_out, score_out, seam_far, seam_near, seam_rows, moments,
    field, rim, core, ratio_far, forcing_far, back, stage,
    xsend, xrecv, csend, crecv, ends, ends_far, stats,
    load_sem, send_sem, ysend_sem, scale_recv, rim_recv, inner_recv, ends_recv, outer_recv,
    xrecv_sem, yrecv_sem, cxrecv_sem, cyrecv_sem, stat_recv, seam_sem, hello,
):
    depth, width, height = sizes
    half, planes, inside = width // 2, 2 * height, height - 2
    chunks = depth // rows
    units = chunks // 2
    sent_at = height * half
    inner = pl.ds(PAD, half)
    forcing, ratio = heat_out, score_out
    places = {axis: lax.axis_index(axis) for axis in ("lat", "lon", "lev")}
    counts = {axis: lax.axis_size(axis) for axis in ("lat", "lon", "lev")}
    upper = places["lev"] == 1

    def beside(axis, offset):
        return {axis: lax.rem(places[axis] + offset + counts[axis], counts[axis])}

    def rows_of(c):
        return pl.ds(c * rows, rows)

    def chunk_of(u, side):
        return u + side * (chunks - 1 - 2 * u)

    def first_lanes(shape):
        return lax.broadcasted_iota(jnp.int32, shape, 1) < shape[1] // 2

    def turned(values):
        return pltpu.roll(values, values.shape[1] // 2, 1)

    def remote(source, target, send_sem, recv_sem, device):
        return pltpu.make_async_remote_copy(
            src_ref=source, dst_ref=target, send_sem=send_sem, recv_sem=recv_sem,
            device_id=device, device_id_type=MESH,
        )

    partner = beside("lev", 1)

    def load(kind, c, slot):
        source = (heat_in, ratio_in, forcing_in)[kind]
        return pltpu.make_async_copy(source.at[rows_of(c)], stage.at[kind, slot], load_sem.at[kind, slot])

    def ratio_copy(u, span):
        cells = pl.ds(sent_at, sent_at)
        return remote(ratio.at[span, cells], ratio_far.at[span], send_sem.at[0], scale_recv.at[u], partner)

    def forcing_copy(u, span):
        cells = pl.ds(sent_at, sent_at)
        return remote(forcing.at[span, cells], forcing_far.at[span], send_sem.at[1], scale_recv.at[u], partner)

    def rim_copy(end, u, c):
        return remote(
            rim.at[end, rows_of(c)], field.at[0, (height, planes - 1)[end], pl.ds(1 + c * rows, rows), inner],
            send_sem.at[2], rim_recv.at[u], partner,
        )

    def inner_copy(u, c):
        return remote(
            field.at[STEPS % 2, pl.ds(height + 1, inside), pl.ds(1 + c * rows, rows), inner],
            back.at[pl.ds(1, inside), rows_of(c)], send_sem.at[3], inner_recv.at[u], partner,
        )

    def outer_copy(end, u, c):
        return remote(
            field.at[STEPS % 2, (height, planes - 1)[end], pl.ds(1 + c * rows, rows), inner],
            back.at[(0, height - 1)[end], rows_of(c)], send_sem.at[9], outer_recv.at[u], partner,
        )

    def ends_copy(u):
        return remote(ends.at[1, u], ends_far.at[u], send_sem.at[8], ends_recv.at[u], partner)

    def xcopy(level, side, u):
        return remote(
            xsend.at[level, u, side], xrecv.at[level, u, 1 - side],
            send_sem.at[4], xrecv_sem.at[lax.rem(level, 2), u], beside("lon", (-1, 1)[side]),
        )

    def ycopy(level, side):
        p = lax.rem(level, 2)
        return remote(
            field.at[p, :, (1, depth)[side], inner], field.at[p, :, (depth + 1, 0)[side], inner],
            ysend_sem.at[p], yrecv_sem.at[p], beside("lat", (-1, 1)[side]),
        )

    def core_xcopy(side, u):
        return remote(
            csend.at[u, side], crecv.at[u, 1 - side], send_sem.at[5], cxrecv_sem.at[u], beside("lon", (-1, 1)[side])
        )

    def core_ycopy(side):
        return remote(
            core.at[:, (1, depth)[side], inner], core.at[:, (depth + 1, 0)[side], inner],
            send_sem.at[6], cyrecv_sem.at[0], beside("lat", (-1, 1)[side]),
        )

    def stat_copy(offset, u):
        return remote(
            stats.at[0, u], stats.at[offset, u], send_sem.at[7], stat_recv.at[lax.rem(u, 2)], beside("lon", offset)
        )

    def wait_all(ref, sem):
        pltpu.make_async_copy(ref, ref, sem).wait()

    def over(count, body):
        def step(i, carry):
            body(i)
            return carry

        lax.fori_loop(0, count, step, 0)


    def split(kind, slot, i, z, x):
        low = stage[kind, slot, i, pl.ds(x * height + z, XBLOCK, stride=height), :]
        high = stage[kind, slot, i, pl.ds((half + x) * height + z, XBLOCK, stride=height), :]
        mask = first_lanes(low.shape)
        one = jnp.where(mask, low, turned(high))
        two = jnp.where(mask, turned(low), high)
        return jnp.where(upper, two, one), jnp.where(upper, one, two)

    def split_into(target, kind, slot, c):
        def row(i):
            for z in range(height):
                for x in range(0, half, XBLOCK):
                    kept, sent = split(kind, slot, i, z, x)
                    target[c * rows + i, pl.ds(z * half + x, XBLOCK), :] = kept
                    target[c * rows + i, pl.ds(sent_at + z * half + x, XBLOCK), :] = sent

        over(rows, row)

    def split_heat(u, slot, c):
        def row(i):
            y = c * rows + i
            for z in range(height):
                for x in range(0, half, XBLOCK):
                    here = pl.ds(PAD + x, XBLOCK)
                    kept, sent = split(0, slot, i, z, x)
                    field[0, z, y + 1, here, :] = kept
                    if 0 < z < height - 1:
                        core[z - 1, y + 1, here, :] = sent
                        field[0, height + z, y + 1, here, :] = jnp.zeros_like(sent)
                    else:
                        rim[min(z, 1), y, pl.ds(x, XBLOCK), :] = sent
            for side, x in ((0, PAD), (1, PAD + half - 1)):
                csend[u, side, slot * rows + i] = jnp.zeros(csend.shape[3:], csend.dtype)
                for n in range(inside):
                    csend[u, side, slot * rows + i, pl.ds(n, 1), :] = core[n, y + 1, pl.ds(x, 1), :]

        over(rows, row)

    def prepare(u, side):
        c = chunk_of(u, side)
        load(1, c, side).wait()
        split_into(ratio, 1, side, c)

        @pl.when((u == 0) & (side == 0) & jnp.logical_not(upper))
        def _():
            pl.semaphore_wait(barrier, 1)
            pl.semaphore_signal(hello.at[0], inc=1, device_id=partner, device_id_type=MESH)

        @pl.when((u == 0) & (side == 0) & upper)
        def _():
            pl.semaphore_wait(hello.at[0], 1)
            for device in around:
                pl.semaphore_signal(barrier, inc=1, device_id=device, device_id_type=MESH)

        ratio_copy(u, rows_of(c)).start()
        load(0, c, side).wait()
        split_heat(u, side, c)
        for end in (0, 1):
            rim_copy(end, u, c).start()

        @pl.when((u == 0) & (side == 1) & upper)
        def _():
            pl.semaphore_wait(barrier, len(around))
            pl.semaphore_signal(hello.at[1], inc=1, device_id=partner, device_id_type=MESH)

        @pl.when((u == 0) & (side == 1) & jnp.logical_not(upper))
        def _():
            pl.semaphore_wait(hello.at[1], 1)

        @pl.when(side == 1)
        def _():
            for end in (0, 1):
                core_xcopy(end, u).start()

        @pl.when((side == 1) & (u == 0))
        def _():
            for end in (0, 1):
                core_ycopy(end).start()

        load(2, c, side).wait()
        split_into(forcing, 2, side, c)

        @pl.when(u < units - 1)
        def _():
            for kind in (1, 0, 2):
                load(kind, chunk_of(u + 1, side), side).start()

    def correct(u, side):
        c = chunk_of(u, side)

        @pl.when(side == 0)
        def _():
            wait_all(crecv.at[u], cxrecv_sem.at[u])

        @pl.when((side == 0) & (u == 0))
        def _():
            wait_all(core.at[:, pl.ds(0, 2), inner], cyrecv_sem.at[0])

        def row(i):
            y = c * rows + i
            k = side * rows + i
            mask = first_lanes(crecv.shape[3:])
            left = turned(jnp.where(mask, csend[u, 1, k], crecv[u, 0, k]))
            right = turned(jnp.where(mask, crecv[u, 1, k], csend[u, 0, k]))
            for n in range(inside):
                core[n, y + 1, pl.ds(PAD - 1, 1), :] = left[n:n + 1]
                core[n, y + 1, pl.ds(PAD + half, 1), :] = right[n:n + 1]
            for x in range(0, half, XBLOCK):
                here = pl.ds(PAD + x, XBLOCK)
                middles = {n: core[n, y + 1, here, :] for n in range(inside)}
                for z in range(height):
                    parts = [middles[n] for n in (z - 2, z) if n in middles]
                    n = z - 1
                    if n in middles:
                        parts += [
                            core[n, y, here, :] + core[n, y + 2, here, :],
                            core[n, y + 1, pl.ds(PAD + x - 1, XBLOCK), :] + core[n, y + 1, pl.ds(PAD + x + 1, XBLOCK), :],
                            -6.0 * middles[n],
                        ]
                    cells = pl.ds(sent_at + z * half + x, XBLOCK)
                    forcing[y, cells, :] = forcing[y, cells, :] + ratio[y, cells, :] * sum(parts[1:], parts[0])

        over(rows, row)
        forcing_copy(u, rows_of(c)).start()

    barrier = pltpu.get_barrier_semaphore()
    around = [beside("lat", -1), beside("lat", 1)]
    around += [beside("lon", offset) for offset in range(1, counts["lon"])]

    @pl.when(upper)
    def _():
        pl.semaphore_signal(barrier, inc=1, device_id=partner, device_id_type=MESH)

    for side in (0, 1):
        for kind in (1, 0, 2):
            load(kind, chunk_of(0, side), side).start()

    def inputs(u):
        @pl.when(u < units)
        def _():
            over(2, lambda side: prepare(u, side))

        @pl.when(u > 0)
        def _():
            over(2, lambda side: correct(u - 1, side))

    over(units + 1, inputs)


    def publish(level, u):
        p = lax.rem(level, 2)

        def row(k):
            y = row_of(u, k)
            for side, x in ((0, PAD), (1, PAD + half - 1)):
                for z in range(planes):
                    xsend[level, u, side, k, pl.ds(z, 1), :] = field[p, z, y + 1, pl.ds(x, 1), :]

        over(2 * rows, row)
        for side in (0, 1):
            xcopy(level, side, u).start()

        @pl.when(u == 0)
        def _():
            for side in (0, 1):
                ycopy(level, side).start()

    def arrive(u):
        wait_all(ratio_far.at[pl.ds(0, 4 * rows)], scale_recv.at[u])
        wait_all(rim.at[:, pl.ds(0, 2 * rows)], rim_recv.at[u])
        publish(0, u)

    def advance(s, u):
        level = s - 1
        p = lax.rem(level, 2)
        q = 1 - p

        @pl.when(u == 0)
        def _():
            wait_all(field.at[p, :, pl.ds(0, 2), inner], yrecv_sem.at[p])

        @pl.when((u == 0) & (s >= 2))
        def _():
            wait_all(field.at[q, :, pl.ds(0, 2), inner], ysend_sem.at[q])

        wait_all(xrecv.at[level, u], xrecv_sem.at[p, u])
        over(2, lambda side: march_rows(level, p, q, u, side))

        @pl.when(s < STEPS)
        def _():
            publish(s, u)

        @pl.when(s == STEPS)
        def _():
            for side in (0, 1):
                inner_copy(u, chunk_of(u, side)).start()
            over(2 * rows, lambda k: end_moments(u, k))
            ends_copy(u).start()

        @pl.when((s == STEPS) & (u > 0))
        def _():
            for side in (0, 1):
                for end in (0, 1):
                    outer_copy(end, u - 1, chunk_of(u - 1, side)).start()

        @pl.when((s == STEPS) & (u == units - 1))
        def _():
            over(2 * rows, lambda k: keep_seam(u, k))
            for end in (0, 1):
                seam_copy(end).start()

    def keep_seam(u, k):
        for end in (0, 1):
            seam_near[end, k] = field[STEPS % 2, end * (height - 1), row_of(u, k) + 1, inner, :]

    def seam_copy(end):
        span = pl.ds((units - 1) * rows + 1, 2 * rows)
        plane = field.at[STEPS % 2, (height, planes - 1)[end], span, inner]
        return pltpu.make_async_copy(plane, seam_far.at[end], seam_sem.at[end])

    def row_of(u, k):
        return chunk_of(u, k // rows) * rows + lax.rem(k, rows)

    def end_moments(u, k):
        for whose in (0, 1):
            for end in (0, 1):
                line = field[STEPS % 2, whose * height + end * (height - 1), row_of(u, k) + 1, inner, :]
                mean = both_halves(jnp.sum(line, axis=0, keepdims=True)) * (1.0 / width)
                centred = line - mean
                squares = both_halves(jnp.sum(centred * centred, axis=0, keepdims=True))
                ends[whose, u, pl.ds(2 * k + end, 1), :] = jnp.where(first_lanes(mean.shape), mean, squares)

    def both_halves(sums):
        tall = jnp.broadcast_to(sums, (8, sums.shape[1]))
        return (tall + turned(tall))[:1]

    def march_rows(level, p, q, u, side):
        c = chunk_of(u, side)

        def row(i):
            y = c * rows + i
            k = side * rows + i
            mask = first_lanes(xrecv.shape[4:])
            left = turned(jnp.where(mask, xsend[level, u, 1, k], xrecv[level, u, 0, k]))
            right = turned(jnp.where(mask, xrecv[level, u, 1, k], xsend[level, u, 0, k]))
            for z in range(planes):
                field[p, z, y + 1, pl.ds(PAD - 1, 1), :] = left[z:z + 1]
                field[p, z, y + 1, pl.ds(PAD + half, 1), :] = right[z:z + 1]
            for x in range(0, half, XCELLS):
                here = pl.ds(PAD + x, XCELLS)
                middles = [field[p, z, y + 1, here, :] for z in range(planes)]
                for z in range(planes):
                    middle = middles[z]
                    spread = (
                        field[p, z, y, here, :] + field[p, z, y + 2, here, :]
                        + field[p, z, y + 1, pl.ds(PAD + x - 1, XCELLS), :]
                        + field[p, z, y + 1, pl.ds(PAD + x + 1, XCELLS), :]
                        + middles[z - 1] + middles[(z + 1) % planes]
                        - 6.0 * middle
                    )
                    if z < height:
                        cells = pl.ds(z * half + x, XCELLS)
                        scale, source = ratio[y, cells, :], forcing[y, cells, :]
                    else:
                        cells = pl.ds((z - height) * half + x, XCELLS)
                        scale, source = ratio_far[y, cells, :], forcing_far[y, cells, :]
                    field[q, z, y + 1, here, :] = middle + scale * spread + source

        over(rows, row)

    def wave(w):
        @pl.when(w < units)
        def _():
            arrive(w)

        def step(i):
            u = w - 1 - i

            @pl.when((u >= 0) & (u < units))
            def _():
                advance(i + 1, u)

        over(STEPS, step)

    over(units + STEPS, wave)


    def join(y, z, x):
        here = pl.ds(PAD + x, XBLOCK)
        kept, other = field[STEPS % 2, z, y + 1, here, :], back[z, y, pl.ds(x, XBLOCK), :]
        if 0 < z < height - 1:
            other = other + core[z - 1, y + 1, here, :]
        mask = first_lanes(kept.shape)
        one, two = jnp.where(upper, other, kept), jnp.where(upper, kept, other)
        low = jnp.where(mask, one, turned(two))
        high = jnp.where(mask, turned(one), two)
        heat_out[y, pl.ds(x * height + z, XBLOCK, stride=height), :] = low
        heat_out[y, pl.ds((half + x) * height + z, XBLOCK, stride=height), :] = high
        return [low, high]

    def join_inner(u, k):
        y = row_of(u, k)
        for z in range(1, height - 1):
            line = jnp.concatenate(sum([join(y, z, x) for x in range(0, half, XBLOCK)], []), axis=0)
            mean = jnp.sum(line, axis=0, keepdims=True) * (1.0 / width)
            centred = line - mean
            stats[0, u, 0, pl.ds(k * height + z, 1), :] = mean
            stats[0, u, 1, pl.ds(k * height + z, 1), :] = jnp.sum(centred * centred, axis=0, keepdims=True)

    def share_moments(u):
        mask = first_lanes(ends_far.shape[1:])
        mine, far = ends[0, u], ends_far[u]
        one, two = jnp.where(upper, far, mine), jnp.where(upper, mine, far)
        for kind, lines in ((0, jnp.where(mask, one, turned(two))), (1, jnp.where(mask, turned(one), two))):
            for k in range(2 * rows):
                for end in (0, 1):
                    at = k * height + end * (height - 1)
                    stats[0, u, kind, pl.ds(at, 1), :] = lines[2 * k + end:2 * k + end + 1]
        for offset in range(1, counts["lon"]):
            stat_copy(offset, u).start()

    def combine(u):
        wait_all(stats.at[pl.ds(1, counts["lon"] - 1), u], stat_recv.at[lax.rem(u, 2)])
        means = [stats[offset, u, 0] for offset in range(counts["lon"])]
        mean = sum(means[1:], means[0]) * (1.0 / counts["lon"])
        squares = sum([stats[offset, u, 1] for offset in range(1, counts["lon"])], stats[0, u, 1])
        apart = sum([(other - mean) * (other - mean) for other in means[1:]], (means[0] - mean) * (means[0] - mean))
        variance = (squares + width * apart) * (1.0 / (width * counts["lon"]))
        scale = lax.rsqrt(variance + 0.0001)
        for k in range(2 * rows):
            for copy in range(2):
                for kind, values in ((0, mean), (1, scale)):
                    moments[u, kind, k, pl.ds(copy * height, height), :] = values[k * height:(k + 1) * height]

    def join_outer(u, k):
        y = row_of(u, k)
        for z in (0, height - 1):
            for x in range(0, half, XBLOCK):
                join(y, z, x)
        values = heat_out[y]
        tall = values.reshape(half, 2 * height, values.shape[1])
        score_out[y] = ((tall - moments[u, 0, k][None]) * moments[u, 1, k][None]).reshape(values.shape)

    wait_all(ratio.at[:, pl.ds(sent_at, sent_at)], send_sem.at[0])
    wait_all(forcing.at[:, pl.ds(sent_at, sent_at)], send_sem.at[1])

    def finish(u):
        wait_all(back.at[pl.ds(0, inside), pl.ds(0, 2 * rows)], inner_recv.at[u])
        over(2 * rows, lambda k: join_inner(u, k))
        wait_all(ends_far.at[u], ends_recv.at[u])
        share_moments(u)
        combine(u)

        @pl.when(u > 0)
        def _():
            wait_all(back.at[pl.ds(0, 2), pl.ds(0, 2 * rows)], outer_recv.at[u - 1])
            over(2 * rows, lambda k: join_outer(u - 1, k))

    over(units, finish)

    def seam_row(k):
        seam_rows[k] = heat_out[row_of(units - 1, k)]

    over(2 * rows, seam_row)
    wait_all(rim, send_sem.at[2])
    for end in (0, 1):
        seam_copy(end).wait()
    wait_all(field.at[STEPS % 2, pl.ds(height + 1, inside), pl.ds(1, depth), inner], send_sem.at[3])
    wait_all(field.at[STEPS % 2, pl.ds(height, 2), pl.ds(1, depth - 2 * rows), inner], send_sem.at[9])
    wait_all(xsend, send_sem.at[4])
    wait_all(csend, send_sem.at[5])
    wait_all(core.at[:, pl.ds(0, 2), inner], send_sem.at[6])
    wait_all(field.at[(STEPS - 1) % 2, :, pl.ds(0, 2), inner], ysend_sem.at[(STEPS - 1) % 2])
    wait_all(stats.at[pl.ds(1, counts["lon"] - 1)], send_sem.at[7])
    wait_all(ends_far, send_sem.at[8])


def swap(sizes, arrays):
    depth, width, height = sizes
    members = arrays[0].shape[-1]
    rows = 2
    chunks = depth // rows
    units = chunks // 2
    half = width // 2
    lon = lax.axis_size("lon")
    flat = (depth, width * height, members)
    f32 = jnp.float32
    dma = pltpu.SemaphoreType.DMA
    vmem = lambda *shape: pltpu.VMEM((*shape, members), f32)
    return pl.pallas_call(
        functools.partial(swap_kernel, sizes, rows),
        out_shape=(
            pltpu.VMEM(flat, f32), pltpu.VMEM(flat, f32),
            jax.ShapeDtypeStruct((2, 2 * rows, half, members), f32), vmem(2, 2 * rows, half),
            vmem(2 * rows, width * height), vmem(units, 2, 2 * rows, 2 * height),
        ),
        in_specs=[pl.BlockSpec(memory_space=pl.ANY)] * 3,
        out_specs=tuple(pl.BlockSpec(memory_space=pltpu.HBM if i == 2 else pltpu.VMEM) for i in range(6)),
        scratch_shapes=[
            vmem(2, 2 * height, depth + 2, half + 2 * PAD),
            vmem(2, depth, half),
            vmem(height - 2, depth + 2, half + 2 * PAD),
            vmem(depth, half * height),
            vmem(depth, half * height),
            vmem(height, depth, half),
            vmem(3, 2, rows, width * height),
            vmem(STEPS, units, 2, 2 * rows, 2 * height), vmem(STEPS, units, 2, 2 * rows, 2 * height),
            vmem(units, 2, 2 * rows, 8), vmem(units, 2, 2 * rows, 8),
            vmem(2, units, 4 * rows), vmem(units, 4 * rows),
            vmem(lon, units, 2, 2 * rows * height),
            dma((3, 2)), dma((10,)), dma((2,)),
            dma((units,)), dma((units,)), dma((units,)), dma((units,)), dma((units,)),
            dma((2, units)), dma((2,)), dma((units,)), dma((1,)), dma((2,)), dma((2,)), pltpu.SemaphoreType.REGULAR((2,)),
        ],
        compiler_params=pltpu.CompilerParams(
            collective_id=1, has_side_effects=True, vmem_limit_bytes=46 * 1024 * 1024
        ),
        name="swap",
    )(*arrays)


def march(sizes, arrays):
    depth, width, height = sizes
    members = arrays[0].shape[-1]
    rows = 2
    chunks = depth // rows
    lon = lax.axis_size("lon")
    flat = (depth, width * height, members)
    f32 = jnp.float32
    anywhere = pl.BlockSpec(memory_space=pl.ANY)
    dma = pltpu.SemaphoreType.DMA
    return pl.pallas_call(
        functools.partial(march_kernel, (depth, width, height), chunks, rows),
        out_shape=(pltpu.VMEM(flat, f32), pltpu.VMEM((2, depth, 2 * height, members), f32)),
        in_specs=[anywhere] * 3,
        out_specs=(pl.BlockSpec(memory_space=pltpu.VMEM),) * 2,
        scratch_shapes=[
            pltpu.VMEM((2, height + 2, depth + 2, width + 2 * PAD, members), f32),
            pltpu.VMEM(flat, f32),
            pltpu.VMEM(flat, f32),
            pltpu.VMEM((2, 2, chunks, rows * height, members), f32),
            pltpu.VMEM((2, 2, chunks, rows * height, members), f32),
            pltpu.VMEM((lon, chunks, 2, rows * height, members), f32),
            dma((chunks,)), dma((chunks,)), dma((chunks,)),
            dma((2, 2, chunks)), dma((2, 2, chunks)),
            dma((2, 2, chunks)), dma((2, 2, chunks)),
            dma((2, 2)), dma((2, 2)),
            dma((lon - 1, chunks)), dma((lon - 1, chunks)),
        ],
        compiler_params=pltpu.CompilerParams(
            collective_id=0, has_side_effects=True, vmem_limit_bytes=48 * 1024 * 1024
        ),
        name="march",
    )(*arrays)


def copy_kernel(spans, heat, scored, score, end, sem):
    copies = []
    for c, (first, rows) in enumerate(spans):
        span = pl.ds(first, rows)
        copies.append(pltpu.make_async_copy(heat.at[span], end.at[span], sem.at[0, c]))
        copies.append(pltpu.make_async_copy(scored.at[span], score.at[span], sem.at[1, c]))
    for copy in copies:
        copy.start()
    for copy in copies:
        copy.wait()


def seam_kernel(sizes, far, near, rows_in, moments, score_in, end_in, score, end, joined, scored, sem):
    width, height, first = sizes
    half = width // 2
    unit = moments.shape[0] - 1
    upper = lax.axis_index("lev") == 1

    def out_copies(k):
        return [
            pltpu.make_async_copy(source.at[k], target.at[first + k], sem.at[kind, k])
            for kind, (source, target) in enumerate(((joined, end), (scored, score)))
        ]

    def row(k, carry):
        joined[k] = rows_in[k]
        for side, z in ((0, 0), (1, height - 1)):
            for x in range(0, half, XBLOCK):
                kept, other = near[side, k, pl.ds(x, XBLOCK), :], far[side, k, pl.ds(x, XBLOCK), :]
                mask = lax.broadcasted_iota(jnp.int32, kept.shape, 1) < kept.shape[1] // 2
                one, two = jnp.where(upper, other, kept), jnp.where(upper, kept, other)
                turn = kept.shape[1] // 2
                joined[k, pl.ds(x * height + z, XBLOCK, stride=height), :] = jnp.where(mask, one, pltpu.roll(two, turn, 1))
                joined[k, pl.ds((half + x) * height + z, XBLOCK, stride=height), :] = jnp.where(
                    mask, pltpu.roll(one, turn, 1), two
                )
        out_copies(k)[0].start()
        values = joined[k]
        tall = values.reshape(half, 2 * height, values.shape[1])
        scored[k] = ((tall - moments[unit, 0, k][None]) * moments[unit, 1, k][None]).reshape(values.shape)
        out_copies(k)[1].start()
        return carry

    lax.fori_loop(0, joined.shape[0], row, 0)
    for k in range(joined.shape[0]):
        for copy in out_copies(k):
            copy.wait()


def score_kernel(chunks, heat, moments, score, end, scaled, score_sem, end_sem):
    rows = heat.shape[0] // chunks
    finish = pltpu.make_async_copy(heat, end, end_sem)
    finish.start()

    def out_copy(c):
        span = pl.ds(c * rows, rows)
        return pltpu.make_async_copy(scaled.at[span], score.at[span], score_sem.at[c])

    def chunk(c, carry):
        def row(i, carry):
            y = c * rows + i
            mean, scale = moments[0, y], moments[1, y]
            values = heat[y]
            tall = values.reshape(values.shape[0] // mean.shape[0], *mean.shape)
            scaled[y] = ((tall - mean[None]) * scale[None]).reshape(values.shape)
            return carry

        lax.fori_loop(0, rows, row, 0)
        out_copy(c).start()
        return carry

    def drain(c, carry):
        out_copy(c).wait()
        return carry

    lax.fori_loop(0, chunks, chunk, 0)
    lax.fori_loop(0, chunks, drain, 0)
    finish.wait()


def local(initial_heat, diffusivity_ratio, forcing_term):
    depth, width, height, members = initial_heat.shape
    flat = (depth, width * height, members)
    f32 = jnp.float32
    anywhere = pl.BlockSpec(memory_space=pl.ANY)
    dma = pltpu.SemaphoreType.DMA
    arrays = [a.reshape(flat) for a in (initial_heat, diffusivity_ratio, forcing_term)]
    swaps = lax.axis_size("lev") == 2 and 3 <= height and 3 * height + 2 < 4 * STEPS
    swaps = swaps and depth % 4 == 0 and width % (2 * XBLOCK) == 0
    sizes = (depth, width, height)
    common = dict(out_shape=(jax.ShapeDtypeStruct(flat, f32),) * 2, out_specs=(anywhere,) * 2)
    inputs = [pl.BlockSpec(memory_space=pltpu.VMEM)] * 2
    if swaps:
        heat, scored, far, near, seam_rows, moments = swap(sizes, arrays)
        far = lax.ppermute(far, "lev", [(0, 1), (1, 0)])
        taken = seam_rows.shape[0]
        first = (depth - taken) // 2
        fourth = first // 2
        spans = [(at + i * fourth, fourth + i * (first - 2 * fourth)) for at in (0, first + taken) for i in (0, 1)]
        in_hbm = pl.BlockSpec(memory_space=pltpu.HBM)
        score, end = pl.pallas_call(
            functools.partial(copy_kernel, spans), out_shape=common["out_shape"], out_specs=(in_hbm,) * 2,
            in_specs=inputs, scratch_shapes=[dma((2, len(spans)))],
            cost_estimate=pl.CostEstimate(flops=60000000, bytes_accessed=4 * heat.nbytes, transcendentals=0),
            compiler_params=pltpu.CompilerParams(vmem_limit_bytes=8 * 1024 * 1024),
            name="emit",
        )(heat, scored)
        score, end = pl.pallas_call(
            functools.partial(seam_kernel, (width, height, first)),
            out_shape=common["out_shape"], out_specs=(in_hbm,) * 2,
            in_specs=[pl.BlockSpec(memory_space=pltpu.VMEM)] * 4 + [in_hbm] * 2,
            scratch_shapes=[pltpu.VMEM(seam_rows.shape, f32)] * 2 + [dma((2, taken))],
            input_output_aliases={4: 0, 5: 1},
            compiler_params=pltpu.CompilerParams(vmem_limit_bytes=8 * 1024 * 1024),
            name="seam",
        )(far, near, seam_rows, moments, score, end)
    else:
        parts = min(8, depth)
        score, end = pl.pallas_call(
            functools.partial(score_kernel, parts), **common, in_specs=inputs,
            scratch_shapes=[pltpu.VMEM(flat, f32), dma((parts,)), dma(())],
            compiler_params=pltpu.CompilerParams(vmem_limit_bytes=24 * 1024 * 1024),
            name="score",
        )(*march(sizes, arrays))
    return score.reshape(initial_heat.shape), end.reshape(initial_heat.shape)


def solution(mesh):
    placed = P("lat", "lon", "lev", None)
    return jax.shard_map(
        local, mesh=mesh, in_specs=(placed,) * 3, out_specs=(placed,) * 2, check_vma=False
    )
```
